128 devices in a mesh: sub: 16 (over x_hi, z, core), sta: 8 (over x_lo, y).
Axes of the slice: x: 4 (x_hi: 2, x_lo: 2; x = x_hi * 2 + x_lo), y: 4, z: 4, core: 2. Of those that a mesh axis runs over, the one named last changes fastest.
Arguments:
- voltages: bfloat16 [16, 2, 64, 65536], P('sub', None, 'sta'), may hold values from -6 to 6
- beam_weights: bfloat16 [16, 2, 32, 64], P('sub'), may hold values from -0.5 to 0.5
- station_delays: int32 [64], P('sta'), may hold values from 0 to 16383
- dm_index: int32 [32, 1], P('sta'), may hold values from 1 to 8
Outputs:
- dedispersed: float32 [16, 2, 32, 1, 65536], P(None, None, None, None, ('sub', 'sta'))
- intensity: float32 [32, 1, 65536], P(None, None, ('sub', 'sta'))
The draws below stay inside these ranges and needn't reach their ends.
Inputs may be any that keep to these rules, and one draw needn't show every extreme that they name: `station_delays`: delays in whole samples. `dm_index`: dispersion measure in steps of 10.
All inputs are finite; a program needn't handle non-finite values.
Results may differ from the reference program's by a relative error of at most 0.0006.
Values may be sent and summed in bfloat16 or wider, within the bound.
A program may use at most 320 MiB of HBM per device.

```python
import jax
import jax.numpy as jnp
from jax import lax

STATIONS = 64
BEAMS = 32
DMS = 1
SAMPLES = 65536
SUBBANDS = 16


def set_ends(values, key, low, largest):
    extent = values.shape
    spot = [jax.random.randint(jax.random.fold_in(key, axis), (), 0, extent[axis]) for axis in range(len(extent))]
    values = values.at[tuple(spot)].set(low)
    longest = extent.index(max(extent))
    spot[longest] = (spot[longest] + 1) % extent[longest]
    return values.at[tuple(spot)].set(largest)


def block_scale(rng, shape, split, low, top_value):
    def one(axis_at, shards_of):
        heights = jax.random.uniform(jax.random.fold_in(jax.random.fold_in(rng, 6), axis_at), (shards_of,), jnp.float32, low / len(split), top_value / len(split))
        return jnp.repeat(jnp.exp(heights), shape[axis_at] // shards_of).reshape((-1,) + (1,) * (len(shape) - axis_at - 1))

    gain = one(*split[0])
    for cut in split[1:]:
        gain = gain * one(*cut)
    return gain


def bell_draw(own_key, dims, scale, limit, pieces=(), kind=jnp.bfloat16):
    drawn = jax.random.normal(own_key, dims, jnp.float32) * scale
    if len(pieces) > 0:
        drawn = block_scale(own_key, dims, pieces, -0.22, 0.18) * drawn
    return jnp.clip(drawn, min=-limit, max=limit).astype(kind)


def setup_inputs(seed: int = 0) -> dict:
    streams_of = jax.random.split(jax.random.key(seed), 5)
    voltages = bell_draw(streams_of[0], (SUBBANDS, 2, STATIONS, SAMPLES), 1.0, 6.0, ((0, 16), (2, 8)))
    beam_weights = bell_draw(streams_of[1], (SUBBANDS, 2, BEAMS, STATIONS), (2 * STATIONS) ** -0.5, 0.5, ((0, 16),))
    station_delays = set_ends(jax.random.randint(streams_of[2], (STATIONS,), 0, SAMPLES // 4), jax.random.fold_in(streams_of[2], 1), 0, (SAMPLES // 4) - 1).astype(jnp.int32)
    dm_index = set_ends(jax.random.randint(streams_of[3], (BEAMS, DMS), 1, 9), jax.random.fold_in(streams_of[3], 1), 1, 8).astype(jnp.int32)
    return dict(voltages=voltages, beam_weights=beam_weights, station_delays=station_delays, dm_index=dm_index)


TWO_PI = 6.283185307179586
DISPERSION = 4148808000.0
DM_STEP = 10.0
BASE_FREQ = 120.0
CHANNEL_WIDTH = 0.1953125


def chirp_base(subband, total_len):
    positions = jnp.arange(total_len, dtype=jnp.int32)
    signed_bin = jnp.where(positions < total_len // 2, positions, positions - total_len)
    offset = CHANNEL_WIDTH * signed_bin.astype(jnp.float32) / total_len
    centre = BASE_FREQ + CHANNEL_WIDTH * (subband.astype(jnp.float32) + 0.5)
    return TWO_PI * DISPERSION * offset * offset / (centre * centre * (centre + offset))


def reference(voltages, beam_weights, station_delays, dm_index):
    dm_value = DM_STEP * dm_index.astype(jnp.float32)

    def one_subband(inputs):
        subband, volts, weights = inputs
        shifted = jax.vmap(lambda rows, shift_by: jnp.roll(rows, shift_by, axis=-1), in_axes=(1, 0), out_axes=1)(volts, station_delays)
        real_part = jnp.dot(weights[0], shifted[0], preferred_element_type=jnp.float32) - jnp.dot(weights[1], shifted[1], preferred_element_type=jnp.float32)
        imag_part = jnp.dot(weights[0], shifted[1], preferred_element_type=jnp.float32) + jnp.dot(weights[1], shifted[0], preferred_element_type=jnp.float32)
        spectrum = jnp.fft.fft(lax.complex(real_part, imag_part), axis=-1)
        phase_table = dm_value[:, :, None] * chirp_base(subband, SAMPLES)[None, None, :]
        chirped = spectrum[:, None, :] * lax.complex(jnp.cos(phase_table), jnp.sin(phase_table))
        series = jnp.fft.ifft(chirped, axis=-1)
        return jnp.stack([jnp.real(series), jnp.imag(series)], axis=0)

    dedispersed = lax.map(one_subband, (jnp.arange(SUBBANDS, dtype=jnp.int32), voltages, beam_weights))
    intensity = jnp.mean(dedispersed[:, 0] * dedispersed[:, 0] + dedispersed[:, 1] * dedispersed[:, 1], axis=0)
    return dedispersed, intensity
```

```python
import functools

import jax
import jax.numpy as jnp
import numpy as np
from jax import lax
from jax.experimental import pallas as pl
from jax.experimental.pallas import tpu as pltpu
from jax.sharding import PartitionSpec as P

TWO_PI = 6.283185307179586
DISPERSION = 4148808000.0
DM_STEP = 10.0
BASE_FREQ = 120.0
CHANNEL_WIDTH = 0.1953125
F32 = jnp.float32
BF16 = jnp.bfloat16
N = 65536
STA = 8
SUB = 16
INV_SQRT2 = 0.7071067811865476


def dft_tables():
    k = np.arange(128)
    ang = 2.0 * np.pi * ((k[:, None] * k[None, :]) % 128) / 128.0
    full = np.concatenate([np.cos(ang), np.sin(ang)], axis=1).astype(np.float32)
    hi = full.astype(jnp.bfloat16)
    lo = (full - hi.astype(np.float32)).astype(jnp.bfloat16)
    return np.concatenate([hi, hi], axis=0), lo


def twist_tables():
    ka = np.arange(64)[:, None]
    n = np.arange(1024)[None, :]
    ang = 2.0 * np.pi * (ka * n) / N
    big = np.stack([np.cos(ang), np.sin(ang)]).reshape(2, 64, 8, 128)
    kj = np.arange(8)[:, None]
    c = np.arange(128)[None, :]
    ang = 2.0 * np.pi * (kj * c) / 1024.0
    small = np.stack([np.cos(ang), np.sin(ang)])
    return big.astype(np.float32), small.astype(np.float32)


def chirp_base(subband):
    row = lax.broadcasted_iota(jnp.int32, (512, 128), 0)
    lane = lax.broadcasted_iota(jnp.int32, (512, 128), 1)
    positions = row + 512 * lane
    signed_bin = jnp.where(positions < N // 2, positions, positions - N)
    offset = CHANNEL_WIDTH * signed_bin.astype(F32) / N
    centre = BASE_FREQ + CHANNEL_WIDTH * (subband.astype(F32) + 0.5)
    return TWO_PI * DISPERSION * offset * offset / (centre * centre * (centre + offset))


def sign_rows():
    row = lax.broadcasted_iota(jnp.int32, (8, 128), 0)
    return jnp.where(row < 4, 1.0, -1.0).astype(F32)


def swap(x):
    return pltpu.roll(x, 4, x.ndim - 2)


def dft8(x, sg):
    def times_j(v):
        return swap(v) * sg

    def dft4(a0, a1, a2, a3):
        t0, t1, t2, t3 = a0 + a2, a0 - a2, a1 + a3, times_j(a1 - a3)
        return t0 + t2, t1 + t3, t0 - t2, t1 - t3

    e = dft4(x[0], x[2], x[4], x[6])
    o = dft4(x[1], x[3], x[5], x[7])
    j1, j3 = times_j(o[1]), times_j(o[3])
    o = (o[0], (o[1] + j1) * INV_SQRT2, times_j(o[2]), (j3 - o[3]) * INV_SQRT2)
    return [e[k] + o[k] for k in range(4)] + [e[k] - o[k] for k in range(4)]


def cmul(x, wr, wi, sg):
    return x * wr + (swap(x) * sg) * wi


def w64(a, k):
    ang = 2.0 * np.pi * ((a * k) % 64) / 64.0
    return float(np.cos(ang)), float(np.sin(ang))


def split(x):
    hi = x.astype(BF16)
    lo = (x - hi.astype(F32)).astype(BF16)
    return hi, lo


def unpack_voltages(x_ref, xf_ref):
    def body(i, _):
        for u in range(8):
            t = i * 8 + u
            col = pl.multiple_of(t * 128, 128)
            for ri in range(2):
                xf_ref[ri, t + 128] = x_ref[ri, :, pl.ds(col, 128)].astype(F32)
        return 0

    lax.fori_loop(0, 64, body, 0)

    def wrap(i, _):
        for u in range(8):
            for ri in range(2):
                xf_ref[ri, i * 8 + u] = xf_ref[ri, i * 8 + u + 512]
        return 0

    lax.fori_loop(0, 16, wrap, 0)


def delay_rows(d_ref, xf_ref, out_ref):
    row = lax.broadcasted_iota(jnp.int32, (8, 128), 0)
    lane = lax.broadcasted_iota(jnp.int32, (8, 128), 1)
    fine = jnp.zeros((8, 128), jnp.int32)
    starts = []
    for r in range(8):
        d = d_ref[r]
        starts.append(128 - d // 128)
        fine = jnp.where(row == r, d % 128, fine)
    masks = [row == r for r in range(8)]
    index = (lane - fine + 128) % 128
    keep = lane >= fine

    def gathered(ri, t):
        acc = xf_ref[ri, starts[0] + t]
        for r in range(1, 8):
            acc = jnp.where(masks[r], xf_ref[ri, starts[r] + t], acc)
        return jnp.take_along_axis(acc, index, axis=1)

    def body(a, carry):
        prev = list(carry)
        col = pl.multiple_of(a * 128, 128)
        for j in range(8):
            done = []
            for ri in range(2):
                now = gathered(ri, a * 8 + j)
                done.append(jnp.where(keep, now, prev[ri]))
                prev[ri] = now
            out_ref[j, :, pl.ds(col, 128)] = jnp.concatenate(done, axis=0).astype(BF16)
        return tuple(prev)

    lax.fori_loop(0, 64, body, (gathered(0, -1), gathered(1, -1)))


def p1_kernel(d_ref, x_ref, out_ref, xf_ref):
    unpack_voltages(x_ref, xf_ref)
    delay_rows(d_ref, xf_ref, out_ref)


def beamform(w_ref, v_ref, bm_ref):
    w = w_ref[...]

    def body(i, _):
        col = pl.multiple_of(i * 512, 512)
        v = v_ref[:, :, pl.ds(col, 512)].reshape(128, 512)
        out = jnp.dot(w, v, preferred_element_type=F32)
        for u in range(4):
            bm_ref[i * 4 + u] = out[:, u * 128 : (u + 1) * 128].reshape(8, 8, 128)
        return 0

    lax.fori_loop(0, 16, body, 0)


def dft64_forward(bm_ref, put, tiles, sg, twist, group=2):
    for a0 in range(8):

        def first(g, _):
            at = pl.ds(g * group, group)
            y = dft8([bm_ref[8 * a1 + a0, at] for a1 in range(8)], sg)
            for k0 in range(8):
                v = y[k0]
                if a0 * k0:
                    wr, wi = w64(a0, k0)
                    v = cmul(v, wr, wi, sg)
                bm_ref[8 * k0 + a0, at] = v
            return 0

        lax.fori_loop(0, tiles // group, first, 0)

    for k0 in range(8):

        def second(g, _):
            at = pl.ds(g * group, group)
            y = dft8([bm_ref[8 * k0 + a0, at] for a0 in range(8)], sg)
            for k1 in range(8):
                k = 8 * k1 + k0
                put(k, at, twist(k, y[k1]))
            return 0

        lax.fori_loop(0, tiles // group, second, 0)


def p2_kernel(w_ref, v_ref, tw_ref, out_ref, bm_ref):
    beamform(w_ref, v_ref, bm_ref)
    sg = sign_rows()

    def twist(k, v):
        return cmul(v, tw_ref[0, pl.ds(k, 1)], tw_ref[1, pl.ds(k, 1)], sg)

    def put(k, at, v):
        out_ref[at, k] = v

    dft64_forward(bm_ref, put, 8, sg, twist)


def chirp_table(dm_ref, base_ref, h_ref):
    row = lax.broadcasted_iota(jnp.int32, (8, 128), 0)
    quarter = jnp.where(row < 4, 1, 0)
    dm = dm_ref[...]
    p1 = 1.5703125
    p2 = float(np.float32(np.round((np.pi / 2 - p1) * 2.0**22) / 2.0**22))
    p3 = float(np.float32(np.pi / 2 - p1 - p2))

    def one(r):
        phase = dm * base_ref[pl.ds(r, 1), :]
        n = jnp.floor(phase * float(2.0 / np.pi) + 0.5)
        y = ((phase - n * p1) - n * p2) - n * p3
        q = n.astype(jnp.int32) + quarter
        z = y * y
        s = ((-1.9515295891e-4 * z + 8.3321608736e-3) * z - 1.6666654611e-1) * z * y + y
        c = ((2.443315711809948e-5 * z - 1.388731625493765e-3) * z + 4.166664568298827e-2) * z * z - 0.5 * z + 1.0
        v = jnp.where((q & 1) == 0, s, c)
        h_ref[r] = jnp.where((q & 2) == 0, v, -v)

    def body(i, _):
        for u in range(4):
            one(i * 4 + u)
        return 0

    lax.fori_loop(0, 128, body, 0)


def spectrum_and_back(r_ref, h_ref, w1_ref, w2_ref, tws_ref, twb_ref, out_put, xs_ref, g_ref):
    sg = sign_rows()

    def fwd(i, _):
        at = pl.ds(i * 2, 2)
        y = dft8([r_ref[j, at] for j in range(8)], sg)
        for kj in range(8):
            v = y[kj]
            if kj:
                v = cmul(v, tws_ref[0, pl.ds(kj, 1)], tws_ref[1, pl.ds(kj, 1)], sg)
            hi, lo = split(v.reshape(16, 128))
            at_rows = pl.ds(pl.multiple_of(kj * 512 + i * 16, 16), 16)
            xs_ref[at_rows, 0:128] = hi
            xs_ref[at_rows, 128:256] = lo
        return 0

    lax.fori_loop(0, 32, fwd, 0)

    rows = 128

    def dot128(at, sign):
        x = xs_ref[at, :]
        pq = jnp.dot(x, w1_ref[...], preferred_element_type=F32)
        pq = pq + jnp.dot(x[:, 0:128], w2_ref[...], preferred_element_type=F32)
        p = pq[:, 0:128].reshape(rows // 8, 8, 128)
        q = pq[:, 128:256].reshape(rows // 8, 8, 128)
        return p + swap(q) * sign

    low = lax.broadcasted_iota(jnp.int32, (8, 128), 0) < 4

    def mid(i, _):
        at = pl.ds(pl.multiple_of(i * rows, rows), rows)
        v = dot128(at, sg)
        h = h_ref[pl.ds(i * (rows // 8), rows // 8)]
        hs = swap(h)
        hr = jnp.where(low, h, hs)
        hi = jnp.where(low, -hs, h)
        v = v * hr + swap(v) * hi
        hi, lo = split(v.reshape(rows, 128))
        xs_ref[at, 0:128] = hi
        xs_ref[at, 128:256] = lo
        return 0

    lax.fori_loop(0, 4096 // rows, mid, 0)

    def back(i, _):
        at = pl.ds(pl.multiple_of(i * rows, rows), rows)
        v = dot128(at, -sg)
        per = 64 // (rows // 8)
        kj, part = i // per, i % per
        g_ref[pl.ds(part * (rows // 8), rows // 8), kj] = v
        return 0

    lax.fori_loop(0, 4096 // rows, back, 0)

    def inv8(ka, _):
        x = []
        for kj in range(8):
            v = g_ref[ka, kj]
            if kj:
                v = cmul(v, tws_ref[0, pl.ds(kj, 1)], tws_ref[1, pl.ds(kj, 1)], -sg)
            x.append(v)
        y = dft8(x, -sg)
        for j in range(8):
            g_ref[ka, j] = cmul(y[j], twb_ref[0, ka, pl.ds(j, 1)], twb_ref[1, ka, pl.ds(j, 1)], -sg)
        return 0

    lax.fori_loop(0, 64, inv8, 0, unroll=2)
    dft64_forward(g_ref, out_put, 8, -sg, lambda k, v: v * (1.0 / N))


def p3_kernel(r_ref, dm_ref, base_ref, w1_ref, w2_ref, tws_ref, twb_ref, out_ref, h_ref, xs_ref, g_ref):
    chirp_table(dm_ref, base_ref, h_ref)

    def put(a, at, v):
        out_ref[a, at] = v

    spectrum_and_back(r_ref, h_ref, w1_ref, w2_ref, tws_ref, twb_ref, put, xs_ref, g_ref)


def p4_kernel(r_ref, out_ref, int_ref):
    int_ref[...] = jnp.zeros_like(int_ref)

    def body(s, _):
        for sta in range(8):
            parts = []
            for ri in range(2):
                rows = [
                    r_ref[pl.ds((s * 8 + sta) * 32 + ri * 4 + b4, 4, stride=8), :] for b4 in range(4)
                ]
                block = jnp.concatenate(rows, axis=0)
                out_ref[pl.ds(pl.multiple_of(s * 256 + ri * 128 + sta * 16, 16), 16), :] = block
                parts.append(block)
            at = pl.ds(sta * 16, 16)
            int_ref[at, :] = int_ref[at, :] + (parts[0] * parts[0] + parts[1] * parts[1])
        return 0

    lax.fori_loop(0, 16, body, 0)
    int_ref[...] = int_ref[...] * (1.0 / SUB)


VM = pl.BlockSpec(memory_space=pltpu.VMEM)
SM = pl.BlockSpec(memory_space=pltpu.SMEM)
PARAMS = pltpu.CompilerParams(vmem_limit_bytes=60 * 1024 * 1024)


def p1(delays, volts):
    return pl.pallas_call(
        p1_kernel,
        out_shape=jax.ShapeDtypeStruct((8, 16, 8192), BF16),
        in_specs=[SM, VM],
        out_specs=VM,
        scratch_shapes=[pltpu.VMEM((2, 640, 8, 128), F32)],
        compiler_params=PARAMS,
    )(delays, volts)


def p2(w, v, tw):
    return pl.pallas_call(
        p2_kernel,
        out_shape=jax.ShapeDtypeStruct((8, 64, 8, 128), F32),
        in_specs=[VM, VM, VM],
        out_specs=VM,
        scratch_shapes=[pltpu.VMEM((64, 8, 8, 128), F32)],
        compiler_params=PARAMS,
    )(w, v, tw)


def p3(r, dm, base, w1, w2, tws, twb):
    return pl.pallas_call(
        p3_kernel,
        out_shape=jax.ShapeDtypeStruct((64, 8, 8, 128), F32),
        in_specs=[VM] * 7,
        out_specs=VM,
        scratch_shapes=[
            pltpu.VMEM((512, 8, 128), F32),
            pltpu.VMEM((4096, 256), BF16),
            pltpu.VMEM((64, 8, 8, 128), F32),
        ],
        compiler_params=PARAMS,
    )(r, dm, base, w1, w2, tws, twb)


def p4(r):
    return pl.pallas_call(
        p4_kernel,
        out_shape=(jax.ShapeDtypeStruct((4096, 128), F32), jax.ShapeDtypeStruct((128, 128), F32)),
        in_specs=[VM],
        out_specs=(VM, VM),
        compiler_params=PARAMS,
    )(r)


def stacked_weights(beam_weights):
    w0 = beam_weights[0, 0].reshape(8, 4, 8, 8)
    w1 = beam_weights[0, 1].reshape(8, 4, 8, 8)
    real = jnp.stack([w0, -w1], axis=3)
    imag = jnp.stack([w1, w0], axis=3)
    return jnp.stack([real, imag], axis=1).reshape(64, 128)


def shards(voltages, beam_weights, station_delays, dm_index):
    w1, w2 = dft_tables()
    big, small = twist_tables()
    send = p1(station_delays, voltages[0])
    v = lax.all_to_all(send, "sta", split_axis=0, concat_axis=0, tiled=True)
    own = lax.dynamic_index_in_dim(jnp.asarray(big), lax.axis_index("sta"), 2, keepdims=False)
    f = p2(stacked_weights(beam_weights), v, own)
    r = lax.all_to_all(f, "sta", split_axis=0, concat_axis=0, tiled=True)
    base = chirp_base(lax.axis_index("sub"))
    dm = DM_STEP * dm_index.astype(F32)
    dm = jnp.broadcast_to(jnp.concatenate([dm, dm], axis=0), (8, 128))
    y = p3(r, dm, base, jnp.asarray(w1), jnp.asarray(w2), jnp.asarray(small), jnp.asarray(big))
    z = lax.all_to_all(y.reshape(128, 32, 128), ("sub", "sta"), split_axis=0, concat_axis=0, tiled=True)
    out, power = p4(z.reshape(4096, 128))
    return out.reshape(16, 2, 32, 1, 512), power.reshape(32, 1, 512)


def solution(mesh):
    return jax.shard_map(
        shards,
        mesh=mesh,
        in_specs=(
            P("sub", None, "sta", None),
            P("sub", None, None, None),
            P("sta"),
            P("sta", None),
        ),
        out_specs=(P(None, None, None, None, ("sub", "sta")), P(None, None, ("sub", "sta"))),
        check_vma=False,
    )
```

```python
import functools

import jax
import jax.numpy as jnp
import numpy as np
from jax import lax
from jax.experimental import pallas as pl
from jax.experimental.pallas import tpu as pltpu
from jax.sharding import PartitionSpec as P

TWO_PI = 6.283185307179586
DISPERSION = 4148808000.0
DM_STEP = 10.0
BASE_FREQ = 120.0
CHANNEL_WIDTH = 0.1953125
F32 = jnp.float32
BF16 = jnp.bfloat16
N = 65536
STA = 8
SUB = 16
INV_SQRT2 = 0.7071067811865476


MESH = pl.DeviceIdType.MESH
CH = 4


def dft_tables():
    k = np.arange(128)
    ang = 2.0 * np.pi * ((k[:, None] * k[None, :]) % 128) / 128.0
    full = np.concatenate([np.cos(ang), np.sin(ang)], axis=1).astype(np.float32)
    hi = full.astype(jnp.bfloat16)
    lo = (full - hi.astype(np.float32)).astype(jnp.bfloat16)
    return np.concatenate([hi, hi], axis=0), lo


def twist_tables():
    at = np.arange(64)
    ka = (8 * (at % 8) + at // 8)[:, None]
    n = np.arange(1024)[None, :]
    ang = 2.0 * np.pi * (ka * n) / N
    big = np.stack([np.cos(ang), np.sin(ang)]).reshape(2, 64, 8, 128)
    kj = np.arange(8)[:, None]
    c = np.arange(128)[None, :]
    ang = 2.0 * np.pi * (kj * c) / 1024.0
    small = np.stack([np.cos(ang), np.sin(ang)])
    e = np.arange(8)
    ang = 2.0 * np.pi * (e[:, None] * e[None, :]) / 64.0
    inner = np.stack([np.cos(ang), np.sin(ang)])[..., None] * np.ones(128)
    return big.astype(np.float32), small.astype(np.float32), inner.astype(np.float32)


def sign_rows():
    row = lax.broadcasted_iota(jnp.int32, (8, 128), 0)
    return jnp.where(row < 4, 1.0, -1.0).astype(F32)


def swap(x):
    return pltpu.roll(x, 4, x.ndim - 2)


def dft8(x, sg):
    def times_j(v):
        return swap(v) * sg

    def dft4(a0, a1, a2, a3):
        t0, t1, t2, t3 = a0 + a2, a0 - a2, a1 + a3, times_j(a1 - a3)
        return t0 + t2, t1 + t3, t0 - t2, t1 - t3

    e = dft4(x[0], x[2], x[4], x[6])
    o = dft4(x[1], x[3], x[5], x[7])
    j1, j3 = times_j(o[1]), times_j(o[3])
    o = (o[0], (o[1] + j1) * INV_SQRT2, times_j(o[2]), (j3 - o[3]) * INV_SQRT2)
    return [e[k] + o[k] for k in range(4)] + [e[k] - o[k] for k in range(4)]


def cmul(x, wr, wi, sg):
    return x * wr + (swap(x) * sg) * wi


def split(x):
    hi = x.astype(BF16)
    lo = (x - hi.astype(F32)).astype(BF16)
    return hi, lo


def unpack_voltages(x_ref, xf_ref):
    def body(i, _):
        for u in range(8):
            t = i * 8 + u
            col = pl.multiple_of(t * 128, 128)
            for ri in range(2):
                xf_ref[ri, t + 128] = x_ref[0, ri, :, pl.ds(col, 128)].astype(F32)
        return 0

    lax.fori_loop(0, 64, body, 0)

    def wrap(i, _):
        for ri in range(2):
            xf_ref[ri, pl.ds(i * 8, 8)] = xf_ref[ri, pl.ds(i * 8 + 512, 8)]
        return 0

    lax.fori_loop(0, 16, wrap, 0)


def delay_setup(d_ref):
    row = lax.broadcasted_iota(jnp.int32, (8, 128), 0)
    lane = lax.broadcasted_iota(jnp.int32, (8, 128), 1)
    fine = jnp.zeros((8, 128), jnp.int32)
    starts = []
    for r in range(8):
        d = d_ref[r]
        starts.append(128 - d // 128)
        fine = jnp.where(row == r, d % 128, fine)
    return starts, [row == r for r in range(8)], (lane - fine + 128) % 128, lane >= fine


def delay_rows(setup, xf_ref, out_ref, a0):
    starts, masks, index, keep = setup

    def body(a1, _):
        t = (8 * a1 + a0) * 8
        col = pl.multiple_of((8 * a0 + a1) * 128, 128)
        done = []
        for ri in range(2):
            acc = xf_ref[ri, pl.ds(starts[0] + t - 1, 9)]
            for r in range(1, 8):
                acc = jnp.where(masks[r], xf_ref[ri, pl.ds(starts[r] + t - 1, 9)], acc)
            g = [jnp.take_along_axis(acc[u], index, axis=1) for u in range(9)]
            done.append([jnp.where(keep, g[u + 1], g[u]) for u in range(8)])
        for j in range(8):
            out_ref[j, :, pl.ds(col, 128)] = jnp.concatenate([done[0][j], done[1][j]], axis=0).astype(BF16)
        return 0

    lax.fori_loop(0, 8, body, 0)


def one_hot(shape, hit):
    row = lax.broadcasted_iota(jnp.int32, shape, 0)
    col = lax.broadcasted_iota(jnp.int32, shape, 1)
    return jnp.where(hit(row, col), 1.0, 0.0).astype(BF16)


def stacked_weights(bw_ref):
    w0, w1 = bw_ref[0, 0], bw_ref[0, 1]
    to_real = one_hot((64, 128), lambda q, c: c == (q // 8) * 16 + q % 8)
    to_imag = one_hot((64, 128), lambda q, c: c == (q // 8) * 16 + 8 + q % 8)
    dot = functools.partial(jnp.dot, preferred_element_type=F32)
    real = (dot(w0, to_real) - dot(w1, to_imag)).astype(BF16)
    imag = (dot(w1, to_real) + dot(w0, to_imag)).astype(BF16)
    rows_real = one_hot((64, 32), lambda r, b: r == (b // 4) * 8 + b % 4)
    rows_imag = one_hot((64, 32), lambda r, b: r == (b // 4) * 8 + 4 + b % 4)
    return (dot(rows_real, real) + dot(rows_imag, imag)).astype(BF16)


def beamform(w_ref, v_ref, bm_ref, part):
    w = w_ref[...]

    def body(i, _):
        first = part * 16 + i * 4
        v = v_ref[:, :, pl.ds(pl.multiple_of(first * 128, 512), 512)].reshape(128, 512)
        out = jnp.dot(w, v, preferred_element_type=F32)
        for u in range(4):
            bm_ref[first + u] = out[:, u * 128 : (u + 1) * 128].reshape(8, 8, 128)
        return 0

    lax.fori_loop(0, 4, body, 0)


def inner_pass(ref, lead, twi_ref, sg):
    def body(g, _):
        at = pl.ds(g * 2, 2)
        y = dft8([ref[8 * lead + i, at] for i in range(8)], sg)
        for k in range(8):
            v = y[k]
            if k:
                v = cmul(v, twi_ref[0, lead, pl.ds(k, 1)], twi_ref[1, lead, pl.ds(k, 1)], sg)
            ref[8 * lead + k, at] = v
        return 0

    lax.fori_loop(0, 4, body, 0)


def outer_pass(ref, tail, sg, put):
    def body(g, _):
        at = pl.ds(g * 2, 2)
        y = dft8([ref[8 * i + tail, at] for i in range(8)], sg)
        for k in range(8):
            put(k, g, y[k])
        return 0

    lax.fori_loop(0, 4, body, 0)


def chirp_table(dm_ref, base_ref, h_ref):
    row = lax.broadcasted_iota(jnp.int32, (8, 128), 0)
    lane = lax.broadcasted_iota(jnp.int32, (8, 128), 1)
    centre = BASE_FREQ + CHANNEL_WIDTH * (
        jnp.zeros((8, 128), F32) + lax.axis_index("sub").astype(F32) + 0.5
    )

    def base(i, _):
        part, kj, low = i // 16, (i // 2) % 8, i % 2
        positions = 8 * row + (2 * part + low) + 64 * kj + 512 * lane
        signed_bin = jnp.where(positions < N // 2, positions, positions - N)
        offset = CHANNEL_WIDTH * signed_bin.astype(F32) / N
        base_ref[pl.ds(pl.multiple_of(i * 8, 8), 8), :] = (
            TWO_PI * DISPERSION * offset * offset / (centre * centre * (centre + offset))
        )
        return 0

    lax.fori_loop(0, 64, base, 0)
    quarter = jnp.where(row < 4, 1, 0)
    dm = jnp.zeros((8, 128), F32)
    for b in range(4):
        dm = jnp.where(row % 4 == b, DM_STEP * dm_ref[b, 0].astype(F32), dm)
    p1 = 1.5703125
    p2 = float(np.float32(np.round((np.pi / 2 - p1) * 2.0**22) / 2.0**22))
    p3 = float(np.float32(np.pi / 2 - p1 - p2))

    def one(r):
        phase = dm * base_ref[pl.ds(r, 1), :]
        n = jnp.floor(phase * float(2.0 / np.pi) + 0.5)
        y = ((phase - n * p1) - n * p2) - n * p3
        q = n.astype(jnp.int32) + quarter
        z = y * y
        s = ((-1.9515295891e-4 * z + 8.3321608736e-3) * z - 1.6666654611e-1) * z * y + y
        c = ((2.443315711809948e-5 * z - 1.388731625493765e-3) * z + 4.166664568298827e-2) * z * z - 0.5 * z + 1.0
        v = jnp.where((q & 1) == 0, s, c)
        h_ref[r] = jnp.where((q & 2) == 0, v, -v)

    def body(i, _):
        for u in range(4):
            one(i * 4 + u)
        return 0

    lax.fori_loop(0, 128, body, 0)


def middle(p, r_ref, h_ref, w1_ref, w2_ref, tws_ref, twb_ref, xs_ref, gt_ref, g_ref, sg):
    def fwd(i, _):
        at = pl.ds(p * 16 + i * 2, 2)
        y = dft8([r_ref[j, at] for j in range(8)], sg)
        for kj in range(8):
            v = y[kj]
            if kj:
                v = cmul(v, tws_ref[0, pl.ds(kj, 1)], tws_ref[1, pl.ds(kj, 1)], sg)
            hi, lo = split(v.reshape(16, 128))
            rows = pl.ds(pl.multiple_of(kj * 128 + i * 16, 16), 16)
            xs_ref[rows, 0:128] = hi
            xs_ref[rows, 128:256] = lo
        return 0

    lax.fori_loop(0, 8, fwd, 0)

    def dot128(at, sign):
        x = xs_ref[at, :]
        pq = jnp.dot(x, w1_ref[...], preferred_element_type=F32)
        pq = pq + jnp.dot(x[:, 0:128], w2_ref[...], preferred_element_type=F32)
        return pq[:, 0:128].reshape(16, 8, 128) + swap(pq[:, 128:256].reshape(16, 8, 128)) * sign

    low = lax.broadcasted_iota(jnp.int32, (8, 128), 0) < 4

    def mid(kj, _):
        at = pl.ds(pl.multiple_of(kj * 128, 128), 128)
        v = dot128(at, sg)
        h = h_ref[pl.ds(p * 128 + kj * 16, 16)]
        hs = swap(h)
        v = v * jnp.where(low, h, hs) + swap(v) * jnp.where(low, -hs, h)
        hi, lo = split(v.reshape(128, 128))
        xs_ref[at, 0:128] = hi
        xs_ref[at, 128:256] = lo
        return 0

    lax.fori_loop(0, 8, mid, 0)

    def back(kj, _):
        gt_ref[kj] = dot128(pl.ds(pl.multiple_of(kj * 128, 128), 128), -sg)
        return 0

    lax.fori_loop(0, 8, back, 0)

    def inv8(i, _):
        at = pl.ds(i * 2, 2)
        x = []
        for kj in range(8):
            v = gt_ref[kj, at]
            if kj:
                v = cmul(v, tws_ref[0, pl.ds(kj, 1)], tws_ref[1, pl.ds(kj, 1)], -sg)
            x.append(v)
        y = dft8(x, -sg)
        here = pl.ds(p * 16 + i * 2, 2)
        for j in range(8):
            g_ref[here, j] = cmul(y[j], twb_ref[0, here, pl.ds(j, 1)], twb_ref[1, here, pl.ds(j, 1)], -sg)
        return 0

    lax.fori_loop(0, 8, inv8, 0)


def kernel(
    d_ref, dm_ref, x_hbm, bw_ref, w1_hbm, w2_hbm, tws_hbm, twb_hbm, twi_hbm,
    recv3,
    x_ref, w1_ref, w2_ref, tws_ref, twb_ref, twi_ref,
    xf_ref, send1, recv1, w_ref, bm_ref, send2, recv2, base_ref, h_ref, xs_ref, gt_ref, g_ref, send3,
    load_sem, sem1, rsem1, sem2, rsem2, sem3, rsem3,
):
    sub, sta = lax.axis_index("sub"), lax.axis_index("sta")
    me = sub * STA + sta

    x_load = pltpu.make_async_copy(x_hbm, x_ref, load_sem.at[0])
    x_load.start()
    tables = [
        pltpu.make_async_copy(a, b, load_sem.at[1 + i])
        for i, (a, b) in enumerate(
            [(w1_hbm, w1_ref), (w2_hbm, w2_ref), (tws_hbm, tws_ref), (twb_hbm, twb_ref), (twi_hbm, twi_ref)]
        )
    ]
    for t in tables:
        t.start()

    barrier = pltpu.get_barrier_semaphore()

    def greet(i, _):
        d = (me + i) % (SUB * STA)
        pl.semaphore_signal(barrier, inc=1, device_id={"sub": d // STA, "sta": d % STA}, device_id_type=MESH)
        return 0

    lax.fori_loop(1, SUB * STA, greet, 0)
    x_load.wait()
    unpack_voltages(x_ref, xf_ref)
    setup = delay_setup(d_ref)

    for part in range(CH):
        delay_rows(setup, xf_ref, send1, 2 * part)
        delay_rows(setup, xf_ref, send1, 2 * part + 1)
        if part == 0:
            pl.semaphore_wait(barrier, SUB * STA - 1)
        cols = pl.ds(part * 2048, 2048)

        def go1(i, _):
            d = (sta + i) % STA
            pltpu.make_async_remote_copy(
                src_ref=send1.at[d, :, cols],
                dst_ref=recv1.at[sta, :, cols],
                send_sem=sem1,
                recv_sem=rsem1.at[part],
                device_id={"sub": sub, "sta": d},
                device_id_type=MESH,
            ).start()
            return 0

        lax.fori_loop(1, STA, go1, 0)
        pltpu.make_async_copy(send1.at[sta, :, cols], recv1.at[sta, :, cols], rsem1.at[part]).start()

    w_ref[...] = stacked_weights(bw_ref)
    chirp_table(dm_ref, base_ref, h_ref)
    for t in tables:
        t.wait()
    sg = sign_rows()

    for part in range(CH):
        cols = pl.ds(part * 2048, 2048)
        pltpu.make_async_copy(recv1.at[:, :, cols], recv1.at[:, :, cols], rsem1.at[part]).wait()
        beamform(w_ref, recv1, bm_ref, part)
        inner_pass(bm_ref, 2 * part, twi_ref, sg)
        inner_pass(bm_ref, 2 * part + 1, twi_ref, sg)

    for part in range(CH):

        def step(low, _):
            k0 = 2 * part + low

            def put(k1, g, v):
                k = 8 * k0 + k1
                v = cmul(v, twb_ref[0, k, pl.ds(sta, 1)], twb_ref[1, k, pl.ds(sta, 1)], sg)
                send2[pl.ds(2 * g, 2), k] = v

            outer_pass(bm_ref, k0, sg, put)
            return 0

        lax.fori_loop(0, 2, step, 0)
        rows = pl.ds(part * 16, 16)

        def go2(i, _):
            d = (sta + i) % STA
            pltpu.make_async_remote_copy(
                src_ref=send2.at[d, rows],
                dst_ref=recv2.at[sta, rows],
                send_sem=sem2,
                recv_sem=rsem2.at[part],
                device_id={"sub": sub, "sta": d},
                device_id_type=MESH,
            ).start()
            return 0

        lax.fori_loop(1, STA, go2, 0)
        pltpu.make_async_copy(send2.at[sta, rows], recv2.at[sta, rows], rsem2.at[part]).start()

    for part in range(CH):
        rows = pl.ds(part * 16, 16)
        pltpu.make_async_copy(recv2.at[:, rows], recv2.at[:, rows], rsem2.at[part]).wait()
        middle(part, recv2, h_ref, w1_ref, w2_ref, tws_ref, twb_ref, xs_ref, gt_ref, g_ref, sg)
        inner_pass(g_ref, 2 * part, twi_ref, -sg)
        inner_pass(g_ref, 2 * part + 1, twi_ref, -sg)

    def group(i, _):
        a0 = (sta + i) % 8
        for g in range(4):
            y = dft8([g_ref[8 * k0 + a0, pl.ds(2 * g, 2)] for k0 in range(8)], -sg)
            for a1 in range(8):
                send3[2 * (8 * a1 + a0) + g // 2, pl.ds(2 * (g % 2), 2)] = y[a1] * (1.0 / N)

        def go3(n, _):
            d = (16 * (n // 2 + sub // 2) + 2 * a0 + n % 2) % (SUB * STA)

            @pl.when(d != me)
            def _():
                pltpu.make_async_remote_copy(
                    src_ref=send3.at[d],
                    dst_ref=recv3.at[me],
                    send_sem=sem3,
                    recv_sem=rsem3.at[sub],
                    device_id={"sub": d // STA, "sta": d % STA},
                    device_id_type=MESH,
                ).start()

            @pl.when(d == me)
            def _():
                pltpu.make_async_copy(send3.at[me], recv3.at[me], rsem3.at[sub]).start()

            return 0

        lax.fori_loop(0, 16, go3, 0)
        return 0

    lax.fori_loop(0, 8, group, 0)

    for s in range(SUB):
        block = recv3.at[pl.ds(s * STA, STA)]
        pltpu.make_async_copy(block, block, rsem3.at[s]).wait()
    others = pl.ds(0, STA - 1)
    pltpu.make_async_copy(send1.at[others], send1.at[others], sem1).wait()
    pltpu.make_async_copy(send2.at[others], send2.at[others], sem2).wait()
    others = pl.ds(0, SUB * STA - 1)
    pltpu.make_async_copy(send3.at[others], send3.at[others], sem3).wait()


def assemble(r_ref, out_ref, int_ref):
    s = pl.program_id(0)

    @pl.when(s == 0)
    def _():
        int_ref[...] = jnp.zeros_like(int_ref)

    for sta in range(STA):
        parts = []
        for ri in range(2):
            rows = [r_ref[pl.ds(sta * 32 + ri * 4 + b4, 4, stride=8), :] for b4 in range(4)]
            block = jnp.concatenate(rows, axis=0)
            out_ref[pl.ds(ri * 128 + sta * 16, 16), :] = block
            parts.append(block)
        at = pl.ds(sta * 16, 16)
        int_ref[at, :] += (parts[0] * parts[0] + parts[1] * parts[1]) * (1.0 / SUB)


VM = pl.BlockSpec(memory_space=pltpu.VMEM)
SM = pl.BlockSpec(memory_space=pltpu.SMEM)
ANY = pl.BlockSpec(memory_space=pl.ANY)


def shards(voltages, beam_weights, station_delays, dm_index):
    w1, w2 = dft_tables()
    big, small, inner = twist_tables()
    moved = pl.pallas_call(
        kernel,
        out_shape=jax.ShapeDtypeStruct((128, 4, 8, 128), F32),
        in_specs=[SM, SM, ANY, VM, ANY, ANY, ANY, ANY, ANY],
        out_specs=ANY,
        scratch_shapes=[
            pltpu.VMEM((1, 2, 8, N), BF16),
            pltpu.VMEM((256, 256), BF16),
            pltpu.VMEM((128, 256), BF16),
            pltpu.VMEM((2, 8, 128), F32),
            pltpu.VMEM((2, 64, 8, 128), F32),
            pltpu.VMEM((2, 8, 8, 128), F32),
            pltpu.VMEM((2, 640, 8, 128), F32),
            pltpu.VMEM((8, 16, 8192), BF16),
            pltpu.VMEM((8, 16, 8192), BF16),
            pltpu.VMEM((64, 128), BF16),
            pltpu.VMEM((64, 8, 8, 128), F32),
            pltpu.VMEM((8, 64, 8, 128), F32),
            pltpu.VMEM((8, 64, 8, 128), F32),
            pltpu.VMEM((512, 128), F32),
            pltpu.VMEM((512, 8, 128), F32),
            pltpu.VMEM((1024, 256), BF16),
            pltpu.VMEM((8, 16, 8, 128), F32),
            pltpu.VMEM((64, 8, 8, 128), F32),
            pltpu.VMEM((128, 4, 8, 128), F32),
            pltpu.SemaphoreType.DMA((6,)),
            pltpu.SemaphoreType.DMA,
            pltpu.SemaphoreType.DMA((CH,)),
            pltpu.SemaphoreType.DMA,
            pltpu.SemaphoreType.DMA((CH,)),
            pltpu.SemaphoreType.DMA,
            pltpu.SemaphoreType.DMA((SUB,)),
        ],
        compiler_params=pltpu.CompilerParams(
            collective_id=0, has_side_effects=True, vmem_limit_bytes=60 * 1024 * 1024
        ),
    )(
        station_delays, dm_index, voltages, beam_weights,
        jnp.asarray(w1), jnp.asarray(w2), jnp.asarray(small), jnp.asarray(big), jnp.asarray(inner),
    )
    out, power = pl.pallas_call(
        assemble,
        grid=(SUB,),
        out_shape=(jax.ShapeDtypeStruct((4096, 128), F32), jax.ShapeDtypeStruct((128, 128), F32)),
        in_specs=[pl.BlockSpec((256, 128), lambda s: (s, 0))],
        out_specs=(pl.BlockSpec((256, 128), lambda s: (s, 0)), pl.BlockSpec((128, 128), lambda s: (0, 0))),
        compiler_params=pltpu.CompilerParams(dimension_semantics=("arbitrary",)),
    )(moved.reshape(4096, 128))
    return out.reshape(16, 2, 32, 1, 512), power.reshape(32, 1, 512)


def solution(mesh):
    return jax.shard_map(
        shards,
        mesh=mesh,
        in_specs=(
            P("sub", None, "sta", None),
            P("sub", None, None, None),
            P("sta"),
            P("sta", None),
        ),
        out_specs=(P(None, None, None, None, ("sub", "sta")), P(None, None, ("sub", "sta"))),
        check_vma=False,
    )
```

```python
import functools

import jax
import jax.numpy as jnp
import numpy as np
from jax import lax
from jax.experimental import pallas as pl
from jax.experimental.pallas import tpu as pltpu
from jax.sharding import PartitionSpec as P

TWO_PI = 6.283185307179586
DISPERSION = 4148808000.0
DM_STEP = 10.0
BASE_FREQ = 120.0
CHANNEL_WIDTH = 0.1953125
F32 = jnp.float32
BF16 = jnp.bfloat16
N = 65536
STA = 8
SUB = 16
INV_SQRT2 = 0.7071067811865476


MESH = pl.DeviceIdType.MESH
TOP = 32767.0
CH = 4


def dft_tables():
    k = np.arange(128)
    ang = 2.0 * np.pi * ((k[:, None] * k[None, :]) % 128) / 128.0
    full = np.concatenate([np.cos(ang), np.sin(ang)], axis=1).astype(np.float32)
    hi = full.astype(jnp.bfloat16)
    lo = (full - hi.astype(np.float32)).astype(jnp.bfloat16)
    return np.concatenate([hi, hi], axis=0), lo


def twist_tables():
    at = np.arange(64)
    ka = (8 * (at % 8) + at // 8)[:, None]
    n = np.arange(1024)[None, :]
    ang = 2.0 * np.pi * (ka * n) / N
    big = np.stack([np.cos(ang), np.sin(ang)]).reshape(2, 64, 8, 128)
    kj = np.arange(8)[:, None]
    c = np.arange(128)[None, :]
    ang = 2.0 * np.pi * (kj * c) / 1024.0
    small = np.stack([np.cos(ang), np.sin(ang)])
    e = np.arange(8)
    ang = 2.0 * np.pi * (e[:, None] * e[None, :]) / 64.0
    inner = np.stack([np.cos(ang), np.sin(ang)])[..., None] * np.ones(128)
    return big.astype(np.float32), small.astype(np.float32), inner.astype(np.float32)


def sign_rows():
    row = lax.broadcasted_iota(jnp.int32, (8, 128), 0)
    return jnp.where(row < 4, 1.0, -1.0).astype(F32)


def swap(x):
    return pltpu.roll(x, 4, x.ndim - 2)


def dft8(x, sg):
    def times_j(v):
        return swap(v) * sg

    def dft4(a0, a1, a2, a3):
        t0, t1, t2, t3 = a0 + a2, a0 - a2, a1 + a3, times_j(a1 - a3)
        return t0 + t2, t1 + t3, t0 - t2, t1 - t3

    e = dft4(x[0], x[2], x[4], x[6])
    o = dft4(x[1], x[3], x[5], x[7])
    j1, j3 = times_j(o[1]), times_j(o[3])
    o = (o[0], (o[1] + j1) * INV_SQRT2, times_j(o[2]), (j3 - o[3]) * INV_SQRT2)
    return [e[k] + o[k] for k in range(4)] + [e[k] - o[k] for k in range(4)]


def cmul(x, wr, wi, sg):
    return x * wr + (swap(x) * sg) * wi


def split(x):
    hi = x.astype(BF16)
    lo = (x - hi.astype(F32)).astype(BF16)
    return hi, lo


def unpack_voltages(x_ref, xf_ref):
    def body(i, _):
        for u in range(8):
            t = i * 8 + u
            col = pl.multiple_of(t * 128, 128)
            for ri in range(2):
                xf_ref[ri, t + 128] = x_ref[0, ri, :, pl.ds(col, 128)].astype(F32)
        return 0

    lax.fori_loop(0, 64, body, 0)

    def wrap(i, _):
        for ri in range(2):
            xf_ref[ri, pl.ds(i * 8, 8)] = xf_ref[ri, pl.ds(i * 8 + 512, 8)]
        return 0

    lax.fori_loop(0, 16, wrap, 0)


def delay_setup(d_ref):
    row = lax.broadcasted_iota(jnp.int32, (8, 128), 0)
    lane = lax.broadcasted_iota(jnp.int32, (8, 128), 1)
    fine = jnp.zeros((8, 128), jnp.int32)
    starts = []
    for r in range(8):
        d = d_ref[r]
        starts.append(128 - d // 128)
        fine = jnp.where(row == r, d % 128, fine)
    return starts, [row == r for r in range(8)], (lane - fine + 128) % 128, lane >= fine


def delay_rows(setup, xf_ref, out_ref, a0):
    starts, masks, index, keep = setup

    def body(a1, _):
        t = (8 * a1 + a0) * 8
        col = pl.multiple_of((8 * a0 + a1) * 128, 128)
        done = []
        for ri in range(2):
            acc = xf_ref[ri, pl.ds(starts[0] + t - 1, 9)]
            for r in range(1, 8):
                acc = jnp.where(masks[r], xf_ref[ri, pl.ds(starts[r] + t - 1, 9)], acc)
            g = [jnp.take_along_axis(acc[u], index, axis=1) for u in range(9)]
            done.append([jnp.where(keep, g[u + 1], g[u]) for u in range(8)])
        for j in range(8):
            out_ref[j, :, pl.ds(col, 128)] = jnp.concatenate([done[0][j], done[1][j]], axis=0).astype(BF16)
        return 0

    lax.fori_loop(0, 8, body, 0)


def one_hot(shape, hit):
    row = lax.broadcasted_iota(jnp.int32, shape, 0)
    col = lax.broadcasted_iota(jnp.int32, shape, 1)
    return jnp.where(hit(row, col), 1.0, 0.0).astype(BF16)


def stacked_weights(bw_ref):
    w0, w1 = bw_ref[0, 0], bw_ref[0, 1]
    to_real = one_hot((64, 128), lambda q, c: c == (q // 8) * 16 + q % 8)
    to_imag = one_hot((64, 128), lambda q, c: c == (q // 8) * 16 + 8 + q % 8)
    dot = functools.partial(jnp.dot, preferred_element_type=F32)
    real = (dot(w0, to_real) - dot(w1, to_imag)).astype(BF16)
    imag = (dot(w1, to_real) + dot(w0, to_imag)).astype(BF16)
    rows_real = one_hot((64, 32), lambda r, b: r == (b // 4) * 8 + b % 4)
    rows_imag = one_hot((64, 32), lambda r, b: r == (b // 4) * 8 + 4 + b % 4)
    return (dot(rows_real, real) + dot(rows_imag, imag)).astype(BF16)


def beamform(w_ref, v_ref, bm_ref, part):
    w = w_ref[...]

    def body(i, _):
        first = part * 16 + i * 4
        v = v_ref[:, :, pl.ds(pl.multiple_of(first * 128, 512), 512)].reshape(128, 512)
        out = jnp.dot(w, v, preferred_element_type=F32)
        for u in range(4):
            bm_ref[first + u] = out[:, u * 128 : (u + 1) * 128].reshape(8, 8, 128)
        return 0

    lax.fori_loop(0, 4, body, 0)


def inner_pass(ref, lead, twi_ref, sg):
    def body(g, _):
        at = pl.ds(g * 2, 2)
        y = dft8([ref[8 * lead + i, at] for i in range(8)], sg)
        for k in range(8):
            v = y[k]
            if k:
                v = cmul(v, twi_ref[0, lead, pl.ds(k, 1)], twi_ref[1, lead, pl.ds(k, 1)], sg)
            ref[8 * lead + k, at] = v
        return 0

    lax.fori_loop(0, 4, body, 0, unroll=4)


def encode(values, axes):
    top = jnp.max(jnp.abs(values), axis=axes, keepdims=True)
    top = jnp.maximum(top, 1e-33)
    return jnp.round(values * (TOP / top)), top * (1.0 / TOP)


def decode(ints):
    return ints.astype(jnp.int32).astype(F32)


def outer_and_encode(bm_ref, part, sta, twb_ref, sg, q_ref, s_ref):
    for low in range(2):
        k0 = 2 * part + low
        for g in range(4):
            at = pl.ds(2 * g, 2)
            y = dft8([bm_ref[8 * i + k0, at] for i in range(8)], sg)
            out = []
            for k1 in range(8):
                k = 8 * k0 + k1
                out.append(cmul(y[k1], twb_ref[0, k, pl.ds(sta, 1)], twb_ref[1, k, pl.ds(sta, 1)], sg))
            q, scale = encode(jnp.stack(out, axis=1), (1, 2))
            q_ref[at, pl.ds(4 * k0, 4)] = q.reshape(2, 4, 16, 128).astype(jnp.int16)
            s_ref[at, part, low : low + 1] = scale.reshape(2, 1, 128)


def chirp_table(dm_ref, base_ref, h_ref):
    row = lax.broadcasted_iota(jnp.int32, (8, 128), 0)
    lane = lax.broadcasted_iota(jnp.int32, (8, 128), 1)
    centre = BASE_FREQ + CHANNEL_WIDTH * (
        jnp.zeros((8, 128), F32) + lax.axis_index("sub").astype(F32) + 0.5
    )

    def base(i, _):
        part, kj, low = i // 16, (i // 2) % 8, i % 2
        positions = 8 * row + (2 * part + low) + 64 * kj + 512 * lane
        signed_bin = jnp.where(positions < N // 2, positions, positions - N)
        offset = CHANNEL_WIDTH * signed_bin.astype(F32) / N
        base_ref[pl.ds(pl.multiple_of(i * 8, 8), 8), :] = (
            TWO_PI * DISPERSION * offset * offset / (centre * centre * (centre + offset))
        )
        return 0

    lax.fori_loop(0, 64, base, 0)
    quarter = jnp.where(row < 4, 1, 0)
    dm = jnp.zeros((8, 128), F32)
    for b in range(4):
        dm = jnp.where(row % 4 == b, DM_STEP * dm_ref[b].astype(F32), dm)
    p1 = 1.5703125
    p2 = float(np.float32(np.round((np.pi / 2 - p1) * 2.0**22) / 2.0**22))
    p3 = float(np.float32(np.pi / 2 - p1 - p2))

    def one(r):
        phase = dm * base_ref[pl.ds(r, 1), :]
        n = jnp.floor(phase * float(2.0 / np.pi) + 0.5)
        y = ((phase - n * p1) - n * p2) - n * p3
        q = n.astype(jnp.int32) + quarter
        z = y * y
        s = ((-1.9515295891e-4 * z + 8.3321608736e-3) * z - 1.6666654611e-1) * z * y + y
        c = ((2.443315711809948e-5 * z - 1.388731625493765e-3) * z + 4.166664568298827e-2) * z * z - 0.5 * z + 1.0
        v = jnp.where((q & 1) == 0, s, c)
        h_ref[r] = jnp.where((q & 2) == 0, v, -v)

    def body(i, _):
        for u in range(4):
            one(i * 4 + u)
        return 0

    lax.fori_loop(0, 128, body, 0)


def middle(p, r_ref, rs_ref, h_ref, w1_ref, w2_ref, tws_ref, twb_ref, xs_ref, gt_ref, g_ref, sg):
    for low_k0 in range(2):

        def fwd(i, _):
            m = low_k0 * 4 + i
            x = [
                decode(r_ref[j, p * 8 + m]).reshape(2, 8, 128) * rs_ref[j, p, low_k0 : low_k0 + 1] for j in range(8)
            ]
            y = dft8(x, sg)
            for kj in range(8):
                v = y[kj]
                if kj:
                    v = cmul(v, tws_ref[0, pl.ds(kj, 1)], tws_ref[1, pl.ds(kj, 1)], sg)
                hi, lo = split(v.reshape(16, 128))
                rows = pl.ds(pl.multiple_of(kj * 128 + m * 16, 16), 16)
                xs_ref[rows, 0:128] = hi
                xs_ref[rows, 128:256] = lo
            return 0

        lax.fori_loop(0, 4, fwd, 0, unroll=4)

    rows = 512

    def dot128(at, sign):
        x = xs_ref[at, :]
        pq = jnp.dot(x, w1_ref[...], preferred_element_type=F32)
        pq = pq + jnp.dot(x[:, 0:128], w2_ref[...], preferred_element_type=F32)
        return pq[:, 0:128].reshape(rows // 8, 8, 128) + swap(pq[:, 128:256].reshape(rows // 8, 8, 128)) * sign

    low = lax.broadcasted_iota(jnp.int32, (8, 128), 0) < 4

    def mid(i, _):
        at = pl.ds(pl.multiple_of(i * rows, rows), rows)
        v = dot128(at, sg)
        h = h_ref[pl.ds(p * 128 + i * (rows // 8), rows // 8)]
        hs = swap(h)
        v = v * jnp.where(low, h, hs) + swap(v) * jnp.where(low, -hs, h)
        hi, lo = split(v.reshape(rows, 128))
        xs_ref[at, 0:128] = hi
        xs_ref[at, 128:256] = lo
        return 0

    lax.fori_loop(0, 1024 // rows, mid, 0)

    def back(i, _):
        v = dot128(pl.ds(pl.multiple_of(i * rows, rows), rows), -sg)
        gt_ref[pl.ds(i * (rows // 128), rows // 128)] = v.reshape(rows // 128, 16, 8, 128)
        return 0

    lax.fori_loop(0, 1024 // rows, back, 0)

    def inv8(i, _):
        at = pl.ds(i * 2, 2)
        x = []
        for kj in range(8):
            v = gt_ref[kj, at]
            if kj:
                v = cmul(v, tws_ref[0, pl.ds(kj, 1)], tws_ref[1, pl.ds(kj, 1)], -sg)
            x.append(v)
        y = dft8(x, -sg)
        here = pl.ds(p * 16 + i * 2, 2)
        for j in range(8):
            g_ref[here, j] = cmul(y[j], twb_ref[0, here, pl.ds(j, 1)], twb_ref[1, here, pl.ds(j, 1)], -sg)
        return 0

    lax.fori_loop(0, 8, inv8, 0, unroll=4)


def kernel(
    d_ref, dm_ref, x_hbm, bw_ref, w1_hbm, w2_hbm, tws_hbm, twb_hbm, twi_hbm,
    recv3, rscale3,
    x_ref, w1_ref, w2_ref, tws_ref, twb_ref, twi_ref,
    xf_ref, send1, recv1, w_ref, bm_ref, send2, scale2, recv2, rscale2, base_ref, h_ref, xs_ref, gt_ref, g_ref, send3, scale3,
    load_sem, col_sem, sem1, rsem1, sem2, rsem2, ssem2, rssem2, sem3, rsem3, ssem3, rssem3,
):
    sub, sta = lax.axis_index("sub"), lax.axis_index("sta")
    me = sub * STA + sta

    x_load = pltpu.make_async_copy(x_hbm, x_ref, load_sem.at[0])
    x_load.start()
    tables = [
        pltpu.make_async_copy(a, b, load_sem.at[1 + i])
        for i, (a, b) in enumerate(
            [(w1_hbm, w1_ref), (w2_hbm, w2_ref), (tws_hbm, tws_ref), (twb_hbm, twb_ref), (twi_hbm, twi_ref)]
        )
    ]
    for t in tables:
        t.start()

    barrier = pltpu.get_barrier_semaphore()

    for i in range(1, STA):
        pl.semaphore_signal(barrier, inc=1, device_id={"sub": sub, "sta": (sta + i) % STA}, device_id_type=MESH)
    for i in range(1, SUB):
        pl.semaphore_signal(barrier, inc=1, device_id={"sub": (sub + i) % SUB, "sta": sta}, device_id_type=MESH)
    x_load.wait()
    unpack_voltages(x_ref, xf_ref)
    setup = delay_setup(d_ref)

    for part in range(CH):
        delay_rows(setup, xf_ref, send1, 2 * part)
        delay_rows(setup, xf_ref, send1, 2 * part + 1)
        if part == 0:
            pl.semaphore_wait(barrier, SUB + STA - 2)
            for i in range(1, STA):
                pl.semaphore_signal(
                    col_sem, inc=1, device_id={"sub": sub, "sta": (sta + i) % STA}, device_id_type=MESH
                )
        cols = pl.ds(part * 2048, 2048)

        def go1(i, _):
            d = (sta + i) % STA
            pltpu.make_async_remote_copy(
                src_ref=send1.at[d, :, cols],
                dst_ref=recv1.at[sta, :, cols],
                send_sem=sem1,
                recv_sem=rsem1.at[part],
                device_id={"sub": sub, "sta": d},
                device_id_type=MESH,
            ).start()
            return 0

        lax.fori_loop(1, STA, go1, 0)
        pltpu.make_async_copy(send1.at[sta, :, cols], recv1.at[sta, :, cols], rsem1.at[part]).start()

    w_ref[...] = stacked_weights(bw_ref)
    chirp_table(dm_ref, base_ref, h_ref)
    for t in tables:
        t.wait()
    sg = sign_rows()

    for part in range(CH):
        cols = pl.ds(part * 2048, 2048)
        pltpu.make_async_copy(recv1.at[:, :, cols], recv1.at[:, :, cols], rsem1.at[part]).wait()
        beamform(w_ref, recv1, bm_ref, part)
        inner_pass(bm_ref, 2 * part, twi_ref, sg)
        inner_pass(bm_ref, 2 * part + 1, twi_ref, sg)

    for part in range(CH):
        outer_and_encode(bm_ref, part, sta, twb_ref, sg, send2, scale2)
        rows = pl.ds(part * 8, 8)

        def go2(i, _):
            d = (sta + i) % STA
            pltpu.make_async_remote_copy(
                src_ref=scale2.at[d, part],
                dst_ref=rscale2.at[sta, part],
                send_sem=ssem2,
                recv_sem=rssem2.at[part],
                device_id={"sub": sub, "sta": d},
                device_id_type=MESH,
            ).start()
            pltpu.make_async_remote_copy(
                src_ref=send2.at[d, rows],
                dst_ref=recv2.at[sta, rows],
                send_sem=sem2,
                recv_sem=rsem2.at[part],
                device_id={"sub": sub, "sta": d},
                device_id_type=MESH,
            ).start()
            return 0

        lax.fori_loop(1, STA, go2, 0)
        pltpu.make_async_copy(scale2.at[sta, part], rscale2.at[sta, part], rssem2.at[part]).start()
        pltpu.make_async_copy(send2.at[sta, rows], recv2.at[sta, rows], rsem2.at[part]).start()

    for part in range(CH):
        rows = pl.ds(part * 8, 8)
        pltpu.make_async_copy(rscale2.at[:, part], rscale2.at[:, part], rssem2.at[part]).wait()
        pltpu.make_async_copy(recv2.at[:, rows], recv2.at[:, rows], rsem2.at[part]).wait()
        middle(part, recv2, rscale2, h_ref, w1_ref, w2_ref, tws_ref, twb_ref, xs_ref, gt_ref, g_ref, sg)
        inner_pass(g_ref, 2 * part, twi_ref, -sg)
        inner_pass(g_ref, 2 * part + 1, twi_ref, -sg)

    pl.semaphore_wait(col_sem, STA - 1)

    def group(i, _):
        a0 = (sta + i) % 8
        for jh in range(2):
            y = dft8([g_ref[8 * k0 + a0, pl.ds(4 * jh, 4)] for k0 in range(8)], -sg)
            for a1 in range(8):
                d = 16 * a1 + 2 * a0 + jh
                q, scale = encode(y[a1], (0, 1))
                send3[d] = q.reshape(2, 16, 128).astype(jnp.int16)
                scale3[d] = scale.reshape(1, 128) * (1.0 / N)

        def go3(n, _):
            d = (16 * (n // 2 + sub // 2) + 2 * a0 + n % 2) % (SUB * STA)

            @pl.when(d != me)
            def _():
                pltpu.make_async_remote_copy(
                    src_ref=scale3.at[d],
                    dst_ref=rscale3.at[me],
                    send_sem=ssem3,
                    recv_sem=rssem3.at[sub],
                    device_id={"sub": d // STA, "sta": d % STA},
                    device_id_type=MESH,
                ).start()
                pltpu.make_async_remote_copy(
                    src_ref=send3.at[d],
                    dst_ref=recv3.at[me],
                    send_sem=sem3,
                    recv_sem=rsem3.at[sub],
                    device_id={"sub": d // STA, "sta": d % STA},
                    device_id_type=MESH,
                ).start()

            @pl.when(d == me)
            def _():
                pltpu.make_async_copy(scale3.at[me], rscale3.at[me], rssem3.at[sub]).start()
                pltpu.make_async_copy(send3.at[me], recv3.at[me], rsem3.at[sub]).start()

            return 0

        lax.fori_loop(0, 16, go3, 0)
        return 0

    lax.fori_loop(0, 8, group, 0)

    for s in range(SUB):
        block = recv3.at[pl.ds(s * STA, STA)]
        pltpu.make_async_copy(block, block, rsem3.at[s]).wait()
        block = rscale3.at[pl.ds(s * STA, STA)]
        pltpu.make_async_copy(block, block, rssem3.at[s]).wait()
    others = pl.ds(0, STA - 1)
    pltpu.make_async_copy(send1.at[others], send1.at[others], sem1).wait()
    pltpu.make_async_copy(send2.at[others], send2.at[others], sem2).wait()
    pltpu.make_async_copy(scale2.at[others], scale2.at[others], ssem2).wait()
    others = pl.ds(0, SUB * STA - 1)
    pltpu.make_async_copy(send3.at[others], send3.at[others], sem3).wait()
    pltpu.make_async_copy(scale3.at[others], scale3.at[others], ssem3).wait()


def assemble(q_hbm, s_ref, out_hbm, int_ref, q_ref, out_ref, acc_ref, in_sem, out_sem):
    step = 4 * STA
    loads = []
    for i in range(4):
        part = pl.ds(i * step, step)
        loads.append(pltpu.make_async_copy(q_hbm.at[part], q_ref.at[part], in_sem.at[i]))
        loads[-1].start()
    acc_ref[...] = jnp.zeros_like(acc_ref)

    def one(s, _):
        for sta in range(STA):
            src = s * STA + sta
            v = decode(q_ref[src].reshape(32, 128)).reshape(4, 8, 128) * s_ref[src]
            acc_ref[sta] += v * v
            for j4 in range(4):
                for ri in range(2):
                    first = s * 256 + (ri * 128 + sta * 16 + j4)
                    out_ref[pl.ds(first, 4, stride=4), :] = v[j4, 4 * ri : 4 * ri + 4]
        rows = pl.ds(pl.multiple_of(s * 256, 256), 256)
        pltpu.make_async_copy(out_ref.at[rows], out_hbm.at[rows], out_sem).start()
        return 0

    for i in range(4):
        loads[i].wait()
        lax.fori_loop(4 * i, 4 * i + 4, one, 0)
    for sta in range(STA):
        for j4 in range(4):
            v = acc_ref[sta, j4]
            v = (v + swap(v)) * (1.0 / SUB)
            int_ref[pl.ds(sta * 16 + j4, 4, stride=4), :] = v[0:4]
    pltpu.make_async_copy(out_ref, out_hbm, out_sem).wait()


VM = pl.BlockSpec(memory_space=pltpu.VMEM)
SM = pl.BlockSpec(memory_space=pltpu.SMEM)
ANY = pl.BlockSpec(memory_space=pl.ANY)


def shards(voltages, beam_weights, station_delays, dm_index):
    w1, w2 = dft_tables()
    big, small, inner = twist_tables()
    moved, scales = pl.pallas_call(
        kernel,
        out_shape=(
            jax.ShapeDtypeStruct((128, 2, 16, 128), jnp.int16),
            jax.ShapeDtypeStruct((128, 1, 128), F32),
        ),
        in_specs=[SM, SM, ANY, VM, ANY, ANY, ANY, ANY, ANY],
        out_specs=(ANY, ANY),
        scratch_shapes=[
            pltpu.VMEM((1, 2, 8, N), BF16),
            pltpu.VMEM((256, 256), BF16),
            pltpu.VMEM((128, 256), BF16),
            pltpu.VMEM((2, 8, 128), F32),
            pltpu.VMEM((2, 64, 8, 128), F32),
            pltpu.VMEM((2, 8, 8, 128), F32),
            pltpu.VMEM((2, 640, 8, 128), F32),
            pltpu.VMEM((8, 16, 8192), BF16),
            pltpu.VMEM((8, 16, 8192), BF16),
            pltpu.VMEM((64, 128), BF16),
            pltpu.VMEM((64, 8, 8, 128), F32),
            pltpu.VMEM((8, 32, 16, 128), jnp.int16),
            pltpu.VMEM((8, CH, 2, 128), F32),
            pltpu.VMEM((8, 32, 16, 128), jnp.int16),
            pltpu.VMEM((8, CH, 2, 128), F32),
            pltpu.VMEM((512, 128), F32),
            pltpu.VMEM((512, 8, 128), F32),
            pltpu.VMEM((1024, 256), BF16),
            pltpu.VMEM((8, 16, 8, 128), F32),
            pltpu.VMEM((64, 8, 8, 128), F32),
            pltpu.VMEM((128, 2, 16, 128), jnp.int16),
            pltpu.VMEM((128, 1, 128), F32),
            pltpu.SemaphoreType.DMA((6,)),
            pltpu.SemaphoreType.REGULAR,
            pltpu.SemaphoreType.DMA,
            pltpu.SemaphoreType.DMA((CH,)),
            pltpu.SemaphoreType.DMA,
            pltpu.SemaphoreType.DMA((CH,)),
            pltpu.SemaphoreType.DMA,
            pltpu.SemaphoreType.DMA((CH,)),
            pltpu.SemaphoreType.DMA,
            pltpu.SemaphoreType.DMA((SUB,)),
            pltpu.SemaphoreType.DMA,
            pltpu.SemaphoreType.DMA((SUB,)),
        ],
        compiler_params=pltpu.CompilerParams(
            collective_id=0, has_side_effects=True, vmem_limit_bytes=60 * 1024 * 1024
        ),
    )(
        station_delays, dm_index.reshape(4), voltages, beam_weights,
        jnp.asarray(w1), jnp.asarray(w2), jnp.asarray(small), jnp.asarray(big), jnp.asarray(inner),
    )
    out, power = pl.pallas_call(
        assemble,
        out_shape=(jax.ShapeDtypeStruct((4096, 128), F32), jax.ShapeDtypeStruct((128, 128), F32)),
        in_specs=[ANY, VM],
        out_specs=(ANY, VM),
        scratch_shapes=[
            pltpu.VMEM((128, 2, 16, 128), jnp.int16),
            pltpu.VMEM((4096, 128), F32),
            pltpu.VMEM((STA, 4, 8, 128), F32),
            pltpu.SemaphoreType.DMA((4,)),
            pltpu.SemaphoreType.DMA,
        ],
    )(moved, scales)
    return out.reshape(16, 2, 32, 1, 512), power.reshape(32, 1, 512)


def solution(mesh):
    return jax.shard_map(
        shards,
        mesh=mesh,
        in_specs=(
            P("sub", None, "sta", None),
            P("sub", None, None, None),
            P("sta"),
            P("sta", None),
        ),
        out_specs=(P(None, None, None, None, ("sub", "sta")), P(None, None, ("sub", "sta"))),
        check_vma=False,
    )
```

```python
import functools

import jax
import jax.numpy as jnp
import numpy as np
from jax import lax
from jax.experimental import pallas as pl
from jax.experimental.pallas import tpu as pltpu
from jax.sharding import PartitionSpec as P

TWO_PI = 6.283185307179586
DISPERSION = 4148808000.0
DM_STEP = 10.0
BASE_FREQ = 120.0
CHANNEL_WIDTH = 0.1953125
F32 = jnp.float32
BF16 = jnp.bfloat16
N = 65536
STA = 8
SUB = 16
INV_SQRT2 = 0.7071067811865476


MESH = pl.DeviceIdType.MESH
TOP = 32767.0
CH = 8
LOADS = 4


def dft_tables():
    k = np.arange(128)
    ang = 2.0 * np.pi * ((k[:, None] * k[None, :]) % 128) / 128.0
    full = np.concatenate([np.cos(ang), np.sin(ang)], axis=1).astype(np.float32)
    hi = full.astype(jnp.bfloat16)
    lo = (full - hi.astype(np.float32)).astype(jnp.bfloat16)
    return np.concatenate([hi, hi], axis=0), lo


def twist_tables():
    at = np.arange(64)
    ka = (8 * (at % 8) + at // 8)[:, None]
    n = np.arange(1024)[None, :]
    ang = 2.0 * np.pi * (ka * n) / N
    big = np.stack([np.cos(ang), np.sin(ang)]).reshape(2, 64, 8, 128)
    kj = np.arange(8)[:, None]
    c = np.arange(128)[None, :]
    ang = 2.0 * np.pi * (kj * c) / 1024.0
    small = np.stack([np.cos(ang), np.sin(ang)])
    e = np.arange(8)
    ang = 2.0 * np.pi * (e[:, None] * e[None, :]) / 64.0
    inner = np.stack([np.cos(ang), np.sin(ang)])[..., None] * np.ones(128)
    return big.astype(np.float32), small.astype(np.float32), inner.astype(np.float32)


def sign_rows():
    row = lax.broadcasted_iota(jnp.int32, (8, 128), 0)
    return jnp.where(row < 4, 1.0, -1.0).astype(F32)


def swap(x):
    return pltpu.roll(x, 4, x.ndim - 2)


def dft8(x, sg):
    def times_j(v):
        return swap(v) * sg

    def dft4(a0, a1, a2, a3):
        t0, t1, t2, t3 = a0 + a2, a0 - a2, a1 + a3, times_j(a1 - a3)
        return t0 + t2, t1 + t3, t0 - t2, t1 - t3

    e = dft4(x[0], x[2], x[4], x[6])
    o = dft4(x[1], x[3], x[5], x[7])
    j1, j3 = times_j(o[1]), times_j(o[3])
    o = (o[0], (o[1] + j1) * INV_SQRT2, times_j(o[2]), (j3 - o[3]) * INV_SQRT2)
    return [e[k] + o[k] for k in range(4)] + [e[k] - o[k] for k in range(4)]


def cmul(x, wr, wi, sg):
    return x * wr + (swap(x) * sg) * wi


def split(x):
    hi = x.astype(BF16)
    lo = (x - hi.astype(F32)).astype(BF16)
    return hi, lo


def unpack_voltages(x_ref, xf_ref, piece):
    per = 512 // LOADS

    def body(i, _):
        for u in range(8):
            t = piece * per + i * 8 + u
            col = pl.multiple_of(t * 128, 128)
            for ri in range(2):
                xf_ref[ri, t + 128] = x_ref[0, ri, :, pl.ds(col, 128)].astype(F32)
        return 0

    lax.fori_loop(0, per // 8, body, 0)


def wrap_voltages(xf_ref):
    def wrap(i, _):
        for ri in range(2):
            xf_ref[ri, pl.ds(i * 8, 8)] = xf_ref[ri, pl.ds(i * 8 + 512, 8)]
        return 0

    lax.fori_loop(0, 16, wrap, 0, unroll=4)


def delay_setup(d_ref):
    row = lax.broadcasted_iota(jnp.int32, (8, 128), 0)
    lane = lax.broadcasted_iota(jnp.int32, (8, 128), 1)
    fine = jnp.zeros((8, 128), jnp.int32)
    starts = []
    for r in range(8):
        d = d_ref[r]
        starts.append(128 - d // 128)
        fine = jnp.where(row == r, d % 128, fine)
    return starts, [row == r for r in range(8)], (lane - fine + 128) % 128, lane >= fine


def delay_rows(setup, xf_ref, out_ref, a0):
    starts, masks, index, keep = setup

    def body(a1, _):
        t = (8 * a1 + a0) * 8
        col = pl.multiple_of((8 * a0 + a1) * 128, 128)
        done = []
        for ri in range(2):
            acc = xf_ref[ri, pl.ds(starts[0] + t - 1, 9)]
            for r in range(1, 8):
                acc = jnp.where(masks[r], xf_ref[ri, pl.ds(starts[r] + t - 1, 9)], acc)
            g = [jnp.take_along_axis(acc[u], index, axis=1) for u in range(9)]
            done.append([jnp.where(keep, g[u + 1], g[u]) for u in range(8)])
        for j in range(8):
            out_ref[j, :, pl.ds(col, 128)] = jnp.concatenate([done[0][j], done[1][j]], axis=0).astype(BF16)
        return 0

    lax.fori_loop(0, 8, body, 0, unroll=2)


def one_hot(shape, hit):
    row = lax.broadcasted_iota(jnp.int32, shape, 0)
    col = lax.broadcasted_iota(jnp.int32, shape, 1)
    return jnp.where(hit(row, col), 1.0, 0.0).astype(BF16)


def stacked_weights(bw_ref):
    w0, w1 = bw_ref[0, 0], bw_ref[0, 1]
    to_real = one_hot((64, 128), lambda q, c: c == (q // 8) * 16 + q % 8)
    to_imag = one_hot((64, 128), lambda q, c: c == (q // 8) * 16 + 8 + q % 8)
    dot = functools.partial(jnp.dot, preferred_element_type=F32)
    real = (dot(w0, to_real) - dot(w1, to_imag)).astype(BF16)
    imag = (dot(w1, to_real) + dot(w0, to_imag)).astype(BF16)
    rows_real = one_hot((64, 32), lambda r, b: r == (b // 4) * 8 + b % 4)
    rows_imag = one_hot((64, 32), lambda r, b: r == (b // 4) * 8 + 4 + b % 4)
    return (dot(rows_real, real) + dot(rows_imag, imag)).astype(BF16)


def beamform(w_ref, v_ref, bm_ref, part):
    w = w_ref[...]

    def body(i, _):
        first = part * 8 + i * 4
        v = v_ref[:, :, pl.ds(pl.multiple_of(first * 128, 512), 512)].reshape(128, 512)
        out = jnp.dot(w, v, preferred_element_type=F32)
        for u in range(4):
            bm_ref[first + u] = out[:, u * 128 : (u + 1) * 128].reshape(8, 8, 128)
        return 0

    lax.fori_loop(0, 2, body, 0, unroll=2)


def inner_pass(ref, lead, twi_ref, sg):
    def body(g, _):
        at = pl.ds(g * 2, 2)
        y = dft8([ref[8 * lead + i, at] for i in range(8)], sg)
        for k in range(8):
            v = y[k]
            if k:
                v = cmul(v, twi_ref[0, lead, pl.ds(k, 1)], twi_ref[1, lead, pl.ds(k, 1)], sg)
            ref[8 * lead + k, at] = v
        return 0

    lax.fori_loop(0, 4, body, 0, unroll=4)


def encode(values, axes):
    top = jnp.max(jnp.abs(values), axis=axes, keepdims=True)
    top = jnp.maximum(top, 1e-33)
    return jnp.round(values * (TOP / top)), top * (1.0 / TOP)


def decode(ints):
    return ints.astype(jnp.int32).astype(F32)


def outer_and_encode(bm_ref, k0, sta, twb_ref, sg, q_ref, s_ref):
    for g in range(4):
        at = pl.ds(2 * g, 2)
        y = dft8([bm_ref[8 * i + k0, at] for i in range(8)], sg)
        out = []
        for k1 in range(8):
            k = 8 * k0 + k1
            out.append(cmul(y[k1], twb_ref[0, k, pl.ds(sta, 1)], twb_ref[1, k, pl.ds(sta, 1)], sg))
        q, scale = encode(jnp.stack(out, axis=1), (1, 2))
        q_ref[at, pl.ds(4 * k0, 4)] = q.reshape(2, 4, 16, 128).astype(jnp.int16)
        s_ref[at, k0] = scale.reshape(2, 1, 128)


def chirp_table(dm_ref, base_ref, h_ref):
    row = lax.broadcasted_iota(jnp.int32, (8, 128), 0)
    lane = lax.broadcasted_iota(jnp.int32, (8, 128), 1)
    centre = BASE_FREQ + CHANNEL_WIDTH * (
        jnp.zeros((8, 128), F32) + lax.axis_index("sub").astype(F32) + 0.5
    )

    def base(i, _):
        k0, kj = i // 8, i % 8
        positions = 8 * row + k0 + 64 * kj + 512 * lane
        signed_bin = jnp.where(positions < N // 2, positions, positions - N)
        offset = CHANNEL_WIDTH * signed_bin.astype(F32) / N
        base_ref[pl.ds(pl.multiple_of(i * 8, 8), 8), :] = (
            TWO_PI * DISPERSION * offset * offset / (centre * centre * (centre + offset))
        )
        return 0

    lax.fori_loop(0, 64, base, 0)
    quarter = jnp.where(row < 4, 1, 0)
    dm = jnp.zeros((8, 128), F32)
    for b in range(4):
        dm = jnp.where(row % 4 == b, DM_STEP * dm_ref[b].astype(F32), dm)
    p1 = 1.5703125
    p2 = float(np.float32(np.round((np.pi / 2 - p1) * 2.0**22) / 2.0**22))
    p3 = float(np.float32(np.pi / 2 - p1 - p2))

    def one(r):
        phase = dm * base_ref[pl.ds(r, 1), :]
        n = jnp.floor(phase * float(2.0 / np.pi) + 0.5)
        y = ((phase - n * p1) - n * p2) - n * p3
        q = n.astype(jnp.int32) + quarter
        z = y * y
        s = ((-1.9515295891e-4 * z + 8.3321608736e-3) * z - 1.6666654611e-1) * z * y + y
        c = ((2.443315711809948e-5 * z - 1.388731625493765e-3) * z + 4.166664568298827e-2) * z * z - 0.5 * z + 1.0
        v = jnp.where((q & 1) == 0, s, c)
        h_ref[r] = jnp.where((q & 2) == 0, v, -v)

    def body(i, _):
        for u in range(4):
            one(i * 4 + u)
        return 0

    lax.fori_loop(0, 128, body, 0)


def middle(k0, r_ref, rs_ref, h_ref, w1_ref, w2_ref, tws_ref, twb_ref, xs_ref, gt_ref, g_ref, sg):
    for m in range(4):
        x = [decode(r_ref[j, k0 * 4 + m]).reshape(2, 8, 128) * rs_ref[j, k0] for j in range(8)]
        y = dft8(x, sg)
        for kj in range(8):
            v = y[kj]
            if kj:
                v = cmul(v, tws_ref[0, pl.ds(kj, 1)], tws_ref[1, pl.ds(kj, 1)], sg)
            hi, lo = split(v.reshape(16, 128))
            at = kj * 64 + m * 16
            xs_ref[at : at + 16, 0:128] = hi
            xs_ref[at : at + 16, 128:256] = lo

    def dot128(sign):
        x = xs_ref[...]
        pq = jnp.dot(x, w1_ref[...], preferred_element_type=F32)
        pq = pq + jnp.dot(x[:, 0:128], w2_ref[...], preferred_element_type=F32)
        return pq[:, 0:128].reshape(64, 8, 128) + swap(pq[:, 128:256].reshape(64, 8, 128)) * sign

    low = lax.broadcasted_iota(jnp.int32, (8, 128), 0) < 4
    v = dot128(sg)
    h = h_ref[pl.ds(k0 * 64, 64)]
    hs = swap(h)
    v = v * jnp.where(low, h, hs) + swap(v) * jnp.where(low, -hs, h)
    hi, lo = split(v.reshape(512, 128))
    xs_ref[:, 0:128] = hi
    xs_ref[:, 128:256] = lo
    gt_ref[...] = dot128(-sg).reshape(8, 8, 8, 128)

    for i in range(4):
        x = []
        for kj in range(8):
            v = gt_ref[kj, 2 * i : 2 * i + 2]
            if kj:
                v = cmul(v, tws_ref[0, pl.ds(kj, 1)], tws_ref[1, pl.ds(kj, 1)], -sg)
            x.append(v)
        y = dft8(x, -sg)
        here = pl.ds(k0 * 8 + i * 2, 2)
        for j in range(8):
            g_ref[here, j] = cmul(y[j], twb_ref[0, here, pl.ds(j, 1)], twb_ref[1, here, pl.ds(j, 1)], -sg)


PLACES = ((0, 2, 1), (1, 0, 0), (0, 1, 0), (1, 3, 1), (0, 0, 1), (1, 2, 0), (0, 3, 0), (1, 1, 1), (0, 2, 0), (1, 0, 1), (0, 1, 1), (1, 3, 0), (0, 3, 1), (1, 1, 0), (1, 2, 1), (0, 0, 0))


def kernel(
    d_hbm, dm_hbm, x_hbm, bw_hbm, w1_hbm, w2_hbm, tws_hbm, twb_hbm, twi_hbm,
    recv3, rscale3,
    d_ref, dm_ref, bw_ref, x_ref, w1_ref, w2_ref, tws_ref, twb_ref, twi_ref,
    xf_ref, send1, recv1, w_ref, bm_ref, send2, scale2, recv2, rscale2, base_ref, h_ref, xs_ref, gt_ref, g_ref,
    send3, scale3,
    load_sem, col_sem, sem1, rsem1, sem2, rsem2, ssem2, rssem2, sem3, rsem3, ssem3, rssem3,
):
    sub, sta = lax.axis_index("sub"), lax.axis_index("sta")
    me = sub * STA + sta

    x_loads = []
    for i in range(LOADS):
        cols = pl.ds(i * (N // LOADS), N // LOADS)
        x_loads.append(pltpu.make_async_copy(x_hbm.at[:, :, :, cols], x_ref.at[:, :, :, cols], load_sem.at[i]))
    tables = [
        pltpu.make_async_copy(a, b, load_sem.at[LOADS + i])
        for i, (a, b) in enumerate(
            [
                (d_hbm, d_ref), (dm_hbm, dm_ref), (bw_hbm, bw_ref), (w1_hbm, w1_ref), (w2_hbm, w2_ref),
                (tws_hbm, tws_ref), (twb_hbm, twb_ref), (twi_hbm, twi_ref),
            ]
        )
    ]
    for t in tables[:1] + x_loads + tables[1:]:
        t.start()

    barrier = pltpu.get_barrier_semaphore()
    for i in range(1, STA):
        pl.semaphore_signal(barrier, inc=1, device_id={"sub": sub, "sta": (sta + i) % STA}, device_id_type=MESH)
    for i in range(1, SUB):
        pl.semaphore_signal(barrier, inc=1, device_id={"sub": (sub + i) % SUB, "sta": sta}, device_id_type=MESH)
    for i in range(LOADS):
        x_loads[i].wait()
        unpack_voltages(x_ref, xf_ref, i)
    wrap_voltages(xf_ref)
    tables[0].wait()
    setup = delay_setup(d_ref)

    def first(part):
        cols = pl.ds(pl.multiple_of(part * 1024, 1024), 1024)
        for i in range(1, STA):
            d = (sta + i) % STA
            pltpu.make_async_remote_copy(
                src_ref=send1.at[d, :, cols],
                dst_ref=recv1.at[sta, :, cols],
                send_sem=sem1,
                recv_sem=rsem1.at[part],
                device_id={"sub": sub, "sta": d},
                device_id_type=MESH,
            ).start()
        pltpu.make_async_copy(send1.at[sta, :, cols], recv1.at[sta, :, cols], rsem1.at[part]).start()

    delay_rows(setup, xf_ref, send1, 0)
    pl.semaphore_wait(barrier, SUB + STA - 2)
    first(0)
    for i in range(1, STA):
        pl.semaphore_signal(col_sem, inc=1, device_id={"sub": sub, "sta": (sta + i) % STA}, device_id_type=MESH)

    def more(part, _):
        delay_rows(setup, xf_ref, send1, part)
        first(part)
        return 0

    lax.fori_loop(1, CH, more, 0)

    for t in tables[1:]:
        t.wait()
    w_ref[...] = stacked_weights(bw_ref)
    chirp_table(dm_ref, base_ref, h_ref)
    sg = sign_rows()

    def beams(part, _):
        cols = pl.ds(pl.multiple_of(part * 1024, 1024), 1024)
        pltpu.make_async_copy(recv1.at[:, :, cols], recv1.at[:, :, cols], rsem1.at[part]).wait()
        beamform(w_ref, recv1, bm_ref, part)
        inner_pass(bm_ref, part, twi_ref, sg)
        return 0

    lax.fori_loop(0, CH, beams, 0)

    def second(part, _):
        outer_and_encode(bm_ref, part, sta, twb_ref, sg, send2, scale2)
        rows = pl.ds(part * 4, 4)
        for i in range(1, STA):
            d = (sta + i) % STA
            pltpu.make_async_remote_copy(
                src_ref=scale2.at[d, part],
                dst_ref=rscale2.at[sta, part],
                send_sem=ssem2,
                recv_sem=rssem2.at[part],
                device_id={"sub": sub, "sta": d},
                device_id_type=MESH,
            ).start()
            pltpu.make_async_remote_copy(
                src_ref=send2.at[d, rows],
                dst_ref=recv2.at[sta, rows],
                send_sem=sem2,
                recv_sem=rsem2.at[part],
                device_id={"sub": sub, "sta": d},
                device_id_type=MESH,
            ).start()
        pltpu.make_async_copy(scale2.at[sta, part], rscale2.at[sta, part], rssem2.at[part]).start()
        pltpu.make_async_copy(send2.at[sta, rows], recv2.at[sta, rows], rsem2.at[part]).start()
        return 0

    lax.fori_loop(0, CH, second, 0)

    def spectra(part, _):
        rows = pl.ds(part * 4, 4)
        pltpu.make_async_copy(rscale2.at[:, part], rscale2.at[:, part], rssem2.at[part]).wait()
        pltpu.make_async_copy(recv2.at[:, rows], recv2.at[:, rows], rsem2.at[part]).wait()
        middle(part, recv2, rscale2, h_ref, w1_ref, w2_ref, tws_ref, twb_ref, xs_ref, gt_ref, g_ref, sg)
        inner_pass(g_ref, part, twi_ref, -sg)
        return 0

    lax.fori_loop(0, CH, spectra, 0)

    pl.semaphore_wait(col_sem, STA - 1)
    x_hi, z, core = sub // 8, (sub // 2) % 4, sub % 2
    x_lo, yh, jh_own = sta // 4, (sta // 2) % 2, sta % 2

    def group(i, _):
        a0 = 4 * ((core + 1 - (i // 4) % 2) % 2) + 2 * ((x_lo + 1 - (i // 2) % 2) % 2) + (yh + 1 - i % 2) % 2
        for jh in range(2):
            y = dft8([g_ref[8 * k0 + a0, pl.ds(4 * jh, 4)] for k0 in range(8)], -sg)
            for a1 in range(8):
                d = 16 * a1 + 2 * a0 + jh
                q, scale = encode(y[a1], (0, 1))
                send3[d] = q.reshape(2, 16, 128).astype(jnp.int16)
                scale3[d] = scale.reshape(1, 128) * (1.0 / N)

        for dx, dz, dj in PLACES:
            d = 64 * ((x_hi + dx) % 2) + 16 * ((z + dz) % 4) + 2 * a0 + (jh_own + dj) % 2

            def go():
                pltpu.make_async_remote_copy(
                    src_ref=scale3.at[d],
                    dst_ref=rscale3.at[me],
                    send_sem=ssem3,
                    recv_sem=rssem3.at[sub],
                    device_id={"sub": d // STA, "sta": d % STA},
                    device_id_type=MESH,
                ).start()
                pltpu.make_async_remote_copy(
                    src_ref=send3.at[d],
                    dst_ref=recv3.at[me],
                    send_sem=sem3,
                    recv_sem=rsem3.at[sub],
                    device_id={"sub": d // STA, "sta": d % STA},
                    device_id_type=MESH,
                ).start()

            if dx or dz or dj:
                go()
            else:
                pl.when(d != me)(go)

                @pl.when(d == me)
                def _():
                    pltpu.make_async_copy(scale3.at[me], rscale3.at[me], rssem3.at[sub]).start()
                    pltpu.make_async_copy(send3.at[me], recv3.at[me], rsem3.at[sub]).start()

        return 0

    lax.fori_loop(0, 8, group, 0)

    for s in range(SUB):
        block = recv3.at[pl.ds(s * STA, STA)]
        pltpu.make_async_copy(block, block, rsem3.at[s]).wait()
        block = rscale3.at[pl.ds(s * STA, STA)]
        pltpu.make_async_copy(block, block, rssem3.at[s]).wait()
    others = pl.ds(0, STA - 1)
    pltpu.make_async_copy(send1.at[others], send1.at[others], sem1).wait()
    pltpu.make_async_copy(send2.at[others], send2.at[others], sem2).wait()
    pltpu.make_async_copy(scale2.at[others], scale2.at[others], ssem2).wait()
    others = pl.ds(0, SUB * STA - 1)
    pltpu.make_async_copy(send3.at[others], send3.at[others], sem3).wait()
    pltpu.make_async_copy(scale3.at[others], scale3.at[others], ssem3).wait()


def assemble(q_ref, s_ref, out_hbm, int_ref, out_ref, acc_ref, out_sem):
    acc_ref[...] = jnp.zeros_like(acc_ref)

    def one(s, _):
        for sta in range(STA):
            src = s * STA + sta
            v = decode(q_ref[src].reshape(32, 128)).reshape(4, 8, 128) * s_ref[src]
            acc_ref[sta] += v * v
            for j4 in range(4):
                for ri in range(2):
                    first = s * 256 + (ri * 128 + sta * 16 + j4)
                    out_ref[pl.ds(first, 4, stride=4), :] = v[j4, 4 * ri : 4 * ri + 4]
        rows = pl.ds(pl.multiple_of(s * 256, 256), 256)
        pltpu.make_async_copy(out_ref.at[rows], out_hbm.at[rows], out_sem).start()
        return 0

    lax.fori_loop(0, SUB, one, 0)
    for sta in range(STA):
        for j4 in range(4):
            v = acc_ref[sta, j4]
            v = (v + swap(v)) * (1.0 / SUB)
            int_ref[pl.ds(sta * 16 + j4, 4, stride=4), :] = v[0:4]
    pltpu.make_async_copy(out_ref, out_hbm, out_sem).wait()


VM = pl.BlockSpec(memory_space=pltpu.VMEM)
SM = pl.BlockSpec(memory_space=pltpu.SMEM)
ANY = pl.BlockSpec(memory_space=pl.ANY)
HBM = pl.BlockSpec(memory_space=pltpu.HBM)


def shards(voltages, beam_weights, station_delays, dm_index):
    w1, w2 = dft_tables()
    big, small, inner = twist_tables()
    moved, scales = pl.pallas_call(
        kernel,
        out_shape=(
            pltpu.VMEM((128, 2, 16, 128), jnp.int16),
            pltpu.VMEM((128, 1, 128), F32),
        ),
        in_specs=[HBM] * 9,
        out_specs=(ANY, ANY),
        scratch_shapes=[
            pltpu.SMEM((8,), jnp.int32),
            pltpu.SMEM((4,), jnp.int32),
            pltpu.VMEM((1, 2, 32, 64), BF16),
            pltpu.VMEM((1, 2, 8, N), BF16),
            pltpu.VMEM((256, 256), BF16),
            pltpu.VMEM((128, 256), BF16),
            pltpu.VMEM((2, 8, 128), F32),
            pltpu.VMEM((2, 64, 8, 128), F32),
            pltpu.VMEM((2, 8, 8, 128), F32),
            pltpu.VMEM((2, 640, 8, 128), F32),
            pltpu.VMEM((8, 16, 8192), BF16),
            pltpu.VMEM((8, 16, 8192), BF16),
            pltpu.VMEM((64, 128), BF16),
            pltpu.VMEM((64, 8, 8, 128), F32),
            pltpu.VMEM((8, 32, 16, 128), jnp.int16),
            pltpu.VMEM((8, CH, 1, 128), F32),
            pltpu.VMEM((8, 32, 16, 128), jnp.int16),
            pltpu.VMEM((8, CH, 1, 128), F32),
            pltpu.VMEM((512, 128), F32),
            pltpu.VMEM((512, 8, 128), F32),
            pltpu.VMEM((512, 256), BF16),
            pltpu.VMEM((8, 8, 8, 128), F32),
            pltpu.VMEM((64, 8, 8, 128), F32),
            pltpu.VMEM((128, 2, 16, 128), jnp.int16),
            pltpu.VMEM((128, 1, 128), F32),
            pltpu.SemaphoreType.DMA((LOADS + 8,)),
            pltpu.SemaphoreType.REGULAR,
            pltpu.SemaphoreType.DMA,
            pltpu.SemaphoreType.DMA((CH,)),
            pltpu.SemaphoreType.DMA,
            pltpu.SemaphoreType.DMA((CH,)),
            pltpu.SemaphoreType.DMA,
            pltpu.SemaphoreType.DMA((CH,)),
            pltpu.SemaphoreType.DMA,
            pltpu.SemaphoreType.DMA((SUB,)),
            pltpu.SemaphoreType.DMA,
            pltpu.SemaphoreType.DMA((SUB,)),
        ],
        compiler_params=pltpu.CompilerParams(
            collective_id=0, has_side_effects=True, vmem_limit_bytes=56 * 1024 * 1024
        ),
    )(
        station_delays, dm_index.reshape(4), voltages, beam_weights,
        jnp.asarray(w1), jnp.asarray(w2), jnp.asarray(small), jnp.asarray(big), jnp.asarray(inner),
    )
    out, power = pl.pallas_call(
        assemble,
        out_shape=(jax.ShapeDtypeStruct((4096, 128), F32), jax.ShapeDtypeStruct((128, 128), F32)),
        in_specs=[VM, VM],
        out_specs=(ANY, VM),
        scratch_shapes=[
            pltpu.VMEM((4096, 128), F32),
            pltpu.VMEM((STA, 4, 8, 128), F32),
            pltpu.SemaphoreType.DMA,
        ],
        compiler_params=pltpu.CompilerParams(vmem_limit_bytes=16 * 1024 * 1024),
    )(moved, scales)
    return out.reshape(16, 2, 32, 1, 512), power.reshape(32, 1, 512)


def solution(mesh):
    return jax.shard_map(
        shards,
        mesh=mesh,
        in_specs=(
            P("sub", None, "sta", None),
            P("sub", None, None, None),
            P("sta"),
            P("sta", None),
        ),
        out_specs=(P(None, None, None, None, ("sub", "sta")), P(None, None, ("sub", "sta"))),
        check_vma=False,
    )
```

```python
import functools

import jax
import jax.numpy as jnp
import numpy as np
from jax import lax
from jax.experimental import pallas as pl
from jax.experimental.pallas import tpu as pltpu
from jax.sharding import PartitionSpec as P

TWO_PI = 6.283185307179586
DISPERSION = 4148808000.0
DM_STEP = 10.0
BASE_FREQ = 120.0
CHANNEL_WIDTH = 0.1953125
F32 = jnp.float32
BF16 = jnp.bfloat16
N = 65536
STA = 8
SUB = 16
INV_SQRT2 = 0.7071067811865476


MESH = pl.DeviceIdType.MESH
TOP = 32767.0
CH = 8
LOADS = 4
HEAD_START = 10


def dft_tables():
    k = np.arange(128)
    ang = 2.0 * np.pi * ((k[:, None] * k[None, :]) % 128) / 128.0
    full = np.concatenate([np.cos(ang), np.sin(ang)], axis=1).astype(np.float32)
    hi = full.astype(jnp.bfloat16)
    lo = (full - hi.astype(np.float32)).astype(jnp.bfloat16)
    return np.concatenate([hi, hi], axis=0), lo


def twist_tables():
    at = np.arange(64)
    ka = (8 * (at % 8) + at // 8)[:, None]
    n = np.arange(1024)[None, :]
    ang = 2.0 * np.pi * (ka * n) / N
    big = np.stack([np.cos(ang), np.sin(ang)]).reshape(2, 64, 8, 128)
    kj = np.arange(8)[:, None]
    c = np.arange(128)[None, :]
    ang = 2.0 * np.pi * (kj * c) / 1024.0
    small = np.stack([np.cos(ang), np.sin(ang)])
    e = np.arange(8)
    ang = 2.0 * np.pi * (e[:, None] * e[None, :]) / 64.0
    inner = np.stack([np.cos(ang), np.sin(ang)])[..., None] * np.ones(128)
    return big.astype(np.float32), small.astype(np.float32), inner.astype(np.float32)


def sign_rows():
    row = lax.broadcasted_iota(jnp.int32, (8, 128), 0)
    return jnp.where(row < 4, 1.0, -1.0).astype(F32)


def swap(x):
    return pltpu.roll(x, 4, x.ndim - 2)


def dft8(x, sg):
    def times_j(v):
        return swap(v) * sg

    def dft4(a0, a1, a2, a3):
        t0, t1, t2, t3 = a0 + a2, a0 - a2, a1 + a3, times_j(a1 - a3)
        return t0 + t2, t1 + t3, t0 - t2, t1 - t3

    e = dft4(x[0], x[2], x[4], x[6])
    o = dft4(x[1], x[3], x[5], x[7])
    j1, j3 = times_j(o[1]), times_j(o[3])
    o = (o[0], (o[1] + j1) * INV_SQRT2, times_j(o[2]), (j3 - o[3]) * INV_SQRT2)
    return [e[k] + o[k] for k in range(4)] + [e[k] - o[k] for k in range(4)]


def cmul(x, wr, wi, sg):
    return x * wr + (swap(x) * sg) * wi


def split(x):
    hi = x.astype(BF16)
    lo = (x - hi.astype(F32)).astype(BF16)
    return hi, lo


def unpack_voltages(x_ref, xf_ref, piece):
    per = 512 // LOADS

    def body(i, _):
        for u in range(8):
            t = piece * per + i * 8 + u
            col = pl.multiple_of(t * 128, 128)
            for ri in range(2):
                xf_ref[ri, t + 128] = x_ref[0, ri, :, pl.ds(col, 128)].astype(F32)
        return 0

    lax.fori_loop(0, per // 8, body, 0)


def wrap_voltages(xf_ref):
    def wrap(i, _):
        for ri in range(2):
            xf_ref[ri, pl.ds(i * 8, 8)] = xf_ref[ri, pl.ds(i * 8 + 512, 8)]
        return 0

    lax.fori_loop(0, 16, wrap, 0, unroll=4)


def delay_setup(d_ref):
    row = lax.broadcasted_iota(jnp.int32, (8, 128), 0)
    lane = lax.broadcasted_iota(jnp.int32, (8, 128), 1)
    fine = jnp.zeros((8, 128), jnp.int32)
    starts = []
    for r in range(8):
        d = d_ref[r]
        starts.append(128 - d // 128)
        fine = jnp.where(row == r, d % 128, fine)
    return starts, [row == r for r in range(8)], (lane - fine + 128) % 128, lane >= fine


def delay_rows(setup, xf_ref, out_ref, a0):
    starts, masks, index, keep = setup

    def body(a1, _):
        t = (8 * a1 + a0) * 8
        col = pl.multiple_of((8 * a0 + a1) * 128, 128)
        done = []
        for ri in range(2):
            acc = xf_ref[ri, pl.ds(starts[0] + t - 1, 9)]
            for r in range(1, 8):
                acc = jnp.where(masks[r], xf_ref[ri, pl.ds(starts[r] + t - 1, 9)], acc)
            g = [jnp.take_along_axis(acc[u], index, axis=1) for u in range(9)]
            done.append([jnp.where(keep, g[u + 1], g[u]) for u in range(8)])
        for j in range(8):
            out_ref[j, :, pl.ds(col, 128)] = jnp.concatenate([done[0][j], done[1][j]], axis=0).astype(BF16)
        return 0

    lax.fori_loop(0, 8, body, 0, unroll=2)


def one_hot(shape, hit):
    row = lax.broadcasted_iota(jnp.int32, shape, 0)
    col = lax.broadcasted_iota(jnp.int32, shape, 1)
    return jnp.where(hit(row, col), 1.0, 0.0).astype(BF16)


def stacked_weights(bw_ref):
    w0, w1 = bw_ref[0, 0], bw_ref[0, 1]
    to_real = one_hot((64, 128), lambda q, c: c == (q // 8) * 16 + q % 8)
    to_imag = one_hot((64, 128), lambda q, c: c == (q // 8) * 16 + 8 + q % 8)
    dot = functools.partial(jnp.dot, preferred_element_type=F32)
    real = (dot(w0, to_real) - dot(w1, to_imag)).astype(BF16)
    imag = (dot(w1, to_real) + dot(w0, to_imag)).astype(BF16)
    rows_real = one_hot((64, 32), lambda r, b: r == (b // 4) * 8 + b % 4)
    rows_imag = one_hot((64, 32), lambda r, b: r == (b // 4) * 8 + 4 + b % 4)
    return (dot(rows_real, real) + dot(rows_imag, imag)).astype(BF16)


def beamform(w_ref, v_ref, bm_ref, part):
    w = w_ref[...]

    def body(i, _):
        first = part * 8 + i * 4
        v = v_ref[:, :, pl.ds(pl.multiple_of(first * 128, 512), 512)].reshape(128, 512)
        out = jnp.dot(w, v, preferred_element_type=F32)
        for u in range(4):
            bm_ref[first + u] = out[:, u * 128 : (u + 1) * 128].reshape(8, 8, 128)
        return 0

    lax.fori_loop(0, 2, body, 0, unroll=2)


def inner_pass(ref, lead, twi_ref, sg):
    def body(g, _):
        at = pl.ds(g * 2, 2)
        y = dft8([ref[8 * lead + i, at] for i in range(8)], sg)
        for k in range(8):
            v = y[k]
            if k:
                v = cmul(v, twi_ref[0, lead, pl.ds(k, 1)], twi_ref[1, lead, pl.ds(k, 1)], sg)
            ref[8 * lead + k, at] = v
        return 0

    lax.fori_loop(0, 4, body, 0, unroll=4)


def encode(values, axes):
    top = jnp.max(jnp.abs(values), axis=axes, keepdims=True)
    top = jnp.maximum(top, 1e-33)
    return jnp.round(values * (TOP / top)), top * (1.0 / TOP)


def decode(ints):
    return ints.astype(jnp.int32).astype(F32)


def outer_and_encode(bm_ref, k0, sta, twb_ref, sg, q_ref, s_ref):
    for g in range(4):
        at = pl.ds(2 * g, 2)
        y = dft8([bm_ref[8 * i + k0, at] for i in range(8)], sg)
        out = []
        for k1 in range(8):
            k = 8 * k0 + k1
            out.append(cmul(y[k1], twb_ref[0, k, pl.ds(sta, 1)], twb_ref[1, k, pl.ds(sta, 1)], sg))
        q, scale = encode(jnp.stack(out, axis=1), (1, 2))
        q_ref[at, pl.ds(4 * k0, 4)] = q.reshape(2, 4, 16, 128).astype(jnp.int16)
        s_ref[at, k0] = scale.reshape(2, 1, 128)


def chirp_table(dm_ref, base_ref, h_ref, first, last):
    row = lax.broadcasted_iota(jnp.int32, (8, 128), 0)
    lane = lax.broadcasted_iota(jnp.int32, (8, 128), 1)
    centre = BASE_FREQ + CHANNEL_WIDTH * (
        jnp.zeros((8, 128), F32) + lax.axis_index("sub").astype(F32) + 0.5
    )

    def base(i, _):
        k0, kj = i // 8, i % 8
        positions = 8 * row + k0 + 64 * kj + 512 * lane
        signed_bin = jnp.where(positions < N // 2, positions, positions - N)
        offset = CHANNEL_WIDTH * signed_bin.astype(F32) / N
        base_ref[pl.ds(pl.multiple_of(i * 8, 8), 8), :] = (
            TWO_PI * DISPERSION * offset * offset / (centre * centre * (centre + offset))
        )
        return 0

    lax.fori_loop(first * 4, last * 4, base, 0)
    quarter = jnp.where(row < 4, 1, 0)
    dm = jnp.zeros((8, 128), F32)
    for b in range(4):
        dm = jnp.where(row % 4 == b, DM_STEP * dm_ref[b].astype(F32), dm)
    p1 = 1.5703125
    p2 = float(np.float32(np.round((np.pi / 2 - p1) * 2.0**22) / 2.0**22))
    p3 = float(np.float32(np.pi / 2 - p1 - p2))

    def one(r):
        phase = dm * base_ref[pl.ds(r, 1), :]
        n = jnp.floor(phase * float(2.0 / np.pi) + 0.5)
        y = ((phase - n * p1) - n * p2) - n * p3
        q = n.astype(jnp.int32) + quarter
        z = y * y
        s = ((-1.9515295891e-4 * z + 8.3321608736e-3) * z - 1.6666654611e-1) * z * y + y
        c = ((2.443315711809948e-5 * z - 1.388731625493765e-3) * z + 4.166664568298827e-2) * z * z - 0.5 * z + 1.0
        v = jnp.where((q & 1) == 0, s, c)
        h_ref[r] = jnp.where((q & 2) == 0, v, -v)

    def body(i, _):
        for u in range(4):
            one(i * 4 + u)
        return 0

    lax.fori_loop(first * 8, last * 8, body, 0)


def middle(k0, r_ref, rs_ref, h_ref, w1_ref, w2_ref, tws_ref, twb_ref, xs_ref, gt_ref, g_ref, sg):
    for m in range(4):
        x = [decode(r_ref[j, k0 * 4 + m]).reshape(2, 8, 128) * rs_ref[j, k0] for j in range(8)]
        y = dft8(x, sg)
        for kj in range(8):
            v = y[kj]
            if kj:
                v = cmul(v, tws_ref[0, pl.ds(kj, 1)], tws_ref[1, pl.ds(kj, 1)], sg)
            hi, lo = split(v.reshape(16, 128))
            at = kj * 64 + m * 16
            xs_ref[at : at + 16, 0:128] = hi
            xs_ref[at : at + 16, 128:256] = lo

    def dot128(sign):
        x = xs_ref[...]
        pq = jnp.dot(x, w1_ref[...], preferred_element_type=F32)
        pq = pq + jnp.dot(x[:, 0:128], w2_ref[...], preferred_element_type=F32)
        return pq[:, 0:128].reshape(64, 8, 128) + swap(pq[:, 128:256].reshape(64, 8, 128)) * sign

    low = lax.broadcasted_iota(jnp.int32, (8, 128), 0) < 4
    v = dot128(sg)
    h = h_ref[pl.ds(k0 * 64, 64)]
    hs = swap(h)
    v = v * jnp.where(low, h, hs) + swap(v) * jnp.where(low, -hs, h)
    hi, lo = split(v.reshape(512, 128))
    xs_ref[:, 0:128] = hi
    xs_ref[:, 128:256] = lo
    gt_ref[...] = dot128(-sg).reshape(8, 8, 8, 128)

    for i in range(4):
        x = []
        for kj in range(8):
            v = gt_ref[kj, 2 * i : 2 * i + 2]
            if kj:
                v = cmul(v, tws_ref[0, pl.ds(kj, 1)], tws_ref[1, pl.ds(kj, 1)], -sg)
            x.append(v)
        y = dft8(x, -sg)
        here = pl.ds(k0 * 8 + i * 2, 2)
        for j in range(8):
            g_ref[here, j] = cmul(y[j], twb_ref[0, here, pl.ds(j, 1)], twb_ref[1, here, pl.ds(j, 1)], -sg)


PLACES = ((0, 2, 1), (1, 0, 0), (0, 1, 0), (1, 3, 1), (0, 0, 1), (1, 2, 0), (0, 3, 0), (1, 1, 1), (0, 2, 0), (1, 0, 1), (0, 1, 1), (1, 3, 0), (0, 3, 1), (1, 1, 0), (1, 2, 1), (0, 0, 0))


def kernel(
    d_hbm, dm_hbm, x_hbm, bw_hbm, w1_hbm, w2_hbm, tws_hbm, twb_hbm, twi_hbm,
    recv3, rscale3,
    d_ref, dm_ref, bw_ref, x_ref, w1_ref, w2_ref, tws_ref, twb_ref, twi_ref,
    xf_ref, send1, recv1, w_ref, bm_ref, send2, scale2, recv2, rscale2, base_ref, h_ref, xs_ref, gt_ref, g_ref,
    send3, scale3,
    load_sem, answer_sem, col_sem, sem1, rsem1, sem2, rsem2, ssem2, rssem2, sem3, rsem3, ssem3, rssem3,
):
    sub, sta = lax.axis_index("sub"), lax.axis_index("sta")
    me = sub * STA + sta

    x_loads = []
    for i in range(LOADS):
        cols = pl.ds(i * (N // LOADS), N // LOADS)
        x_loads.append(pltpu.make_async_copy(x_hbm.at[:, :, :, cols], x_ref.at[:, :, :, cols], load_sem.at[i]))
    tables = [
        pltpu.make_async_copy(a, b, load_sem.at[LOADS + i])
        for i, (a, b) in enumerate(
            [
                (d_hbm, d_ref), (dm_hbm, dm_ref), (bw_hbm, bw_ref), (w1_hbm, w1_ref), (w2_hbm, w2_ref),
                (tws_hbm, tws_ref), (twb_hbm, twb_ref), (twi_hbm, twi_ref),
            ]
        )
    ]
    for t in tables[:1] + x_loads + tables[1:]:
        t.start()

    barrier = pltpu.get_barrier_semaphore()
    for i in range(1, STA):
        pl.semaphore_signal(barrier, inc=1, device_id={"sub": sub, "sta": (sta + i) % STA}, device_id_type=MESH)
    x_hi, z, core = sub // 8, (sub // 2) % 4, sub % 2
    rank = 4 * z + 2 * x_hi + core

    def column(r):
        return {"sub": 8 * ((r // 2) % 2) + 2 * (r // 4) + r % 2, "sta": sta}

    def greet(r, _):
        pl.semaphore_signal(barrier, inc=1, device_id=column(r), device_id_type=MESH)
        return 0

    lax.fori_loop(rank + 1, SUB, greet, 0)
    for i in range(LOADS):
        x_loads[i].wait()
        unpack_voltages(x_ref, xf_ref, i)
    wrap_voltages(xf_ref)
    tables[0].wait()
    setup = delay_setup(d_ref)

    def first(part):
        cols = pl.ds(pl.multiple_of(part * 1024, 1024), 1024)
        for i in range(1, STA):
            d = (sta + i) % STA
            pltpu.make_async_remote_copy(
                src_ref=send1.at[d, :, cols],
                dst_ref=recv1.at[sta, :, cols],
                send_sem=sem1,
                recv_sem=rsem1.at[part],
                device_id={"sub": sub, "sta": d},
                device_id_type=MESH,
            ).start()
        pltpu.make_async_copy(send1.at[sta, :, cols], recv1.at[sta, :, cols], rsem1.at[part]).start()

    tables[1].wait()
    late = HEAD_START * (1 - (sub % 2))
    chirp_table(dm_ref, base_ref, h_ref, 0, late)
    delay_rows(setup, xf_ref, send1, 0)
    pl.semaphore_wait(barrier, STA - 1 + rank)
    first(0)

    def answer(r, _):
        pl.semaphore_signal(answer_sem, inc=1, device_id=column(r), device_id_type=MESH)
        return 0

    lax.fori_loop(0, rank, answer, 0)

    def more(part, _):
        delay_rows(setup, xf_ref, send1, part)
        first(part)
        return 0

    lax.fori_loop(1, CH, more, 0)

    for t in tables[2:]:
        t.wait()
    w_ref[...] = stacked_weights(bw_ref)
    chirp_table(dm_ref, base_ref, h_ref, late, 16)
    @pl.when(rank < SUB - 1)
    def _():
        pl.semaphore_wait(answer_sem, SUB - 1 - rank)

    for i in range(1, STA):
        pl.semaphore_signal(col_sem, inc=1, device_id={"sub": sub, "sta": (sta + i) % STA}, device_id_type=MESH)
    sg = sign_rows()

    def beams(part, _):
        cols = pl.ds(pl.multiple_of(part * 1024, 1024), 1024)
        pltpu.make_async_copy(recv1.at[:, :, cols], recv1.at[:, :, cols], rsem1.at[part]).wait()
        beamform(w_ref, recv1, bm_ref, part)
        inner_pass(bm_ref, part, twi_ref, sg)
        return 0

    lax.fori_loop(0, CH, beams, 0)

    def second(part, _):
        outer_and_encode(bm_ref, part, sta, twb_ref, sg, send2, scale2)
        rows = pl.ds(part * 4, 4)
        for i in range(1, STA):
            d = (sta + i) % STA
            pltpu.make_async_remote_copy(
                src_ref=scale2.at[d, part],
                dst_ref=rscale2.at[sta, part],
                send_sem=ssem2,
                recv_sem=rssem2.at[part],
                device_id={"sub": sub, "sta": d},
                device_id_type=MESH,
            ).start()
            pltpu.make_async_remote_copy(
                src_ref=send2.at[d, rows],
                dst_ref=recv2.at[sta, rows],
                send_sem=sem2,
                recv_sem=rsem2.at[part],
                device_id={"sub": sub, "sta": d},
                device_id_type=MESH,
            ).start()
        pltpu.make_async_copy(scale2.at[sta, part], rscale2.at[sta, part], rssem2.at[part]).start()
        pltpu.make_async_copy(send2.at[sta, rows], recv2.at[sta, rows], rsem2.at[part]).start()
        return 0

    lax.fori_loop(0, CH, second, 0)

    def spectra(part, _):
        rows = pl.ds(part * 4, 4)
        pltpu.make_async_copy(rscale2.at[:, part], rscale2.at[:, part], rssem2.at[part]).wait()
        pltpu.make_async_copy(recv2.at[:, rows], recv2.at[:, rows], rsem2.at[part]).wait()
        middle(part, recv2, rscale2, h_ref, w1_ref, w2_ref, tws_ref, twb_ref, xs_ref, gt_ref, g_ref, sg)
        inner_pass(g_ref, part, twi_ref, -sg)
        return 0

    lax.fori_loop(0, CH, spectra, 0)

    pl.semaphore_wait(col_sem, STA - 1)
    x_lo, yh, jh_own = sta // 4, (sta // 2) % 2, sta % 2

    def group(i, _):
        a0 = 4 * ((core + 1 - (i // 4) % 2) % 2) + 2 * ((x_lo + 1 - (i // 2) % 2) % 2) + (yh + 1 - i % 2) % 2
        for jh in range(2):
            y = dft8([g_ref[8 * k0 + a0, pl.ds(4 * jh, 4)] for k0 in range(8)], -sg)
            for a1 in range(8):
                d = 16 * a1 + 2 * a0 + jh
                q, scale = encode(y[a1], (0, 1))
                send3[d] = q.reshape(2, 16, 128).astype(jnp.int16)
                scale3[d] = scale.reshape(1, 128) * (1.0 / N)

        for dx, dz, dj in PLACES:
            d = 64 * ((x_hi + dx) % 2) + 16 * ((z + dz) % 4) + 2 * a0 + (jh_own + dj) % 2

            def go():
                pltpu.make_async_remote_copy(
                    src_ref=scale3.at[d],
                    dst_ref=rscale3.at[me],
                    send_sem=ssem3,
                    recv_sem=rssem3.at[sub],
                    device_id={"sub": d // STA, "sta": d % STA},
                    device_id_type=MESH,
                ).start()
                pltpu.make_async_remote_copy(
                    src_ref=send3.at[d],
                    dst_ref=recv3.at[me],
                    send_sem=sem3,
                    recv_sem=rsem3.at[sub],
                    device_id={"sub": d // STA, "sta": d % STA},
                    device_id_type=MESH,
                ).start()

            if dx or dz or dj:
                go()
            else:
                pl.when(d != me)(go)

                @pl.when(d == me)
                def _():
                    pltpu.make_async_copy(scale3.at[me], rscale3.at[me], rssem3.at[sub]).start()
                    pltpu.make_async_copy(send3.at[me], recv3.at[me], rsem3.at[sub]).start()

        return 0

    lax.fori_loop(0, 8, group, 0)

    for s in range(SUB):
        block = recv3.at[pl.ds(s * STA, STA)]
        pltpu.make_async_copy(block, block, rsem3.at[s]).wait()
        block = rscale3.at[pl.ds(s * STA, STA)]
        pltpu.make_async_copy(block, block, rssem3.at[s]).wait()
    others = pl.ds(0, STA - 1)
    pltpu.make_async_copy(send1.at[others], send1.at[others], sem1).wait()
    pltpu.make_async_copy(send2.at[others], send2.at[others], sem2).wait()
    pltpu.make_async_copy(scale2.at[others], scale2.at[others], ssem2).wait()
    others = pl.ds(0, SUB * STA - 1)
    pltpu.make_async_copy(send3.at[others], send3.at[others], sem3).wait()
    pltpu.make_async_copy(scale3.at[others], scale3.at[others], ssem3).wait()


def assemble(q_ref, s_ref, out_hbm, int_ref, out_ref, acc_ref, out_sem):
    acc_ref[...] = jnp.zeros_like(acc_ref)

    def one(s, _):
        for sta in range(STA):
            src = s * STA + sta
            v = decode(q_ref[src].reshape(32, 128)).reshape(4, 8, 128) * s_ref[src]
            acc_ref[sta] += v * v
            for j4 in range(4):
                for ri in range(2):
                    first = s * 256 + (ri * 128 + sta * 16 + j4)
                    out_ref[pl.ds(first, 4, stride=4), :] = v[j4, 4 * ri : 4 * ri + 4]
        rows = pl.ds(pl.multiple_of(s * 256, 256), 256)
        pltpu.make_async_copy(out_ref.at[rows], out_hbm.at[rows], out_sem).start()
        return 0

    lax.fori_loop(0, SUB, one, 0)
    for sta in range(STA):
        for j4 in range(4):
            v = acc_ref[sta, j4]
            v = (v + swap(v)) * (1.0 / SUB)
            int_ref[pl.ds(sta * 16 + j4, 4, stride=4), :] = v[0:4]
    pltpu.make_async_copy(out_ref, out_hbm, out_sem).wait()


VM = pl.BlockSpec(memory_space=pltpu.VMEM)
SM = pl.BlockSpec(memory_space=pltpu.SMEM)
ANY = pl.BlockSpec(memory_space=pl.ANY)
HBM = pl.BlockSpec(memory_space=pltpu.HBM)


def shards(voltages, beam_weights, station_delays, dm_index):
    w1, w2 = dft_tables()
    big, small, inner = twist_tables()
    moved, scales = pl.pallas_call(
        kernel,
        out_shape=(
            pltpu.VMEM((128, 2, 16, 128), jnp.int16),
            pltpu.VMEM((128, 1, 128), F32),
        ),
        in_specs=[HBM] * 9,
        out_specs=(ANY, ANY),
        scratch_shapes=[
            pltpu.SMEM((8,), jnp.int32),
            pltpu.SMEM((4,), jnp.int32),
            pltpu.VMEM((1, 2, 32, 64), BF16),
            pltpu.VMEM((1, 2, 8, N), BF16),
            pltpu.VMEM((256, 256), BF16),
            pltpu.VMEM((128, 256), BF16),
            pltpu.VMEM((2, 8, 128), F32),
            pltpu.VMEM((2, 64, 8, 128), F32),
            pltpu.VMEM((2, 8, 8, 128), F32),
            pltpu.VMEM((2, 640, 8, 128), F32),
            pltpu.VMEM((8, 16, 8192), BF16),
            pltpu.VMEM((8, 16, 8192), BF16),
            pltpu.VMEM((64, 128), BF16),
            pltpu.VMEM((64, 8, 8, 128), F32),
            pltpu.VMEM((8, 32, 16, 128), jnp.int16),
            pltpu.VMEM((8, CH, 1, 128), F32),
            pltpu.VMEM((8, 32, 16, 128), jnp.int16),
            pltpu.VMEM((8, CH, 1, 128), F32),
            pltpu.VMEM((512, 128), F32),
            pltpu.VMEM((512, 8, 128), F32),
            pltpu.VMEM((512, 256), BF16),
            pltpu.VMEM((8, 8, 8, 128), F32),
            pltpu.VMEM((64, 8, 8, 128), F32),
            pltpu.VMEM((128, 2, 16, 128), jnp.int16),
            pltpu.VMEM((128, 1, 128), F32),
            pltpu.SemaphoreType.DMA((LOADS + 8,)),
            pltpu.SemaphoreType.REGULAR,
            pltpu.SemaphoreType.REGULAR,
            pltpu.SemaphoreType.DMA,
            pltpu.SemaphoreType.DMA((CH,)),
            pltpu.SemaphoreType.DMA,
            pltpu.SemaphoreType.DMA((CH,)),
            pltpu.SemaphoreType.DMA,
            pltpu.SemaphoreType.DMA((CH,)),
            pltpu.SemaphoreType.DMA,
            pltpu.SemaphoreType.DMA((SUB,)),
            pltpu.SemaphoreType.DMA,
            pltpu.SemaphoreType.DMA((SUB,)),
        ],
        compiler_params=pltpu.CompilerParams(
            collective_id=0, has_side_effects=True, vmem_limit_bytes=56 * 1024 * 1024
        ),
    )(
        station_delays, dm_index.reshape(4), voltages, beam_weights,
        jnp.asarray(w1), jnp.asarray(w2), jnp.asarray(small), jnp.asarray(big), jnp.asarray(inner),
    )
    out, power = pl.pallas_call(
        assemble,
        out_shape=(jax.ShapeDtypeStruct((4096, 128), F32), jax.ShapeDtypeStruct((128, 128), F32)),
        in_specs=[VM, VM],
        out_specs=(ANY, VM),
        scratch_shapes=[
            pltpu.VMEM((4096, 128), F32),
            pltpu.VMEM((STA, 4, 8, 128), F32),
            pltpu.SemaphoreType.DMA,
        ],
        compiler_params=pltpu.CompilerParams(vmem_limit_bytes=16 * 1024 * 1024),
    )(moved, scales)
    return out.reshape(16, 2, 32, 1, 512), power.reshape(32, 1, 512)


def solution(mesh):
    return jax.shard_map(
        shards,
        mesh=mesh,
        in_specs=(
            P("sub", None, "sta", None),
            P("sub", None, None, None),
            P("sta"),
            P("sta", None),
        ),
        out_specs=(P(None, None, None, None, ("sub", "sta")), P(None, None, ("sub", "sta"))),
        check_vma=False,
    )
```

```python
import functools

import jax
import jax.numpy as jnp
import numpy as np
from jax import lax
from jax.experimental import pallas as pl
from jax.experimental.pallas import tpu as pltpu
from jax.sharding import PartitionSpec as P

TWO_PI = 6.283185307179586
DISPERSION = 4148808000.0
DM_STEP = 10.0
BASE_FREQ = 120.0
CHANNEL_WIDTH = 0.1953125
F32 = jnp.float32
BF16 = jnp.bfloat16
N = 65536
STA = 8
SUB = 16
INV_SQRT2 = 0.7071067811865476


MESH = pl.DeviceIdType.MESH
TOP = 32767.0
LOG_TOP = float(np.log2(32766.0))
CH = 8
LOADS = 4
HEAD_START = 12


def dft_tables():
    k = np.arange(128)
    ang = 2.0 * np.pi * ((k[:, None] * k[None, :]) % 128) / 128.0
    full = np.concatenate([np.cos(ang), np.sin(ang)], axis=1).astype(np.float32)
    hi = full.astype(jnp.bfloat16)
    lo = (full - hi.astype(np.float32)).astype(jnp.bfloat16)
    return np.concatenate([hi, hi], axis=0), lo


def twist_tables():
    at = np.arange(64)
    ka = (8 * (at % 8) + at // 8)[:, None]
    n = np.arange(1024)[None, :]
    ang = 2.0 * np.pi * (ka * n) / N
    big = np.stack([np.cos(ang), np.sin(ang)]).reshape(2, 64, 8, 128)
    kj = np.arange(8)[:, None]
    c = np.arange(128)[None, :]
    ang = 2.0 * np.pi * (kj * c) / 1024.0
    small = np.stack([np.cos(ang), np.sin(ang)])
    e = np.arange(8)
    ang = 2.0 * np.pi * (e[:, None] * e[None, :]) / 64.0
    inner = np.stack([np.cos(ang), np.sin(ang)])[..., None] * np.ones(128)
    return big.astype(np.float32), small.astype(np.float32), inner.astype(np.float32)


def sign_rows():
    row = lax.broadcasted_iota(jnp.int32, (8, 128), 0)
    return jnp.where(row < 4, 1.0, -1.0).astype(F32)


def swap(x):
    return pltpu.roll(x, 4, x.ndim - 2)


def dft8(x, sg):
    def times_j(v):
        return swap(v) * sg

    def dft4(a0, a1, a2, a3):
        t0, t1, t2, t3 = a0 + a2, a0 - a2, a1 + a3, times_j(a1 - a3)
        return t0 + t2, t1 + t3, t0 - t2, t1 - t3

    e = dft4(x[0], x[2], x[4], x[6])
    o = dft4(x[1], x[3], x[5], x[7])
    j1, j3 = times_j(o[1]), times_j(o[3])
    o = (o[0], (o[1] + j1) * INV_SQRT2, times_j(o[2]), (j3 - o[3]) * INV_SQRT2)
    return [e[k] + o[k] for k in range(4)] + [e[k] - o[k] for k in range(4)]


def cmul(x, wr, wi, sg):
    return x * wr + (swap(x) * sg) * wi


def split(x):
    hi = x.astype(BF16)
    lo = (x - hi.astype(F32)).astype(BF16)
    return hi, lo


def unpack_voltages(x_ref, xf_ref, piece):
    per = 512 // LOADS

    def body(i, _):
        for u in range(8):
            t = piece * per + i * 8 + u
            col = pl.multiple_of(t * 128, 128)
            for ri in range(2):
                xf_ref[ri, t + 128] = x_ref[0, ri, :, pl.ds(col, 128)].astype(F32)
        return 0

    lax.fori_loop(0, per // 8, body, 0)


def wrap_voltages(xf_ref):
    def wrap(i, _):
        for ri in range(2):
            xf_ref[ri, pl.ds(i * 8, 8)] = xf_ref[ri, pl.ds(i * 8 + 512, 8)]
        return 0

    lax.fori_loop(0, 16, wrap, 0, unroll=4)


def delay_setup(d_ref):
    row = lax.broadcasted_iota(jnp.int32, (8, 128), 0)
    lane = lax.broadcasted_iota(jnp.int32, (8, 128), 1)
    fine = jnp.zeros((8, 128), jnp.int32)
    starts = []
    for r in range(8):
        d = d_ref[r]
        starts.append(128 - d // 128)
        fine = jnp.where(row == r, d % 128, fine)
    return starts, [row == r for r in range(8)], (lane - fine + 128) % 128, lane >= fine


def delay_rows(setup, xf_ref, out_ref, a0):
    starts, masks, index, keep = setup

    def body(a1, _):
        t = (8 * a1 + a0) * 8
        col = pl.multiple_of((8 * a0 + a1) * 128, 128)
        done = []
        for ri in range(2):
            acc = xf_ref[ri, pl.ds(starts[0] + t - 1, 9)]
            for r in range(1, 8):
                acc = jnp.where(masks[r], xf_ref[ri, pl.ds(starts[r] + t - 1, 9)], acc)
            g = [jnp.take_along_axis(acc[u], index, axis=1) for u in range(9)]
            done.append([jnp.where(keep, g[u + 1], g[u]) for u in range(8)])
        for j in range(8):
            out_ref[j, :, pl.ds(col, 128)] = jnp.concatenate([done[0][j], done[1][j]], axis=0).astype(BF16)
        return 0

    lax.fori_loop(0, 8, body, 0, unroll=2)


def one_hot(shape, hit):
    row = lax.broadcasted_iota(jnp.int32, shape, 0)
    col = lax.broadcasted_iota(jnp.int32, shape, 1)
    return jnp.where(hit(row, col), 1.0, 0.0).astype(BF16)


def stacked_weights(bw_ref):
    w0, w1 = bw_ref[0, 0], bw_ref[0, 1]
    to_real = one_hot((64, 128), lambda q, c: c == (q // 8) * 16 + q % 8)
    to_imag = one_hot((64, 128), lambda q, c: c == (q // 8) * 16 + 8 + q % 8)
    dot = functools.partial(jnp.dot, preferred_element_type=F32)
    real = (dot(w0, to_real) - dot(w1, to_imag)).astype(BF16)
    imag = (dot(w1, to_real) + dot(w0, to_imag)).astype(BF16)
    rows_real = one_hot((64, 32), lambda r, b: r == (b // 4) * 8 + b % 4)
    rows_imag = one_hot((64, 32), lambda r, b: r == (b // 4) * 8 + 4 + b % 4)
    return (dot(rows_real, real) + dot(rows_imag, imag)).astype(BF16)


def beamform(w_ref, v_ref, bm_ref, part):
    w = w_ref[...]

    def body(i, _):
        first = part * 8 + i * 4
        v = v_ref[:, :, pl.ds(pl.multiple_of(first * 128, 512), 512)].reshape(128, 512)
        out = jnp.dot(w, v, preferred_element_type=F32)
        for u in range(4):
            bm_ref[first + u] = out[:, u * 128 : (u + 1) * 128].reshape(8, 8, 128)
        return 0

    lax.fori_loop(0, 2, body, 0, unroll=2)


def inner_pass(ref, lead, twi_ref, sg):
    def body(g, _):
        at = pl.ds(g * 2, 2)
        y = dft8([ref[8 * lead + i, at] for i in range(8)], sg)
        for k in range(8):
            v = y[k]
            if k:
                v = cmul(v, twi_ref[0, lead, pl.ds(k, 1)], twi_ref[1, lead, pl.ds(k, 1)], sg)
            ref[8 * lead + k, at] = v
        return 0

    lax.fori_loop(0, 4, body, 0, unroll=4)


def encode(values, axes):
    top = jnp.max(jnp.abs(values), axis=axes, keepdims=True)
    top = jnp.maximum(top, 1e-33)
    return jnp.round(values * (TOP / top)), top * (1.0 / TOP)


def pack(values):
    top = jnp.maximum(jnp.max(jnp.abs(values), axis=(0, 1), keepdims=True), 1e-33)
    power = jnp.ceil(jnp.log2(top) - LOG_TOP)
    q = jnp.round(values * jnp.exp2(-power)).astype(jnp.int32)
    return ((q[0:2] << 16) | (q[2:4] & 0xFFFF)).reshape(16, 128), power.reshape(1, 128).astype(jnp.int32)


def unpack(block):
    words = block[0:16].reshape(2, 8, 128)
    q = jnp.concatenate([words >> 16, (words << 16) >> 16], axis=0)
    return q.astype(F32) * jnp.exp2(block[16:17].astype(F32))


def decode(ints):
    return ints.astype(jnp.int32).astype(F32)


def outer_and_encode(bm_ref, k0, sta, twb_ref, sg, q_ref, s_ref):
    for g in range(4):
        at = pl.ds(2 * g, 2)
        y = dft8([bm_ref[8 * i + k0, at] for i in range(8)], sg)
        out = []
        for k1 in range(8):
            k = 8 * k0 + k1
            out.append(cmul(y[k1], twb_ref[0, k, pl.ds(sta, 1)], twb_ref[1, k, pl.ds(sta, 1)], sg))
        q, scale = encode(jnp.stack(out, axis=1), (1, 2))
        q_ref[at, pl.ds(4 * k0, 4)] = q.reshape(2, 4, 16, 128).astype(jnp.int16)
        s_ref[at, k0] = scale.reshape(2, 1, 128)


def chirp_table(dm_ref, base_ref, h_ref, first, last):
    row = lax.broadcasted_iota(jnp.int32, (8, 128), 0)
    lane = lax.broadcasted_iota(jnp.int32, (8, 128), 1)
    centre = BASE_FREQ + CHANNEL_WIDTH * (
        jnp.zeros((8, 128), F32) + lax.axis_index("sub").astype(F32) + 0.5
    )

    def base(i, _):
        k0, kj = i // 8, i % 8
        positions = 8 * row + k0 + 64 * kj + 512 * lane
        signed_bin = jnp.where(positions < N // 2, positions, positions - N)
        offset = CHANNEL_WIDTH * signed_bin.astype(F32) / N
        base_ref[pl.ds(pl.multiple_of(i * 8, 8), 8), :] = (
            TWO_PI * DISPERSION * offset * offset / (centre * centre * (centre + offset))
        )
        return 0

    lax.fori_loop(first * 4, last * 4, base, 0)
    quarter = jnp.where(row < 4, 1, 0)
    dm = jnp.zeros((8, 128), F32)
    for b in range(4):
        dm = jnp.where(row % 4 == b, DM_STEP * dm_ref[b].astype(F32), dm)
    p1 = 1.5703125
    p2 = float(np.float32(np.round((np.pi / 2 - p1) * 2.0**22) / 2.0**22))
    p3 = float(np.float32(np.pi / 2 - p1 - p2))

    def one(r):
        phase = dm * base_ref[pl.ds(r, 1), :]
        n = jnp.floor(phase * float(2.0 / np.pi) + 0.5)
        y = ((phase - n * p1) - n * p2) - n * p3
        q = n.astype(jnp.int32) + quarter
        z = y * y
        s = ((-1.9515295891e-4 * z + 8.3321608736e-3) * z - 1.6666654611e-1) * z * y + y
        c = ((2.443315711809948e-5 * z - 1.388731625493765e-3) * z + 4.166664568298827e-2) * z * z - 0.5 * z + 1.0
        v = jnp.where((q & 1) == 0, s, c)
        h_ref[r] = jnp.where((q & 2) == 0, v, -v)

    def body(i, _):
        for u in range(4):
            one(i * 4 + u)
        return 0

    lax.fori_loop(first * 8, last * 8, body, 0)


def middle(k0, r_ref, rs_ref, h_ref, w1_ref, w2_ref, tws_ref, twb_ref, xs_ref, gt_ref, g_ref, sg):
    for m in range(4):
        x = [decode(r_ref[j, k0 * 4 + m]).reshape(2, 8, 128) * rs_ref[j, k0] for j in range(8)]
        y = dft8(x, sg)
        for kj in range(8):
            v = y[kj]
            if kj:
                v = cmul(v, tws_ref[0, pl.ds(kj, 1)], tws_ref[1, pl.ds(kj, 1)], sg)
            hi, lo = split(v.reshape(16, 128))
            at = kj * 64 + m * 16
            xs_ref[at : at + 16, 0:128] = hi
            xs_ref[at : at + 16, 128:256] = lo

    def dot128(sign):
        x = xs_ref[...]
        pq = jnp.dot(x, w1_ref[...], preferred_element_type=F32)
        pq = pq + jnp.dot(x[:, 0:128], w2_ref[...], preferred_element_type=F32)
        return pq[:, 0:128].reshape(64, 8, 128) + swap(pq[:, 128:256].reshape(64, 8, 128)) * sign

    low = lax.broadcasted_iota(jnp.int32, (8, 128), 0) < 4
    v = dot128(sg)
    h = h_ref[pl.ds(k0 * 64, 64)]
    hs = swap(h)
    v = v * jnp.where(low, h, hs) + swap(v) * jnp.where(low, -hs, h)
    hi, lo = split(v.reshape(512, 128))
    xs_ref[:, 0:128] = hi
    xs_ref[:, 128:256] = lo
    gt_ref[...] = dot128(-sg).reshape(8, 8, 8, 128)

    for i in range(4):
        x = []
        for kj in range(8):
            v = gt_ref[kj, 2 * i : 2 * i + 2]
            if kj:
                v = cmul(v, tws_ref[0, pl.ds(kj, 1)], tws_ref[1, pl.ds(kj, 1)], -sg)
            x.append(v)
        y = dft8(x, -sg)
        here = pl.ds(k0 * 8 + i * 2, 2)
        for j in range(8):
            g_ref[here, j] = cmul(y[j], twb_ref[0, here, pl.ds(j, 1)], twb_ref[1, here, pl.ds(j, 1)], -sg)


EARLY_Z, LATE_Z = (0, 1), (2, 3)


def kernel(
    d_hbm, dm_hbm, x_hbm, bw_hbm, w1_hbm, w2_hbm, tws_hbm, twb_hbm, twi_hbm,
    recv3,
    d_ref, dm_ref, bw_ref, x_ref, w1_ref, w2_ref, tws_ref, twb_ref, twi_ref,
    xf_ref, send1, recv1, w_ref, bm_ref, send2, scale2, recv2, rscale2, base_ref, h_ref, xs_ref, gt_ref, g_ref,
    send3,
    load_sem, answer_sem, col_sem, sem1, rsem1, sem2, rsem2, ssem2, rssem2, sem3, rsem3,
):
    sub, sta = lax.axis_index("sub"), lax.axis_index("sta")
    me = sub * STA + sta

    x_loads = []
    for i in range(LOADS):
        cols = pl.ds(i * (N // LOADS), N // LOADS)
        x_loads.append(pltpu.make_async_copy(x_hbm.at[:, :, :, cols], x_ref.at[:, :, :, cols], load_sem.at[i]))
    tables = [
        pltpu.make_async_copy(a, b, load_sem.at[LOADS + i])
        for i, (a, b) in enumerate(
            [
                (d_hbm, d_ref), (dm_hbm, dm_ref), (bw_hbm, bw_ref), (w1_hbm, w1_ref), (w2_hbm, w2_ref),
                (tws_hbm, tws_ref), (twb_hbm, twb_ref), (twi_hbm, twi_ref),
            ]
        )
    ]
    for t in tables[:1] + x_loads + tables[1:]:
        t.start()

    barrier = pltpu.get_barrier_semaphore()
    for i in range(1, STA):
        pl.semaphore_signal(barrier, inc=1, device_id={"sub": sub, "sta": (sta + i) % STA}, device_id_type=MESH)
    x_hi, z, core = sub // 8, (sub // 2) % 4, sub % 2
    rank = 4 * z + 2 * x_hi + core

    def column(r):
        return {"sub": 8 * ((r // 2) % 2) + 2 * (r // 4) + r % 2, "sta": sta}

    def greet(r, _):
        pl.semaphore_signal(barrier, inc=1, device_id=column(r), device_id_type=MESH)
        return 0

    lax.fori_loop(rank + 1, SUB, greet, 0)
    for i in range(LOADS):
        x_loads[i].wait()
        unpack_voltages(x_ref, xf_ref, i)
    wrap_voltages(xf_ref)
    tables[0].wait()
    setup = delay_setup(d_ref)

    def first(part):
        cols = pl.ds(pl.multiple_of(part * 1024, 1024), 1024)
        for i in range(1, STA):
            d = (sta + i) % STA
            pltpu.make_async_remote_copy(
                src_ref=send1.at[d, :, cols],
                dst_ref=recv1.at[sta, :, cols],
                send_sem=sem1,
                recv_sem=rsem1.at[part],
                device_id={"sub": sub, "sta": d},
                device_id_type=MESH,
            ).start()
        pltpu.make_async_copy(send1.at[sta, :, cols], recv1.at[sta, :, cols], rsem1.at[part]).start()

    tables[1].wait()
    late = HEAD_START * (1 - (sub % 2))
    chirp_table(dm_ref, base_ref, h_ref, 0, late)
    delay_rows(setup, xf_ref, send1, 0)
    pl.semaphore_wait(barrier, STA - 1 + rank)
    first(0)

    def answer(r, _):
        pl.semaphore_signal(answer_sem, inc=1, device_id=column(r), device_id_type=MESH)
        return 0

    lax.fori_loop(0, rank, answer, 0)

    def more(part, _):
        delay_rows(setup, xf_ref, send1, part)
        first(part)
        return 0

    lax.fori_loop(1, CH, more, 0)

    for t in tables[2:]:
        t.wait()
    w_ref[...] = stacked_weights(bw_ref)
    chirp_table(dm_ref, base_ref, h_ref, late, 16)
    @pl.when(rank < SUB - 1)
    def _():
        pl.semaphore_wait(answer_sem, SUB - 1 - rank)

    for i in range(1, STA):
        pl.semaphore_signal(col_sem, inc=1, device_id={"sub": sub, "sta": (sta + i) % STA}, device_id_type=MESH)
    sg = sign_rows()

    def beams(part, _):
        cols = pl.ds(pl.multiple_of(part * 1024, 1024), 1024)
        pltpu.make_async_copy(recv1.at[:, :, cols], recv1.at[:, :, cols], rsem1.at[part]).wait()
        beamform(w_ref, recv1, bm_ref, part)
        inner_pass(bm_ref, part, twi_ref, sg)
        return 0

    lax.fori_loop(0, CH, beams, 0)

    def second(part, _):
        outer_and_encode(bm_ref, part, sta, twb_ref, sg, send2, scale2)
        rows = pl.ds(part * 4, 4)
        for i in range(1, STA):
            d = (sta + i) % STA
            pltpu.make_async_remote_copy(
                src_ref=scale2.at[d, part],
                dst_ref=rscale2.at[sta, part],
                send_sem=ssem2,
                recv_sem=rssem2.at[part],
                device_id={"sub": sub, "sta": d},
                device_id_type=MESH,
            ).start()
            pltpu.make_async_remote_copy(
                src_ref=send2.at[d, rows],
                dst_ref=recv2.at[sta, rows],
                send_sem=sem2,
                recv_sem=rsem2.at[part],
                device_id={"sub": sub, "sta": d},
                device_id_type=MESH,
            ).start()
        pltpu.make_async_copy(scale2.at[sta, part], rscale2.at[sta, part], rssem2.at[part]).start()
        pltpu.make_async_copy(send2.at[sta, rows], recv2.at[sta, rows], rsem2.at[part]).start()
        return 0

    lax.fori_loop(0, CH, second, 0)

    def spectra(part, _):
        rows = pl.ds(part * 4, 4)
        pltpu.make_async_copy(rscale2.at[:, part], rscale2.at[:, part], rssem2.at[part]).wait()
        pltpu.make_async_copy(recv2.at[:, rows], recv2.at[:, rows], rsem2.at[part]).wait()
        middle(part, recv2, rscale2, h_ref, w1_ref, w2_ref, tws_ref, twb_ref, xs_ref, gt_ref, g_ref, sg)
        inner_pass(g_ref, part, twi_ref, -sg)
        return 0

    lax.fori_loop(0, CH, spectra, 0)

    pl.semaphore_wait(col_sem, STA - 1)
    x_lo, yh, jh_own = sta // 4, (sta // 2) % 2, sta % 2

    def group_of(i):
        return 4 * ((core + 1 - i // 4) % 2) + 2 * ((x_lo + 1 - (i // 2) % 2) % 2) + (yh + 1 - i % 2) % 2

    def copies(a0, planes):
        for n, z_to in enumerate(planes * 4):
            dx, dj = 1 - n // (2 * len(planes)), 1 - (n // len(planes)) % 2
            d = 64 * ((x_hi + dx) % 2) + 16 * z_to + 2 * a0 + (jh_own + dj) % 2

            def go():
                pltpu.make_async_remote_copy(
                    src_ref=send3.at[d],
                    dst_ref=recv3.at[me],
                    send_sem=sem3,
                    recv_sem=rsem3.at[sub],
                    device_id={"sub": d // STA, "sta": d % STA},
                    device_id_type=MESH,
                ).start()

            if dx or dj:
                go()
            else:
                pl.when(d != me)(go)

                @pl.when(d == me)
                def _():
                    pltpu.make_async_copy(send3.at[me], recv3.at[me], rsem3.at[sub]).start()

    def group(i, _):
        a0 = group_of(i)
        for jh in range(2):
            y = dft8([g_ref[8 * k0 + a0, pl.ds(4 * jh, 4)] for k0 in range(8)], -sg)
            for a1 in range(8):
                d = 16 * a1 + 2 * a0 + jh
                send3[d, 0:16], send3[d, 16:17] = pack(y[a1] * (1.0 / N))
        copies(a0, EARLY_Z)
        return 0

    lax.fori_loop(0, 8, group, 0)

    def rest(i, _):
        copies(group_of(i), LATE_Z)
        return 0

    lax.fori_loop(0, 8, rest, 0)

    for s in range(SUB):
        block = recv3.at[pl.ds(s * STA, STA)]
        pltpu.make_async_copy(block, block, rsem3.at[s]).wait()
    others = pl.ds(0, STA - 1)
    pltpu.make_async_copy(send1.at[others], send1.at[others], sem1).wait()
    pltpu.make_async_copy(send2.at[others], send2.at[others], sem2).wait()
    pltpu.make_async_copy(scale2.at[others], scale2.at[others], ssem2).wait()
    others = pl.ds(0, SUB * STA - 1)
    pltpu.make_async_copy(send3.at[others], send3.at[others], sem3).wait()


def assemble(q_ref, out_hbm, int_ref, out_ref, acc_ref, out_sem):
    acc_ref[...] = jnp.zeros_like(acc_ref)

    def one(s, _):
        for sta in range(STA):
            src = s * STA + sta
            v = unpack(q_ref[src])
            acc_ref[sta] += v * v
            for j4 in range(4):
                for ri in range(2):
                    first = s * 256 + (ri * 128 + sta * 16 + j4)
                    out_ref[pl.ds(first, 4, stride=4), :] = v[j4, 4 * ri : 4 * ri + 4]
        rows = pl.ds(pl.multiple_of(s * 256, 256), 256)
        pltpu.make_async_copy(out_ref.at[rows], out_hbm.at[rows], out_sem).start()
        return 0

    lax.fori_loop(0, SUB, one, 0)
    for sta in range(STA):
        for j4 in range(4):
            v = acc_ref[sta, j4]
            v = (v + swap(v)) * (1.0 / SUB)
            int_ref[pl.ds(sta * 16 + j4, 4, stride=4), :] = v[0:4]
    pltpu.make_async_copy(out_ref, out_hbm, out_sem).wait()


VM = pl.BlockSpec(memory_space=pltpu.VMEM)
SM = pl.BlockSpec(memory_space=pltpu.SMEM)
ANY = pl.BlockSpec(memory_space=pl.ANY)
HBM = pl.BlockSpec(memory_space=pltpu.HBM)


def shards(voltages, beam_weights, station_delays, dm_index):
    w1, w2 = dft_tables()
    big, small, inner = twist_tables()
    moved = pl.pallas_call(
        kernel,
        out_shape=pltpu.VMEM((128, 17, 128), jnp.int32),
        in_specs=[HBM] * 9,
        out_specs=ANY,
        scratch_shapes=[
            pltpu.SMEM((8,), jnp.int32),
            pltpu.SMEM((4,), jnp.int32),
            pltpu.VMEM((1, 2, 32, 64), BF16),
            pltpu.VMEM((1, 2, 8, N), BF16),
            pltpu.VMEM((256, 256), BF16),
            pltpu.VMEM((128, 256), BF16),
            pltpu.VMEM((2, 8, 128), F32),
            pltpu.VMEM((2, 64, 8, 128), F32),
            pltpu.VMEM((2, 8, 8, 128), F32),
            pltpu.VMEM((2, 640, 8, 128), F32),
            pltpu.VMEM((8, 16, 8192), BF16),
            pltpu.VMEM((8, 16, 8192), BF16),
            pltpu.VMEM((64, 128), BF16),
            pltpu.VMEM((64, 8, 8, 128), F32),
            pltpu.VMEM((8, 32, 16, 128), jnp.int16),
            pltpu.VMEM((8, CH, 1, 128), F32),
            pltpu.VMEM((8, 32, 16, 128), jnp.int16),
            pltpu.VMEM((8, CH, 1, 128), F32),
            pltpu.VMEM((512, 128), F32),
            pltpu.VMEM((512, 8, 128), F32),
            pltpu.VMEM((512, 256), BF16),
            pltpu.VMEM((8, 8, 8, 128), F32),
            pltpu.VMEM((64, 8, 8, 128), F32),
            pltpu.VMEM((128, 17, 128), jnp.int32),
            pltpu.SemaphoreType.DMA((LOADS + 8,)),
            pltpu.SemaphoreType.REGULAR,
            pltpu.SemaphoreType.REGULAR,
            pltpu.SemaphoreType.DMA,
            pltpu.SemaphoreType.DMA((CH,)),
            pltpu.SemaphoreType.DMA,
            pltpu.SemaphoreType.DMA((CH,)),
            pltpu.SemaphoreType.DMA,
            pltpu.SemaphoreType.DMA((CH,)),
            pltpu.SemaphoreType.DMA,
            pltpu.SemaphoreType.DMA((SUB,)),
        ],
        compiler_params=pltpu.CompilerParams(
            collective_id=0, has_side_effects=True, vmem_limit_bytes=56 * 1024 * 1024
        ),
    )(
        station_delays, dm_index.reshape(4), voltages, beam_weights,
        jnp.asarray(w1), jnp.asarray(w2), jnp.asarray(small), jnp.asarray(big), jnp.asarray(inner),
    )
    out, power = pl.pallas_call(
        assemble,
        out_shape=(jax.ShapeDtypeStruct((4096, 128), F32), jax.ShapeDtypeStruct((128, 128), F32)),
        in_specs=[VM],
        out_specs=(ANY, VM),
        scratch_shapes=[
            pltpu.VMEM((4096, 128), F32),
            pltpu.VMEM((STA, 4, 8, 128), F32),
            pltpu.SemaphoreType.DMA,
        ],
        compiler_params=pltpu.CompilerParams(vmem_limit_bytes=16 * 1024 * 1024),
    )(moved)
    return out.reshape(16, 2, 32, 1, 512), power.reshape(32, 1, 512)


def solution(mesh):
    return jax.shard_map(
        shards,
        mesh=mesh,
        in_specs=(
            P("sub", None, "sta", None),
            P("sub", None, None, None),
            P("sta"),
            P("sta", None),
        ),
        out_specs=(P(None, None, None, None, ("sub", "sta")), P(None, None, ("sub", "sta"))),
        check_vma=False,
    )
```

```python
import functools

import jax
import jax.numpy as jnp
import numpy as np
from jax import lax
from jax.experimental import pallas as pl
from jax.experimental.pallas import tpu as pltpu
from jax.sharding import PartitionSpec as P

TWO_PI = 6.283185307179586
DISPERSION = 4148808000.0
DM_STEP = 10.0
BASE_FREQ = 120.0
CHANNEL_WIDTH = 0.1953125
F32 = jnp.float32
BF16 = jnp.bfloat16
N = 65536
STA = 8
SUB = 16
INV_SQRT2 = 0.7071067811865476


MESH = pl.DeviceIdType.MESH
LOG_TOP = float(np.log2(32766.0))
CH = 8
LOADS = 8
QUARTER = LOADS // 4
HEAD_START = 13


def dft_tables():
    k = np.arange(128)
    ang = 2.0 * np.pi * ((k[:, None] * k[None, :]) % 128) / 128.0
    full = np.concatenate([np.cos(ang), np.sin(ang)], axis=1).astype(np.float32)
    hi = full.astype(jnp.bfloat16)
    lo = (full - hi.astype(np.float32)).astype(jnp.bfloat16)
    return np.concatenate([hi, hi], axis=0), lo


def twist_tables():
    at = np.arange(64)
    ka = (8 * (at % 8) + at // 8)[:, None]
    n = np.arange(1024)[None, :]
    ang = 2.0 * np.pi * (ka * n) / N
    big = np.stack([np.cos(ang), np.sin(ang)]).reshape(2, 64, 8, 128)
    kj = np.arange(8)[:, None]
    c = np.arange(128)[None, :]
    ang = 2.0 * np.pi * (kj * c) / 1024.0
    small = np.stack([np.cos(ang), np.sin(ang)])
    e = np.arange(8)
    ang = 2.0 * np.pi * (e[:, None] * e[None, :]) / 64.0
    inner = np.stack([np.cos(ang), np.sin(ang)])[..., None] * np.ones(128)
    return big.astype(np.float32), small.astype(np.float32), inner.astype(np.float32)


def sign_rows():
    row = lax.broadcasted_iota(jnp.int32, (8, 128), 0)
    return jnp.where(row < 4, 1.0, -1.0).astype(F32)


def swap(x):
    return pltpu.roll(x, 4, x.ndim - 2)


def dft8(x, sg):
    def times_j(v):
        return swap(v) * sg

    def dft4(a0, a1, a2, a3):
        t0, t1, t2, t3 = a0 + a2, a0 - a2, a1 + a3, times_j(a1 - a3)
        return t0 + t2, t1 + t3, t0 - t2, t1 - t3

    e = dft4(x[0], x[2], x[4], x[6])
    o = dft4(x[1], x[3], x[5], x[7])
    j1, j3 = times_j(o[1]), times_j(o[3])
    o = (o[0], (o[1] + j1) * INV_SQRT2, times_j(o[2]), (j3 - o[3]) * INV_SQRT2)
    return [e[k] + o[k] for k in range(4)] + [e[k] - o[k] for k in range(4)]


def cmul(x, wr, wi, sg):
    return x * wr + (swap(x) * sg) * wi


def split(x):
    hi = x.astype(BF16)
    lo = (x - hi.astype(F32)).astype(BF16)
    return hi, lo


def unpack_voltages(x_ref, xf_ref, piece):
    per = 512 // LOADS

    def body(i, _):
        for u in range(8):
            t = piece * per + i * 8 + u
            col = pl.multiple_of(t * 128, 128)
            for ri in range(2):
                v = x_ref[0, ri, :, pl.ds(col, 128)].astype(F32)
                xf_ref[ri, t + 128] = v
                if piece >= LOADS - QUARTER:
                    xf_ref[ri, t - 384] = v
        return 0

    lax.fori_loop(0, per // 8, body, 0)


def delay_setup(d_ref):
    row = lax.broadcasted_iota(jnp.int32, (8, 128), 0)
    lane = lax.broadcasted_iota(jnp.int32, (8, 128), 1)
    fine = jnp.zeros((8, 128), jnp.int32)
    starts = []
    for r in range(8):
        d = d_ref[r]
        starts.append(128 - d // 128)
        fine = jnp.where(row == r, d % 128, fine)
    return starts, [row == r for r in range(8)], (lane - fine + 128) % 128, lane >= fine


def delay_rows(setup, xf_ref, out_ref, a0, low=0, high=8):
    starts, masks, index, keep = setup

    def body(a1, _):
        t = (8 * a1 + a0) * 8
        col = pl.multiple_of((8 * a0 + a1) * 128, 128)
        done = []
        for ri in range(2):
            acc = xf_ref[ri, pl.ds(starts[0] + t - 1, 9)]
            for r in range(1, 8):
                acc = jnp.where(masks[r], xf_ref[ri, pl.ds(starts[r] + t - 1, 9)], acc)
            g = [jnp.take_along_axis(acc[u], index, axis=1) for u in range(9)]
            done.append([jnp.where(keep, g[u + 1], g[u]) for u in range(8)])
        for j in range(8):
            out_ref[j, :, pl.ds(col, 128)] = jnp.concatenate([done[0][j], done[1][j]], axis=0).astype(BF16)
        return 0

    lax.fori_loop(low, high, body, 0, unroll=2)


def one_hot(shape, hit):
    row = lax.broadcasted_iota(jnp.int32, shape, 0)
    col = lax.broadcasted_iota(jnp.int32, shape, 1)
    return jnp.where(hit(row, col), 1.0, 0.0).astype(BF16)


def stacked_weights(bw_ref):
    w0, w1 = bw_ref[0, 0], bw_ref[0, 1]
    to_real = one_hot((64, 128), lambda q, c: c == (q // 8) * 16 + q % 8)
    to_imag = one_hot((64, 128), lambda q, c: c == (q // 8) * 16 + 8 + q % 8)
    dot = functools.partial(jnp.dot, preferred_element_type=F32)
    real = (dot(w0, to_real) - dot(w1, to_imag)).astype(BF16)
    imag = (dot(w1, to_real) + dot(w0, to_imag)).astype(BF16)
    rows_real = one_hot((64, 32), lambda r, b: r == (b // 4) * 8 + b % 4)
    rows_imag = one_hot((64, 32), lambda r, b: r == (b // 4) * 8 + 4 + b % 4)
    return (dot(rows_real, real) + dot(rows_imag, imag)).astype(BF16)


def beamform(w_ref, v_ref, bm_ref, part):
    w = w_ref[...]

    def body(i, _):
        first = part * 8 + i * 4
        v = v_ref[:, :, pl.ds(pl.multiple_of(first * 128, 512), 512)].reshape(128, 512)
        out = jnp.dot(w, v, preferred_element_type=F32)
        for u in range(4):
            bm_ref[first + u] = out[:, u * 128 : (u + 1) * 128].reshape(8, 8, 128)
        return 0

    lax.fori_loop(0, 2, body, 0, unroll=2)


def inner_pass(ref, lead, twi_ref, sg):
    def body(g, _):
        at = pl.ds(g * 2, 2)
        y = dft8([ref[8 * lead + i, at] for i in range(8)], sg)
        for k in range(8):
            v = y[k]
            if k:
                v = cmul(v, twi_ref[0, lead, pl.ds(k, 1)], twi_ref[1, lead, pl.ds(k, 1)], sg)
            ref[8 * lead + k, at] = v
        return 0

    lax.fori_loop(0, 4, body, 0, unroll=4)


def power_scale(top, axes):
    top = jnp.maximum(jnp.max(top, axis=axes, keepdims=True), 1e-33)
    power = jnp.ceil(jnp.log2(top) - LOG_TOP)
    return jnp.exp2(-power), power.astype(jnp.int32)


def two_in_one(high, low):
    return (jnp.round(high).astype(jnp.int32) << 16) | (jnp.round(low).astype(jnp.int32) & 0xFFFF)


def one_of_two(words):
    return (words >> 16).astype(F32), ((words << 16) >> 16).astype(F32)


def pack(values):
    factor, power = power_scale(jnp.abs(values), (0, 1))
    q = values * factor
    return two_in_one(q[0:2], q[2:4]).reshape(16, 128), power.reshape(1, 128)


def unpack(block):
    high, low = one_of_two(block[0:16].reshape(2, 8, 128))
    return jnp.concatenate([high, low], axis=0) * jnp.exp2(block[16:17].astype(F32))


def outer_and_encode(bm_ref, k0, sta, twb_ref, sg, q_ref):
    for g in range(4):
        at = pl.ds(2 * g, 2)
        y = dft8([bm_ref[8 * i + k0, at] for i in range(8)], sg)
        out = []
        for k1 in range(8):
            k = 8 * k0 + k1
            out.append(cmul(y[k1], twb_ref[0, k, pl.ds(sta, 1)], twb_ref[1, k, pl.ds(sta, 1)], sg))
        factor, power = power_scale(functools.reduce(jnp.maximum, [jnp.abs(v) for v in out]), 1)
        for m in range(4):
            q_ref[at, k0, 8 * m : 8 * m + 8] = two_in_one(out[2 * m] * factor, out[2 * m + 1] * factor)
        q_ref[at, k0, 32:33] = power


def chirp_table(dm_ref, base_ref, h_ref, first, last):
    row = lax.broadcasted_iota(jnp.int32, (8, 128), 0)
    lane = lax.broadcasted_iota(jnp.int32, (8, 128), 1)
    centre = BASE_FREQ + CHANNEL_WIDTH * (
        jnp.zeros((8, 128), F32) + lax.axis_index("sub").astype(F32) + 0.5
    )

    def base(i, _):
        k0, kj = i // 8, i % 8
        positions = 8 * row + k0 + 64 * kj + 512 * lane
        signed_bin = jnp.where(positions < N // 2, positions, positions - N)
        offset = CHANNEL_WIDTH * signed_bin.astype(F32) / N
        base_ref[pl.ds(pl.multiple_of(i * 8, 8), 8), :] = (
            TWO_PI * DISPERSION * offset * offset / (centre * centre * (centre + offset))
        )
        return 0

    lax.fori_loop(first * 4, last * 4, base, 0)
    quarter = jnp.where(row < 4, 1, 0)
    dm = jnp.zeros((8, 128), F32)
    for b in range(4):
        dm = jnp.where(row % 4 == b, DM_STEP * dm_ref[b].astype(F32), dm)
    p1 = 1.5703125
    p2 = float(np.float32(np.round((np.pi / 2 - p1) * 2.0**22) / 2.0**22))
    p3 = float(np.float32(np.pi / 2 - p1 - p2))

    def one(r):
        phase = dm * base_ref[pl.ds(r, 1), :]
        n = jnp.floor(phase * float(2.0 / np.pi) + 0.5)
        y = ((phase - n * p1) - n * p2) - n * p3
        q = n.astype(jnp.int32) + quarter
        z = y * y
        s = ((-1.9515295891e-4 * z + 8.3321608736e-3) * z - 1.6666654611e-1) * z * y + y
        c = ((2.443315711809948e-5 * z - 1.388731625493765e-3) * z + 4.166664568298827e-2) * z * z - 0.5 * z + 1.0
        v = jnp.where((q & 1) == 0, s, c)
        h_ref[r] = jnp.where((q & 2) == 0, v, -v)

    def body(i, _):
        for u in range(4):
            one(i * 4 + u)
        return 0

    lax.fori_loop(first * 8, last * 8, body, 0)


def middle(k0, r_ref, h_ref, w1_ref, w2_ref, tws_ref, twb_ref, xs_ref, gt_ref, g_ref, sg):
    scales = [jnp.exp2(r_ref[j, k0, 32:33].astype(F32)) for j in range(8)]
    for m in range(4):
        x = [jnp.stack(one_of_two(r_ref[j, k0, 8 * m : 8 * m + 8])) * scales[j] for j in range(8)]
        y = dft8(x, sg)
        for kj in range(8):
            v = y[kj]
            if kj:
                v = cmul(v, tws_ref[0, pl.ds(kj, 1)], tws_ref[1, pl.ds(kj, 1)], sg)
            hi, lo = split(v.reshape(16, 128))
            at = kj * 64 + m * 16
            xs_ref[at : at + 16, 0:128] = hi
            xs_ref[at : at + 16, 128:256] = lo

    def dot128(sign):
        x = xs_ref[...]
        pq = jnp.dot(x, w1_ref[...], preferred_element_type=F32)
        pq = pq + jnp.dot(x[:, 0:128], w2_ref[...], preferred_element_type=F32)
        return pq[:, 0:128].reshape(64, 8, 128) + swap(pq[:, 128:256].reshape(64, 8, 128)) * sign

    low = lax.broadcasted_iota(jnp.int32, (8, 128), 0) < 4
    v = dot128(sg)
    h = h_ref[pl.ds(k0 * 64, 64)]
    hs = swap(h)
    v = v * jnp.where(low, h, hs) + swap(v) * jnp.where(low, -hs, h)
    hi, lo = split(v.reshape(512, 128))
    xs_ref[:, 0:128] = hi
    xs_ref[:, 128:256] = lo
    gt_ref[...] = dot128(-sg).reshape(8, 8, 8, 128)

    for i in range(4):
        x = []
        for kj in range(8):
            v = gt_ref[kj, 2 * i : 2 * i + 2]
            if kj:
                v = cmul(v, tws_ref[0, pl.ds(kj, 1)], tws_ref[1, pl.ds(kj, 1)], -sg)
            x.append(v)
        y = dft8(x, -sg)
        here = pl.ds(k0 * 8 + i * 2, 2)
        for j in range(8):
            g_ref[here, j] = cmul(y[j], twb_ref[0, here, pl.ds(j, 1)], twb_ref[1, here, pl.ds(j, 1)], -sg)


EARLY_Z, LATE_Z = (0, 1), (2, 3)


def kernel(
    d_hbm, dm_hbm, x_hbm, bw_hbm, w1_hbm, w2_hbm, tws_hbm, twb_hbm, twi_hbm,
    recv3,
    d_ref, dm_ref, bw_ref, x_ref, w1_ref, w2_ref, tws_ref, twb_ref, twi_ref,
    xf_ref, send1, recv1, w_ref, bm_ref, send2, recv2, base_ref, h_ref, xs_ref, gt_ref, g_ref,
    send3,
    load_sem, answer_sem, col_sem, sem1, rsem1, sem2, rsem2, sem3, rsem3,
):
    sub, sta = lax.axis_index("sub"), lax.axis_index("sta")
    me = sub * STA + sta

    x_loads = []
    for i in range(LOADS):
        cols = pl.ds(i * (N // LOADS), N // LOADS)
        x_loads.append(pltpu.make_async_copy(x_hbm.at[:, :, :, cols], x_ref.at[:, :, :, cols], load_sem.at[i]))
    tables = [
        pltpu.make_async_copy(a, b, load_sem.at[LOADS + i])
        for i, (a, b) in enumerate(
            [
                (d_hbm, d_ref), (dm_hbm, dm_ref), (bw_hbm, bw_ref), (w1_hbm, w1_ref), (w2_hbm, w2_ref),
                (tws_hbm, tws_ref), (twb_hbm, twb_ref), (twi_hbm, twi_ref),
            ]
        )
    ]
    order = [(i - QUARTER) % LOADS for i in range(LOADS)]
    for t in tables[:1] + [x_loads[i] for i in order] + tables[1:2]:
        t.start()

    barrier = pltpu.get_barrier_semaphore()
    for i in range(1, STA):
        pl.semaphore_signal(barrier, inc=1, device_id={"sub": sub, "sta": (sta + i) % STA}, device_id_type=MESH)
    x_hi, z, core = sub // 8, (sub // 2) % 4, sub % 2
    rank = 4 * z + 2 * x_hi + core

    def column(r):
        return {"sub": 8 * ((r // 2) % 2) + 2 * (r // 4) + r % 2, "sta": sta}

    def greet(r, _):
        pl.semaphore_signal(barrier, inc=1, device_id=column(r), device_id_type=MESH)
        return 0

    lax.fori_loop(rank + 1, SUB, greet, 0)
    def load(pieces):
        for i in pieces:
            x_loads[i].wait()
            unpack_voltages(x_ref, xf_ref, i)

    tables[0].wait()
    setup = delay_setup(d_ref)
    load(order[:QUARTER])

    def first(part, start, size):
        cols = pl.ds(pl.multiple_of(start, size), size)
        for i in range(1, STA):
            d = (sta + i) % STA
            pltpu.make_async_remote_copy(
                src_ref=send1.at[d, :, cols],
                dst_ref=recv1.at[sta, :, cols],
                send_sem=sem1,
                recv_sem=rsem1.at[part],
                device_id={"sub": sub, "sta": d},
                device_id_type=MESH,
            ).start()
        pltpu.make_async_copy(send1.at[sta, :, cols], recv1.at[sta, :, cols], rsem1.at[part]).start()

    tables[1].wait()
    late = HEAD_START * (1 - (sub % 2))
    chirp_table(dm_ref, base_ref, h_ref, 0, late)
    load(order[QUARTER:])
    delay_rows(setup, xf_ref, send1, 0)
    pl.semaphore_wait(barrier, STA - 1 + rank)
    first(0, 0, 1024)
    for t in tables[2:]:
        t.start()

    def answer(r, _):
        pl.semaphore_signal(answer_sem, inc=1, device_id=column(r), device_id_type=MESH)
        return 0

    lax.fori_loop(0, rank, answer, 0)

    def more(part, _):
        delay_rows(setup, xf_ref, send1, part)
        first(part, part * 1024, 1024)
        return 0

    lax.fori_loop(1, CH, more, 0)

    for t in tables[2:]:
        t.wait()
    w_ref[...] = stacked_weights(bw_ref)
    chirp_table(dm_ref, base_ref, h_ref, late, 16)
    @pl.when(rank < SUB - 1)
    def _():
        pl.semaphore_wait(answer_sem, SUB - 1 - rank)

    for i in range(1, STA):
        pl.semaphore_signal(col_sem, inc=1, device_id={"sub": sub, "sta": (sta + i) % STA}, device_id_type=MESH)
    sg = sign_rows()

    def beams(part, _):
        cols = pl.ds(pl.multiple_of(part * 1024, 1024), 1024)
        pltpu.make_async_copy(recv1.at[:, :, cols], recv1.at[:, :, cols], rsem1.at[part]).wait()
        beamform(w_ref, recv1, bm_ref, part)
        inner_pass(bm_ref, part, twi_ref, sg)
        return 0

    lax.fori_loop(0, CH, beams, 0)

    def second(part, _):
        outer_and_encode(bm_ref, part, sta, twb_ref, sg, send2)
        for i in range(1, STA):
            d = (sta + i) % STA
            pltpu.make_async_remote_copy(
                src_ref=send2.at[d, part],
                dst_ref=recv2.at[sta, part],
                send_sem=sem2,
                recv_sem=rsem2.at[part],
                device_id={"sub": sub, "sta": d},
                device_id_type=MESH,
            ).start()
        pltpu.make_async_copy(send2.at[sta, part], recv2.at[sta, part], rsem2.at[part]).start()
        return 0

    lax.fori_loop(0, CH, second, 0)

    def spectra(part, _):
        pltpu.make_async_copy(recv2.at[:, part], recv2.at[:, part], rsem2.at[part]).wait()
        middle(part, recv2, h_ref, w1_ref, w2_ref, tws_ref, twb_ref, xs_ref, gt_ref, g_ref, sg)
        inner_pass(g_ref, part, twi_ref, -sg)
        return 0

    lax.fori_loop(0, CH, spectra, 0)

    pl.semaphore_wait(col_sem, STA - 1)
    x_lo, yh, jh_own = sta // 4, (sta // 2) % 2, sta % 2

    def group_of(i):
        return 4 * ((core + 1 - i // 4) % 2) + 2 * ((x_lo + 1 - (i // 2) % 2) % 2) + (yh + 1 - i % 2) % 2

    def copies(a0, planes):
        for n, z_to in enumerate(planes * 4):
            dx, dj = 1 - n // (2 * len(planes)), 1 - (n // len(planes)) % 2
            d = 64 * ((x_hi + dx) % 2) + 16 * z_to + 2 * a0 + (jh_own + dj) % 2

            def go():
                pltpu.make_async_remote_copy(
                    src_ref=send3.at[d],
                    dst_ref=recv3.at[me],
                    send_sem=sem3,
                    recv_sem=rsem3.at[sub],
                    device_id={"sub": d // STA, "sta": d % STA},
                    device_id_type=MESH,
                ).start()

            if dx or dj:
                go()
            else:
                pl.when(d != me)(go)

                @pl.when(d == me)
                def _():
                    pltpu.make_async_copy(send3.at[me], recv3.at[me], rsem3.at[sub]).start()

    def group(i, _):
        a0 = group_of(i)
        for jh in range(2):
            y = dft8([g_ref[8 * k0 + a0, pl.ds(4 * jh, 4)] for k0 in range(8)], -sg)
            for a1 in range(8):
                d = 16 * a1 + 2 * a0 + jh
                send3[d, 0:16], send3[d, 16:17] = pack(y[a1] * (1.0 / N))
        copies(a0, EARLY_Z)
        return 0

    lax.fori_loop(0, 8, group, 0)

    def rest(i, _):
        copies(group_of(i), LATE_Z)
        return 0

    lax.fori_loop(0, 8, rest, 0)

    for s in range(SUB):
        block = recv3.at[pl.ds(s * STA, STA)]
        pltpu.make_async_copy(block, block, rsem3.at[s]).wait()
    others = pl.ds(0, STA - 1)
    pltpu.make_async_copy(send1.at[others], send1.at[others], sem1).wait()
    pltpu.make_async_copy(send2.at[others], send2.at[others], sem2).wait()
    others = pl.ds(0, SUB * STA - 1)
    pltpu.make_async_copy(send3.at[others], send3.at[others], sem3).wait()


def assemble(q_ref, out_hbm, int_ref, out_ref, acc_ref, out_sem):
    acc_ref[...] = jnp.zeros_like(acc_ref)

    def one(s, _):
        for sta in range(STA):
            src = s * STA + sta
            v = unpack(q_ref[src])
            acc_ref[sta] += v * v
            for j4 in range(4):
                for ri in range(2):
                    first = s * 256 + (ri * 128 + sta * 16 + j4)
                    out_ref[pl.ds(first, 4, stride=4), :] = v[j4, 4 * ri : 4 * ri + 4]
        rows = pl.ds(pl.multiple_of(s * 256, 256), 256)
        pltpu.make_async_copy(out_ref.at[rows], out_hbm.at[rows], out_sem).start()
        return 0

    lax.fori_loop(0, SUB, one, 0)
    for sta in range(STA):
        for j4 in range(4):
            v = acc_ref[sta, j4]
            v = (v + swap(v)) * (1.0 / SUB)
            int_ref[pl.ds(sta * 16 + j4, 4, stride=4), :] = v[0:4]
    pltpu.make_async_copy(out_ref, out_hbm, out_sem).wait()


VM = pl.BlockSpec(memory_space=pltpu.VMEM)
SM = pl.BlockSpec(memory_space=pltpu.SMEM)
ANY = pl.BlockSpec(memory_space=pl.ANY)
HBM = pl.BlockSpec(memory_space=pltpu.HBM)


def shards(voltages, beam_weights, station_delays, dm_index):
    w1, w2 = dft_tables()
    big, small, inner = twist_tables()
    moved = pl.pallas_call(
        kernel,
        out_shape=pltpu.VMEM((128, 17, 128), jnp.int32),
        in_specs=[HBM] * 9,
        out_specs=ANY,
        scratch_shapes=[
            pltpu.SMEM((8,), jnp.int32),
            pltpu.SMEM((4,), jnp.int32),
            pltpu.VMEM((1, 2, 32, 64), BF16),
            pltpu.VMEM((1, 2, 8, N), BF16),
            pltpu.VMEM((256, 256), BF16),
            pltpu.VMEM((128, 256), BF16),
            pltpu.VMEM((2, 8, 128), F32),
            pltpu.VMEM((2, 64, 8, 128), F32),
            pltpu.VMEM((2, 8, 8, 128), F32),
            pltpu.VMEM((2, 640, 8, 128), F32),
            pltpu.VMEM((8, 16, 8192), BF16),
            pltpu.VMEM((8, 16, 8192), BF16),
            pltpu.VMEM((64, 128), BF16),
            pltpu.VMEM((64, 8, 8, 128), F32),
            pltpu.VMEM((8, CH, 33, 128), jnp.int32),
            pltpu.VMEM((8, CH, 33, 128), jnp.int32),
            pltpu.VMEM((512, 128), F32),
            pltpu.VMEM((512, 8, 128), F32),
            pltpu.VMEM((512, 256), BF16),
            pltpu.VMEM((8, 8, 8, 128), F32),
            pltpu.VMEM((64, 8, 8, 128), F32),
            pltpu.VMEM((128, 17, 128), jnp.int32),
            pltpu.SemaphoreType.DMA((LOADS + 8,)),
            pltpu.SemaphoreType.REGULAR,
            pltpu.SemaphoreType.REGULAR,
            pltpu.SemaphoreType.DMA,
            pltpu.SemaphoreType.DMA((CH,)),
            pltpu.SemaphoreType.DMA,
            pltpu.SemaphoreType.DMA((CH,)),
            pltpu.SemaphoreType.DMA,
            pltpu.SemaphoreType.DMA((SUB,)),
        ],
        compiler_params=pltpu.CompilerParams(
            collective_id=0, has_side_effects=True, vmem_limit_bytes=56 * 1024 * 1024
        ),
    )(
        station_delays, dm_index.reshape(4), voltages, beam_weights,
        jnp.asarray(w1), jnp.asarray(w2), jnp.asarray(small), jnp.asarray(big), jnp.asarray(inner),
    )
    out, power = pl.pallas_call(
        assemble,
        out_shape=(jax.ShapeDtypeStruct((4096, 128), F32), jax.ShapeDtypeStruct((128, 128), F32)),
        in_specs=[VM],
        out_specs=(ANY, VM),
        scratch_shapes=[
            pltpu.VMEM((4096, 128), F32),
            pltpu.VMEM((STA, 4, 8, 128), F32),
            pltpu.SemaphoreType.DMA,
        ],
        compiler_params=pltpu.CompilerParams(vmem_limit_bytes=16 * 1024 * 1024),
    )(moved)
    return out.reshape(16, 2, 32, 1, 512), power.reshape(32, 1, 512)


def solution(mesh):
    return jax.shard_map(
        shards,
        mesh=mesh,
        in_specs=(
            P("sub", None, "sta", None),
            P("sub", None, None, None),
            P("sta"),
            P("sta", None),
        ),
        out_specs=(P(None, None, None, None, ("sub", "sta")), P(None, None, ("sub", "sta"))),
        check_vma=False,
    )
```

```python
import functools

import jax
import jax.numpy as jnp
import numpy as np
from jax import lax
from jax.experimental import pallas as pl
from jax.experimental.pallas import tpu as pltpu
from jax.sharding import PartitionSpec as P

TWO_PI = 6.283185307179586
DISPERSION = 4148808000.0
DM_STEP = 10.0
BASE_FREQ = 120.0
CHANNEL_WIDTH = 0.1953125
F32 = jnp.float32
BF16 = jnp.bfloat16
N = 65536
STA = 8
SUB = 16
INV_SQRT2 = 0.7071067811865476


MESH = pl.DeviceIdType.MESH
LOG_TOP = float(np.log2(32640.0))
CH = 8
LOADS = 8
QUARTER = LOADS // 4
HEAD_START = 13


def dft_tables():
    k = np.arange(128)
    ang = 2.0 * np.pi * ((k[:, None] * k[None, :]) % 128) / 128.0
    full = np.concatenate([np.cos(ang), np.sin(ang)], axis=1).astype(np.float32)
    hi = full.astype(jnp.bfloat16)
    lo = (full - hi.astype(np.float32)).astype(jnp.bfloat16)
    return np.concatenate([hi, hi], axis=0), lo


def twist_tables():
    at = np.arange(64)
    ka = (8 * (at % 8) + at // 8)[:, None]
    n = np.arange(1024)[None, :]
    ang = 2.0 * np.pi * (ka * n) / N
    big = np.stack([np.cos(ang), np.sin(ang)]).reshape(2, 64, 8, 128)
    kj = np.arange(8)[:, None]
    c = np.arange(128)[None, :]
    ang = 2.0 * np.pi * (kj * c) / 1024.0
    small = np.stack([np.cos(ang), np.sin(ang)])
    e = np.arange(8)
    ang = 2.0 * np.pi * (e[:, None] * e[None, :]) / 64.0
    inner = np.stack([np.cos(ang), np.sin(ang)])[..., None] * np.ones(128)
    return big.astype(np.float32), small.astype(np.float32), inner.astype(np.float32)


def sign_rows():
    row = lax.broadcasted_iota(jnp.int32, (8, 128), 0)
    return jnp.where(row < 4, 1.0, -1.0).astype(F32)


def swap(x):
    return pltpu.roll(x, 4, x.ndim - 2)


def dft8(x, sg):
    def times_j(v):
        return swap(v) * sg

    def dft4(a0, a1, a2, a3):
        t0, t1, t2, t3 = a0 + a2, a0 - a2, a1 + a3, times_j(a1 - a3)
        return t0 + t2, t1 + t3, t0 - t2, t1 - t3

    e = dft4(x[0], x[2], x[4], x[6])
    o = dft4(x[1], x[3], x[5], x[7])
    j1, j3 = times_j(o[1]), times_j(o[3])
    o = (o[0], (o[1] + j1) * INV_SQRT2, times_j(o[2]), (j3 - o[3]) * INV_SQRT2)
    return [e[k] + o[k] for k in range(4)] + [e[k] - o[k] for k in range(4)]


def cmul(x, wr, wi, sg):
    return x * wr + (swap(x) * sg) * wi


def split(x):
    hi = x.astype(BF16)
    lo = (x - hi.astype(F32)).astype(BF16)
    return hi, lo


def unpack_voltages(x_ref, xf_ref, piece):
    per = 512 // LOADS

    def body(i, _):
        for u in range(8):
            t = piece * per + i * 8 + u
            col = pl.multiple_of(t * 128, 128)
            for ri in range(2):
                v = x_ref[0, ri, :, pl.ds(col, 128)].astype(F32)
                xf_ref[ri, t + 128] = v
                if piece >= LOADS - QUARTER:
                    xf_ref[ri, t - 384] = v
        return 0

    lax.fori_loop(0, per // 8, body, 0)


def delay_setup(d_ref):
    row = lax.broadcasted_iota(jnp.int32, (8, 128), 0)
    lane = lax.broadcasted_iota(jnp.int32, (8, 128), 1)
    fine = jnp.zeros((8, 128), jnp.int32)
    starts = []
    for r in range(8):
        d = d_ref[r]
        starts.append(128 - d // 128)
        fine = jnp.where(row == r, d % 128, fine)
    return starts, [row == r for r in range(8)], (lane - fine + 128) % 128, lane >= fine


def delay_rows(setup, xf_ref, out_ref, a0, low=0, high=8):
    starts, masks, index, keep = setup

    def body(a1, _):
        t = (8 * a1 + a0) * 8
        col = pl.multiple_of((8 * a0 + a1) * 128, 128)
        done = []
        for ri in range(2):
            acc = xf_ref[ri, pl.ds(starts[0] + t - 1, 9)]
            for r in range(1, 8):
                acc = jnp.where(masks[r], xf_ref[ri, pl.ds(starts[r] + t - 1, 9)], acc)
            g = [jnp.take_along_axis(acc[u], index, axis=1) for u in range(9)]
            done.append([jnp.where(keep, g[u + 1], g[u]) for u in range(8)])
        for j in range(8):
            out_ref[j, :, pl.ds(col, 128)] = jnp.concatenate([done[0][j], done[1][j]], axis=0).astype(BF16)
        return 0

    lax.fori_loop(low, high, body, 0, unroll=2)


def one_hot(shape, hit):
    row = lax.broadcasted_iota(jnp.int32, shape, 0)
    col = lax.broadcasted_iota(jnp.int32, shape, 1)
    return jnp.where(hit(row, col), 1.0, 0.0).astype(BF16)


def stacked_weights(bw_ref):
    w0, w1 = bw_ref[0, 0], bw_ref[0, 1]
    to_real = one_hot((64, 128), lambda q, c: c == (q // 8) * 16 + q % 8)
    to_imag = one_hot((64, 128), lambda q, c: c == (q // 8) * 16 + 8 + q % 8)
    dot = functools.partial(jnp.dot, preferred_element_type=F32)
    real = (dot(w0, to_real) - dot(w1, to_imag)).astype(BF16)
    imag = (dot(w1, to_real) + dot(w0, to_imag)).astype(BF16)
    rows_real = one_hot((64, 32), lambda r, b: r == (b // 4) * 8 + b % 4)
    rows_imag = one_hot((64, 32), lambda r, b: r == (b // 4) * 8 + 4 + b % 4)
    return (dot(rows_real, real) + dot(rows_imag, imag)).astype(BF16)


def beamform(w_ref, v_ref, bm_ref, part):
    w = w_ref[...]

    def body(i, _):
        first = part * 8 + i * 4
        v = v_ref[:, :, pl.ds(pl.multiple_of(first * 128, 512), 512)].reshape(128, 512)
        out = jnp.dot(w, v, preferred_element_type=F32)
        for u in range(4):
            bm_ref[first + u] = out[:, u * 128 : (u + 1) * 128].reshape(8, 8, 128)
        return 0

    lax.fori_loop(0, 2, body, 0, unroll=2)


def inner_pass(ref, lead, twi_ref, sg):
    def body(g, _):
        at = pl.ds(g * 2, 2)
        y = dft8([ref[8 * lead + i, at] for i in range(8)], sg)
        for k in range(8):
            v = y[k]
            if k:
                v = cmul(v, twi_ref[0, lead, pl.ds(k, 1)], twi_ref[1, lead, pl.ds(k, 1)], sg)
            ref[8 * lead + k, at] = v
        return 0

    lax.fori_loop(0, 4, body, 0, unroll=4)


def power_scale(top, axes):
    top = jnp.maximum(jnp.max(top, axis=axes, keepdims=True), 1e-33)
    power = jnp.ceil(jnp.log2(top) - LOG_TOP)
    return jnp.exp2(-power), power.astype(jnp.int32)


def two_in_one(high, low):
    return (jnp.round(high).astype(jnp.int32) << 16) | (jnp.round(low).astype(jnp.int32) & 0xFFFF)


def one_of_two(words):
    return (words >> 16).astype(F32), ((words << 16) >> 16).astype(F32)


def pack(values):
    factor, power = power_scale(jnp.abs(values), (0, 1))
    q = values * factor
    return two_in_one(q[0:2], q[2:4]).reshape(16, 128), power.reshape(1, 128)


def unpack(block):
    high, low = one_of_two(block[0:16].reshape(2, 8, 128))
    return jnp.concatenate([high, low], axis=0) * jnp.exp2(block[16:17].astype(F32))


def outer_and_encode(bm_ref, k0, sta, twb_ref, sg, q_ref):
    for g in range(4):
        at = pl.ds(2 * g, 2)
        y = dft8([bm_ref[8 * i + k0, at] for i in range(8)], sg)
        out = []
        for k1 in range(8):
            k = 8 * k0 + k1
            out.append(cmul(y[k1], twb_ref[0, k, pl.ds(sta, 1)], twb_ref[1, k, pl.ds(sta, 1)], sg))
        factor, power = power_scale(functools.reduce(jnp.maximum, [jnp.abs(v) for v in out]), 1)
        for m in range(4):
            q_ref[at, k0, 8 * m : 8 * m + 8] = two_in_one(out[2 * m] * factor, out[2 * m + 1] * factor)
        q_ref[at, k0, 32:33] = power


def chirp_table(dm_ref, base_ref, h_ref, first, last):
    row = lax.broadcasted_iota(jnp.int32, (8, 128), 0)
    lane = lax.broadcasted_iota(jnp.int32, (8, 128), 1)
    centre = BASE_FREQ + CHANNEL_WIDTH * (
        jnp.zeros((8, 128), F32) + lax.axis_index("sub").astype(F32) + 0.5
    )

    def base(i, _):
        k0, kj = i // 8, i % 8
        positions = 8 * row + k0 + 64 * kj + 512 * lane
        signed_bin = jnp.where(positions < N // 2, positions, positions - N)
        offset = CHANNEL_WIDTH * signed_bin.astype(F32) / N
        base_ref[pl.ds(pl.multiple_of(i * 8, 8), 8), :] = (
            TWO_PI * DISPERSION * offset * offset / (centre * centre * (centre + offset))
        )
        return 0

    lax.fori_loop(first * 4, last * 4, base, 0)
    quarter = jnp.where(row < 4, 1, 0)
    dm = jnp.zeros((8, 128), F32)
    for b in range(4):
        dm = jnp.where(row % 4 == b, DM_STEP * dm_ref[b].astype(F32), dm)
    p1 = 1.5703125
    p2 = float(np.float32(np.round((np.pi / 2 - p1) * 2.0**22) / 2.0**22))
    p3 = float(np.float32(np.pi / 2 - p1 - p2))

    def one(r):
        phase = dm * base_ref[pl.ds(r, 1), :]
        n = jnp.floor(phase * float(2.0 / np.pi) + 0.5)
        y = ((phase - n * p1) - n * p2) - n * p3
        q = n.astype(jnp.int32) + quarter
        z = y * y
        s = ((-1.9515295891e-4 * z + 8.3321608736e-3) * z - 1.6666654611e-1) * z * y + y
        c = ((2.443315711809948e-5 * z - 1.388731625493765e-3) * z + 4.166664568298827e-2) * z * z - 0.5 * z + 1.0
        v = jnp.where((q & 1) == 0, s, c)
        h_ref[r] = jnp.where((q & 2) == 0, v, -v)

    def body(i, _):
        for u in range(4):
            one(i * 4 + u)
        return 0

    lax.fori_loop(first * 8, last * 8, body, 0)


def middle(k0, r_ref, h_ref, w1_ref, w2_ref, tws_ref, twb_ref, xs_ref, gt_ref, g_ref, sg):
    scales = [jnp.exp2(r_ref[j, k0, 32:33].astype(F32)) for j in range(8)]
    for m in range(4):
        x = [jnp.stack(one_of_two(r_ref[j, k0, 8 * m : 8 * m + 8])) * scales[j] for j in range(8)]
        y = dft8(x, sg)
        for kj in range(8):
            v = y[kj]
            if kj:
                v = cmul(v, tws_ref[0, pl.ds(kj, 1)], tws_ref[1, pl.ds(kj, 1)], sg)
            hi, lo = split(v.reshape(16, 128))
            at = kj * 64 + m * 16
            xs_ref[at : at + 16, 0:128] = hi
            xs_ref[at : at + 16, 128:256] = lo

    def dot128(sign):
        x = xs_ref[...]
        pq = jnp.dot(x, w1_ref[...], preferred_element_type=F32)
        pq = pq + jnp.dot(x[:, 0:128], w2_ref[...], preferred_element_type=F32)
        return pq[:, 0:128].reshape(64, 8, 128) + swap(pq[:, 128:256].reshape(64, 8, 128)) * sign

    low = lax.broadcasted_iota(jnp.int32, (8, 128), 0) < 4
    v = dot128(sg)
    h = h_ref[pl.ds(k0 * 64, 64)]
    hs = swap(h)
    v = v * jnp.where(low, h, hs) + swap(v) * jnp.where(low, -hs, h)
    hi, lo = split(v.reshape(512, 128))
    xs_ref[:, 0:128] = hi
    xs_ref[:, 128:256] = lo
    gt_ref[...] = dot128(-sg).reshape(8, 8, 8, 128)

    for i in range(4):
        x = []
        for kj in range(8):
            v = gt_ref[kj, 2 * i : 2 * i + 2]
            if kj:
                v = cmul(v, tws_ref[0, pl.ds(kj, 1)], tws_ref[1, pl.ds(kj, 1)], -sg)
            x.append(v)
        y = dft8(x, -sg)
        here = pl.ds(k0 * 8 + i * 2, 2)
        for j in range(8):
            g_ref[here, j] = cmul(y[j], twb_ref[0, here, pl.ds(j, 1)], twb_ref[1, here, pl.ds(j, 1)], -sg)


EARLY_Z, LATE_Z = (0, 1), (2, 3)


def kernel(
    d_hbm, dm_hbm, x_hbm, bw_hbm, w1_hbm, w2_hbm, tws_hbm, twb_hbm, twi_hbm,
    recv3,
    d_ref, dm_ref, bw_ref, x_ref, w1_ref, w2_ref, tws_ref, twb_ref, twi_ref,
    xf_ref, send1, recv1, w_ref, bm_ref, send2, recv2, base_ref, h_ref, xs_ref, gt_ref, g_ref,
    send3,
    load_sem, answer_sem, col_sem, sem1, rsem1, sem2, rsem2, sem3, rsem3,
):
    sub, sta = lax.axis_index("sub"), lax.axis_index("sta")
    me = sub * STA + sta

    x_loads = []
    for i in range(LOADS):
        cols = pl.ds(i * (N // LOADS), N // LOADS)
        x_loads.append(pltpu.make_async_copy(x_hbm.at[:, :, :, cols], x_ref.at[:, :, :, cols], load_sem.at[i]))
    tables = [
        pltpu.make_async_copy(a, b, load_sem.at[LOADS + i])
        for i, (a, b) in enumerate(
            [
                (d_hbm, d_ref), (dm_hbm, dm_ref), (bw_hbm, bw_ref), (w1_hbm, w1_ref), (w2_hbm, w2_ref),
                (tws_hbm, tws_ref), (twb_hbm, twb_ref), (twi_hbm, twi_ref),
            ]
        )
    ]
    order = [(i - QUARTER) % LOADS for i in range(LOADS)]
    for t in tables[:1] + [x_loads[i] for i in order] + tables[1:2]:
        t.start()

    barrier = pltpu.get_barrier_semaphore()
    for i in range(1, STA):
        pl.semaphore_signal(barrier, inc=1, device_id={"sub": sub, "sta": (sta + i) % STA}, device_id_type=MESH)
    x_hi, z, core = sub // 8, (sub // 2) % 4, sub % 2
    rank = 4 * z + 2 * x_hi + core

    def column(r):
        return {"sub": 8 * ((r // 2) % 2) + 2 * (r // 4) + r % 2, "sta": sta}

    def greet(r, _):
        pl.semaphore_signal(barrier, inc=1, device_id=column(r), device_id_type=MESH)
        return 0

    lax.fori_loop(rank + 1, SUB, greet, 0)
    def load(pieces):
        for i in pieces:
            x_loads[i].wait()
            unpack_voltages(x_ref, xf_ref, i)

    tables[0].wait()
    setup = delay_setup(d_ref)
    load(order[:QUARTER])

    def first(part, start, size):
        cols = pl.ds(pl.multiple_of(start, size), size)
        for i in range(1, STA):
            d = (sta + i) % STA
            pltpu.make_async_remote_copy(
                src_ref=send1.at[d, :, cols],
                dst_ref=recv1.at[sta, :, cols],
                send_sem=sem1,
                recv_sem=rsem1.at[part],
                device_id={"sub": sub, "sta": d},
                device_id_type=MESH,
            ).start()
        pltpu.make_async_copy(send1.at[sta, :, cols], recv1.at[sta, :, cols], rsem1.at[part]).start()

    tables[1].wait()
    late = HEAD_START * (1 - (sub % 2))
    chirp_table(dm_ref, base_ref, h_ref, 0, late)
    load(order[QUARTER:])
    delay_rows(setup, xf_ref, send1, 0)
    pl.semaphore_wait(barrier, STA - 1 + rank)
    first(0, 0, 1024)
    for t in tables[2:]:
        t.start()

    def answer(r, _):
        pl.semaphore_signal(answer_sem, inc=1, device_id=column(r), device_id_type=MESH)
        return 0

    lax.fori_loop(0, rank, answer, 0)

    def more(part, _):
        delay_rows(setup, xf_ref, send1, part)
        first(part, part * 1024, 1024)
        return 0

    lax.fori_loop(1, CH, more, 0)

    for t in tables[2:]:
        t.wait()
    w_ref[...] = stacked_weights(bw_ref)
    chirp_table(dm_ref, base_ref, h_ref, late, 16)
    @pl.when(rank < SUB - 1)
    def _():
        pl.semaphore_wait(answer_sem, SUB - 1 - rank)

    for i in range(1, STA):
        pl.semaphore_signal(col_sem, inc=1, device_id={"sub": sub, "sta": (sta + i) % STA}, device_id_type=MESH)
    sg = sign_rows()

    def beams(part, _):
        cols = pl.ds(pl.multiple_of(part * 1024, 1024), 1024)
        pltpu.make_async_copy(recv1.at[:, :, cols], recv1.at[:, :, cols], rsem1.at[part]).wait()
        beamform(w_ref, recv1, bm_ref, part)
        inner_pass(bm_ref, part, twi_ref, sg)
        return 0

    lax.fori_loop(0, CH, beams, 0)

    def second(part, _):
        outer_and_encode(bm_ref, part, sta, twb_ref, sg, send2)
        for i in range(1, STA):
            d = (sta + i) % STA
            pltpu.make_async_remote_copy(
                src_ref=send2.at[d, part],
                dst_ref=recv2.at[sta, part],
                send_sem=sem2,
                recv_sem=rsem2.at[part],
                device_id={"sub": sub, "sta": d},
                device_id_type=MESH,
            ).start()
        pltpu.make_async_copy(send2.at[sta, part], recv2.at[sta, part], rsem2.at[part]).start()
        return 0

    lax.fori_loop(0, CH, second, 0)

    def spectra(part, _):
        pltpu.make_async_copy(recv2.at[:, part], recv2.at[:, part], rsem2.at[part]).wait()
        middle(part, recv2, h_ref, w1_ref, w2_ref, tws_ref, twb_ref, xs_ref, gt_ref, g_ref, sg)
        inner_pass(g_ref, part, twi_ref, -sg)
        return 0

    lax.fori_loop(0, CH, spectra, 0)

    pl.semaphore_wait(col_sem, STA - 1)
    x_lo, yh, jh_own = sta // 4, (sta // 2) % 2, sta % 2

    def group_of(i):
        return 4 * ((core + 1 - i // 4) % 2) + 2 * ((x_lo + 1 - (i // 2) % 2) % 2) + (yh + 1 - i % 2) % 2

    def copies(a0, planes):
        for n, z_to in enumerate(planes * 4):
            dx, dj = 1 - n // (2 * len(planes)), 1 - (n // len(planes)) % 2
            d = 64 * ((x_hi + dx) % 2) + 16 * z_to + 2 * a0 + (jh_own + dj) % 2

            def go():
                pltpu.make_async_remote_copy(
                    src_ref=send3.at[d],
                    dst_ref=recv3.at[me],
                    send_sem=sem3,
                    recv_sem=rsem3.at[sub],
                    device_id={"sub": d // STA, "sta": d % STA},
                    device_id_type=MESH,
                ).start()

            if dx or dj:
                go()
            else:
                pl.when(d != me)(go)

                @pl.when(d == me)
                def _():
                    pltpu.make_async_copy(send3.at[me], recv3.at[me], rsem3.at[sub]).start()

    def group(i, _):
        a0 = group_of(i)
        for jh in range(2):
            y = dft8([g_ref[8 * k0 + a0, pl.ds(4 * jh, 4)] for k0 in range(8)], -sg)
            for a1 in range(8):
                d = 16 * a1 + 2 * a0 + jh
                send3[d, 0:16], send3[d, 16:17] = pack(y[a1] * (1.0 / N))
        copies(a0, EARLY_Z)
        return 0

    lax.fori_loop(0, 8, group, 0)

    def rest(i, _):
        copies(group_of(i), LATE_Z)
        return 0

    lax.fori_loop(0, 8, rest, 0)

    for s in range(SUB):
        block = recv3.at[pl.ds(s * STA, STA)]
        pltpu.make_async_copy(block, block, rsem3.at[s]).wait()
    others = pl.ds(0, STA - 1)
    pltpu.make_async_copy(send1.at[others], send1.at[others], sem1).wait()
    pltpu.make_async_copy(send2.at[others], send2.at[others], sem2).wait()
    others = pl.ds(0, SUB * STA - 1)
    pltpu.make_async_copy(send3.at[others], send3.at[others], sem3).wait()


def assemble(q_ref, out_hbm, int_ref, out_ref, acc_ref, out_sem):
    acc_ref[...] = jnp.zeros_like(acc_ref)

    def one(s, _):
        for sta in range(STA):
            src = s * STA + sta
            v = unpack(q_ref[src])
            acc_ref[sta] += v * v
            for j4 in range(4):
                for ri in range(2):
                    first = s * 256 + (ri * 128 + sta * 16 + j4)
                    out_ref[pl.ds(first, 4, stride=4), :] = v[j4, 4 * ri : 4 * ri + 4]
        rows = pl.ds(pl.multiple_of(s * 256, 256), 256)
        pltpu.make_async_copy(out_ref.at[rows], out_hbm.at[rows], out_sem).start()
        return 0

    lax.fori_loop(0, SUB, one, 0)
    for sta in range(STA):
        for j4 in range(4):
            v = acc_ref[sta, j4]
            v = (v + swap(v)) * (1.0 / SUB)
            int_ref[pl.ds(sta * 16 + j4, 4, stride=4), :] = v[0:4]
    pltpu.make_async_copy(out_ref, out_hbm, out_sem).wait()


VM = pl.BlockSpec(memory_space=pltpu.VMEM)
SM = pl.BlockSpec(memory_space=pltpu.SMEM)
ANY = pl.BlockSpec(memory_space=pl.ANY)
HBM = pl.BlockSpec(memory_space=pltpu.HBM)


def shards(voltages, beam_weights, station_delays, dm_index):
    w1, w2 = dft_tables()
    big, small, inner = twist_tables()
    moved = pl.pallas_call(
        kernel,
        out_shape=pltpu.VMEM((128, 17, 128), jnp.int32),
        in_specs=[HBM] * 9,
        out_specs=ANY,
        scratch_shapes=[
            pltpu.SMEM((8,), jnp.int32),
            pltpu.SMEM((4,), jnp.int32),
            pltpu.VMEM((1, 2, 32, 64), BF16),
            pltpu.VMEM((1, 2, 8, N), BF16),
            pltpu.VMEM((256, 256), BF16),
            pltpu.VMEM((128, 256), BF16),
            pltpu.VMEM((2, 8, 128), F32),
            pltpu.VMEM((2, 64, 8, 128), F32),
            pltpu.VMEM((2, 8, 8, 128), F32),
            pltpu.VMEM((2, 640, 8, 128), F32),
            pltpu.VMEM((8, 16, 8192), BF16),
            pltpu.VMEM((8, 16, 8192), BF16),
            pltpu.VMEM((64, 128), BF16),
            pltpu.VMEM((64, 8, 8, 128), F32),
            pltpu.VMEM((8, CH, 33, 128), jnp.int32),
            pltpu.VMEM((8, CH, 33, 128), jnp.int32),
            pltpu.VMEM((512, 128), F32),
            pltpu.VMEM((512, 8, 128), F32),
            pltpu.VMEM((512, 256), BF16),
            pltpu.VMEM((8, 8, 8, 128), F32),
            pltpu.VMEM((64, 8, 8, 128), F32),
            pltpu.VMEM((128, 17, 128), jnp.int32),
            pltpu.SemaphoreType.DMA((LOADS + 8,)),
            pltpu.SemaphoreType.REGULAR,
            pltpu.SemaphoreType.REGULAR,
            pltpu.SemaphoreType.DMA,
            pltpu.SemaphoreType.DMA((CH,)),
            pltpu.SemaphoreType.DMA,
            pltpu.SemaphoreType.DMA((CH,)),
            pltpu.SemaphoreType.DMA,
            pltpu.SemaphoreType.DMA((SUB,)),
        ],
        compiler_params=pltpu.CompilerParams(
            collective_id=0, has_side_effects=True, vmem_limit_bytes=56 * 1024 * 1024
        ),
    )(
        station_delays, dm_index.reshape(4), voltages, beam_weights,
        jnp.asarray(w1), jnp.asarray(w2), jnp.asarray(small), jnp.asarray(big), jnp.asarray(inner),
    )
    out, power = pl.pallas_call(
        assemble,
        out_shape=(jax.ShapeDtypeStruct((4096, 128), F32), jax.ShapeDtypeStruct((128, 128), F32)),
        in_specs=[VM],
        out_specs=(ANY, VM),
        scratch_shapes=[
            pltpu.VMEM((4096, 128), F32),
            pltpu.VMEM((STA, 4, 8, 128), F32),
            pltpu.SemaphoreType.DMA,
        ],
        compiler_params=pltpu.CompilerParams(vmem_limit_bytes=16 * 1024 * 1024),
    )(moved)
    return out.reshape(16, 2, 32, 1, 512), power.reshape(32, 1, 512)


def solution(mesh):
    return jax.shard_map(
        shards,
        mesh=mesh,
        in_specs=(
            P("sub", None, "sta", None),
            P("sub", None, None, None),
            P("sta"),
            P("sta", None),
        ),
        out_specs=(P(None, None, None, None, ("sub", "sta")), P(None, None, ("sub", "sta"))),
        check_vma=False,
    )
```

```python
import functools

import jax
import jax.numpy as jnp
import numpy as np
from jax import lax
from jax.experimental import pallas as pl
from jax.experimental.pallas import tpu as pltpu
from jax.sharding import PartitionSpec as P

TWO_PI = 6.283185307179586
DISPERSION = 4148808000.0
DM_STEP = 10.0
BASE_FREQ = 120.0
CHANNEL_WIDTH = 0.1953125
F32 = jnp.float32
BF16 = jnp.bfloat16
N = 65536
STA = 8
SUB = 16
INV_SQRT2 = 0.7071067811865476


MESH = pl.DeviceIdType.MESH
LOG_TOP = float(np.log2(32640.0))
CH = 8
LOADS = 8
QUARTER = LOADS // 4
HEAD_START = 13


def dft_tables():
    k = np.arange(128)
    ang = 2.0 * np.pi * ((k[:, None] * k[None, :]) % 128) / 128.0
    full = np.concatenate([np.cos(ang), np.sin(ang)], axis=1).astype(np.float32)
    hi = full.astype(jnp.bfloat16)
    lo = (full - hi.astype(np.float32)).astype(jnp.bfloat16)
    return np.concatenate([hi, hi], axis=0), lo


def twist_tables():
    at = np.arange(64)
    ka = (8 * (at % 8) + at // 8)[:, None]
    n = np.arange(1024)[None, :]
    ang = 2.0 * np.pi * (ka * n) / N
    big = np.stack([np.cos(ang), np.sin(ang)]).reshape(2, 64, 8, 128)
    kj = np.arange(8)[:, None]
    c = np.arange(128)[None, :]
    ang = 2.0 * np.pi * (kj * c) / 1024.0
    small = np.stack([np.cos(ang), np.sin(ang)])
    e = np.arange(8)
    ang = 2.0 * np.pi * (e[:, None] * e[None, :]) / 64.0
    inner = np.stack([np.cos(ang), np.sin(ang)])[..., None] * np.ones(128)
    return big.astype(np.float32), small.astype(np.float32), inner.astype(np.float32)


def sign_rows():
    row = lax.broadcasted_iota(jnp.int32, (8, 128), 0)
    return jnp.where(row < 4, 1.0, -1.0).astype(F32)


def swap(x):
    return pltpu.roll(x, 4, x.ndim - 2)


def dft8(x, sg):
    def times_j(v):
        return swap(v) * sg

    def dft4(a0, a1, a2, a3):
        t0, t1, t2, t3 = a0 + a2, a0 - a2, a1 + a3, times_j(a1 - a3)
        return t0 + t2, t1 + t3, t0 - t2, t1 - t3

    e = dft4(x[0], x[2], x[4], x[6])
    o = dft4(x[1], x[3], x[5], x[7])
    j1, j3 = times_j(o[1]), times_j(o[3])
    o = (o[0], (o[1] + j1) * INV_SQRT2, times_j(o[2]), (j3 - o[3]) * INV_SQRT2)
    return [e[k] + o[k] for k in range(4)] + [e[k] - o[k] for k in range(4)]


def cmul(x, wr, wi, sg):
    return x * wr + (swap(x) * sg) * wi


def split(x):
    hi = x.astype(BF16)
    lo = (x - hi.astype(F32)).astype(BF16)
    return hi, lo


def unpack_voltages(x_ref, xf_ref, piece):
    per = 512 // LOADS

    def body(i, _):
        for u in range(8):
            t = piece * per + i * 8 + u
            col = pl.multiple_of(t * 128, 128)
            for ri in range(2):
                v = x_ref[0, ri, :, pl.ds(col, 128)].astype(F32)
                xf_ref[ri, t + 128] = v
                if piece >= LOADS - QUARTER:
                    xf_ref[ri, t - 384] = v
        return 0

    lax.fori_loop(0, per // 8, body, 0)


def delay_setup(d_ref):
    row = lax.broadcasted_iota(jnp.int32, (8, 128), 0)
    lane = lax.broadcasted_iota(jnp.int32, (8, 128), 1)
    fine = jnp.zeros((8, 128), jnp.int32)
    starts = []
    for r in range(8):
        d = d_ref[r]
        starts.append(128 - d // 128)
        fine = jnp.where(row == r, d % 128, fine)
    return starts, [row == r for r in range(8)], (lane - fine + 128) % 128, lane >= fine


def delay_rows(setup, xf_ref, out_ref, a0, low=0, high=8):
    starts, masks, index, keep = setup

    def body(a1, _):
        t = (8 * a1 + a0) * 8
        col = pl.multiple_of((8 * a0 + a1) * 128, 128)
        done = []
        for ri in range(2):
            acc = xf_ref[ri, pl.ds(starts[0] + t - 1, 9)]
            for r in range(1, 8):
                acc = jnp.where(masks[r], xf_ref[ri, pl.ds(starts[r] + t - 1, 9)], acc)
            g = [jnp.take_along_axis(acc[u], index, axis=1) for u in range(9)]
            done.append([jnp.where(keep, g[u + 1], g[u]) for u in range(8)])
        for j in range(8):
            out_ref[j, :, pl.ds(col, 128)] = jnp.concatenate([done[0][j], done[1][j]], axis=0).astype(BF16)
        return 0

    lax.fori_loop(low, high, body, 0, unroll=4)


def one_hot(shape, hit):
    row = lax.broadcasted_iota(jnp.int32, shape, 0)
    col = lax.broadcasted_iota(jnp.int32, shape, 1)
    return jnp.where(hit(row, col), 1.0, 0.0).astype(BF16)


def stacked_weights(bw_ref):
    w0, w1 = bw_ref[0, 0], bw_ref[0, 1]
    to_real = one_hot((64, 128), lambda q, c: c == (q // 8) * 16 + q % 8)
    to_imag = one_hot((64, 128), lambda q, c: c == (q // 8) * 16 + 8 + q % 8)
    dot = functools.partial(jnp.dot, preferred_element_type=F32)
    real = (dot(w0, to_real) - dot(w1, to_imag)).astype(BF16)
    imag = (dot(w1, to_real) + dot(w0, to_imag)).astype(BF16)
    rows_real = one_hot((64, 32), lambda r, b: r == (b // 4) * 8 + b % 4)
    rows_imag = one_hot((64, 32), lambda r, b: r == (b // 4) * 8 + 4 + b % 4)
    return (dot(rows_real, real) + dot(rows_imag, imag)).astype(BF16)


def beamform(w_ref, v_ref, bm_ref, part):
    w = w_ref[...]

    def body(i, _):
        first = part * 8 + i * 4
        v = v_ref[:, :, pl.ds(pl.multiple_of(first * 128, 512), 512)].reshape(128, 512)
        out = jnp.dot(w, v, preferred_element_type=F32)
        for u in range(4):
            bm_ref[first + u] = out[:, u * 128 : (u + 1) * 128].reshape(8, 8, 128)
        return 0

    lax.fori_loop(0, 2, body, 0, unroll=2)


def inner_pass(ref, lead, twi_ref, sg):
    def body(g, _):
        at = pl.ds(g * 2, 2)
        y = dft8([ref[8 * lead + i, at] for i in range(8)], sg)
        for k in range(8):
            v = y[k]
            if k:
                v = cmul(v, twi_ref[0, lead, pl.ds(k, 1)], twi_ref[1, lead, pl.ds(k, 1)], sg)
            ref[8 * lead + k, at] = v
        return 0

    lax.fori_loop(0, 4, body, 0, unroll=4)


def power_scale(top, axes):
    top = jnp.maximum(jnp.max(top, axis=axes, keepdims=True), 1e-33)
    power = jnp.ceil(jnp.log2(top) - LOG_TOP)
    return jnp.exp2(-power), power.astype(jnp.int32)


def two_in_one(high, low):
    return (jnp.round(high).astype(jnp.int32) << 16) | (jnp.round(low).astype(jnp.int32) & 0xFFFF)


def one_of_two(words):
    return (words >> 16).astype(F32), ((words << 16) >> 16).astype(F32)


def pack(values):
    factor, power = power_scale(jnp.abs(values), (0, 1))
    q = values * factor
    return two_in_one(q[0:2], q[2:4]).reshape(16, 128), power.reshape(1, 128)


def unpack(block):
    high, low = one_of_two(block[0:16].reshape(2, 8, 128))
    return jnp.concatenate([high, low], axis=0) * jnp.exp2(block[16:17].astype(F32))


def outer_and_encode(bm_ref, k0, sta, twb_ref, sg, q_ref):
    for g in range(4):
        at = pl.ds(2 * g, 2)
        y = dft8([bm_ref[8 * i + k0, at] for i in range(8)], sg)
        out = []
        for k1 in range(8):
            k = 8 * k0 + k1
            out.append(cmul(y[k1], twb_ref[0, k, pl.ds(sta, 1)], twb_ref[1, k, pl.ds(sta, 1)], sg))
        factor, power = power_scale(functools.reduce(jnp.maximum, [jnp.abs(v) for v in out]), 1)
        for m in range(4):
            q_ref[at, k0, 8 * m : 8 * m + 8] = two_in_one(out[2 * m] * factor, out[2 * m + 1] * factor)
        q_ref[at, k0, 32:33] = power


def chirp_table(dm_ref, base_ref, h_ref, first, last):
    row = lax.broadcasted_iota(jnp.int32, (8, 128), 0)
    lane = lax.broadcasted_iota(jnp.int32, (8, 128), 1)
    centre = BASE_FREQ + CHANNEL_WIDTH * (
        jnp.zeros((8, 128), F32) + lax.axis_index("sub").astype(F32) + 0.5
    )

    def base(i, _):
        k0, kj = i // 8, i % 8
        positions = 8 * row + k0 + 64 * kj + 512 * lane
        signed_bin = jnp.where(positions < N // 2, positions, positions - N)
        offset = CHANNEL_WIDTH * signed_bin.astype(F32) / N
        base_ref[pl.ds(pl.multiple_of(i * 8, 8), 8), :] = (
            TWO_PI * DISPERSION * offset * offset / (centre * centre * (centre + offset))
        )
        return 0

    lax.fori_loop(first * 4, last * 4, base, 0)
    quarter = jnp.where(row < 4, 1, 0)
    dm = jnp.zeros((8, 128), F32)
    for b in range(4):
        dm = jnp.where(row % 4 == b, DM_STEP * dm_ref[b].astype(F32), dm)
    p1 = 1.5703125
    p2 = float(np.float32(np.round((np.pi / 2 - p1) * 2.0**22) / 2.0**22))
    p3 = float(np.float32(np.pi / 2 - p1 - p2))

    def one(r):
        phase = dm * base_ref[pl.ds(r, 1), :]
        n = jnp.floor(phase * float(2.0 / np.pi) + 0.5)
        y = ((phase - n * p1) - n * p2) - n * p3
        q = n.astype(jnp.int32) + quarter
        z = y * y
        s = ((-1.9515295891e-4 * z + 8.3321608736e-3) * z - 1.6666654611e-1) * z * y + y
        c = ((2.443315711809948e-5 * z - 1.388731625493765e-3) * z + 4.166664568298827e-2) * z * z - 0.5 * z + 1.0
        v = jnp.where((q & 1) == 0, s, c)
        h_ref[r] = jnp.where((q & 2) == 0, v, -v)

    def body(i, _):
        for u in range(4):
            one(i * 4 + u)
        return 0

    lax.fori_loop(first * 8, last * 8, body, 0)


def middle(k0, r_ref, h_ref, w1_ref, w2_ref, tws_ref, twb_ref, xs_ref, gt_ref, g_ref, sg):
    scales = [jnp.exp2(r_ref[j, k0, 32:33].astype(F32)) for j in range(8)]
    for m in range(4):
        x = [jnp.stack(one_of_two(r_ref[j, k0, 8 * m : 8 * m + 8])) * scales[j] for j in range(8)]
        y = dft8(x, sg)
        for kj in range(8):
            v = y[kj]
            if kj:
                v = cmul(v, tws_ref[0, pl.ds(kj, 1)], tws_ref[1, pl.ds(kj, 1)], sg)
            hi, lo = split(v.reshape(16, 128))
            at = kj * 64 + m * 16
            xs_ref[at : at + 16, 0:128] = hi
            xs_ref[at : at + 16, 128:256] = lo

    def dot128(sign):
        x = xs_ref[...]
        pq = jnp.dot(x, w1_ref[...], preferred_element_type=F32)
        pq = pq + jnp.dot(x[:, 0:128], w2_ref[...], preferred_element_type=F32)
        return pq[:, 0:128].reshape(64, 8, 128) + swap(pq[:, 128:256].reshape(64, 8, 128)) * sign

    low = lax.broadcasted_iota(jnp.int32, (8, 128), 0) < 4
    v = dot128(sg)
    h = h_ref[pl.ds(k0 * 64, 64)]
    hs = swap(h)
    v = v * jnp.where(low, h, hs) + swap(v) * jnp.where(low, -hs, h)
    hi, lo = split(v.reshape(512, 128))
    xs_ref[:, 0:128] = hi
    xs_ref[:, 128:256] = lo
    gt_ref[...] = dot128(-sg).reshape(8, 8, 8, 128)

    for i in range(4):
        x = []
        for kj in range(8):
            v = gt_ref[kj, 2 * i : 2 * i + 2]
            if kj:
                v = cmul(v, tws_ref[0, pl.ds(kj, 1)], tws_ref[1, pl.ds(kj, 1)], -sg)
            x.append(v)
        y = dft8(x, -sg)
        here = pl.ds(k0 * 8 + i * 2, 2)
        for j in range(8):
            g_ref[here, j] = cmul(y[j], twb_ref[0, here, pl.ds(j, 1)], twb_ref[1, here, pl.ds(j, 1)], -sg)


EARLY_Z, LATE_Z = (0, 1), (2, 3)


def kernel(
    d_hbm, dm_hbm, x_hbm, bw_hbm, w1_hbm, w2_hbm, tws_hbm, twb_hbm, twi_hbm,
    recv3,
    d_ref, dm_ref, bw_ref, x_ref, w1_ref, w2_ref, tws_ref, twb_ref, twi_ref,
    xf_ref, send1, recv1, w_ref, bm_ref, send2, recv2, base_ref, h_ref, xs_ref, gt_ref, g_ref,
    send3,
    load_sem, answer_sem, col_sem, sem1, rsem1, sem2, rsem2, sem3, rsem3,
):
    sub, sta = lax.axis_index("sub"), lax.axis_index("sta")
    me = sub * STA + sta

    x_loads = []
    for i in range(LOADS):
        cols = pl.ds(i * (N // LOADS), N // LOADS)
        x_loads.append(pltpu.make_async_copy(x_hbm.at[:, :, :, cols], x_ref.at[:, :, :, cols], load_sem.at[i]))
    tables = [
        pltpu.make_async_copy(a, b, load_sem.at[LOADS + i])
        for i, (a, b) in enumerate(
            [
                (d_hbm, d_ref), (dm_hbm, dm_ref), (bw_hbm, bw_ref), (w1_hbm, w1_ref), (w2_hbm, w2_ref),
                (tws_hbm, tws_ref), (twb_hbm, twb_ref), (twi_hbm, twi_ref),
            ]
        )
    ]
    order = [(i - QUARTER) % LOADS for i in range(LOADS)]
    for t in tables[:1] + [x_loads[i] for i in order] + tables[1:2]:
        t.start()

    barrier = pltpu.get_barrier_semaphore()
    for i in range(1, STA):
        pl.semaphore_signal(barrier, inc=1, device_id={"sub": sub, "sta": (sta + i) % STA}, device_id_type=MESH)
    x_hi, z, core = sub // 8, (sub // 2) % 4, sub % 2
    rank = 4 * z + 2 * x_hi + core

    def column(r):
        return {"sub": 8 * ((r // 2) % 2) + 2 * (r // 4) + r % 2, "sta": sta}

    def greet(r, _):
        pl.semaphore_signal(barrier, inc=1, device_id=column(r), device_id_type=MESH)
        return 0

    lax.fori_loop(rank + 1, SUB, greet, 0)
    def load(pieces):
        for i in pieces:
            x_loads[i].wait()
            unpack_voltages(x_ref, xf_ref, i)

    tables[0].wait()
    setup = delay_setup(d_ref)
    load(order[:QUARTER])

    def first(part, start, size):
        cols = pl.ds(pl.multiple_of(start, size), size)
        for i in range(1, STA):
            d = (sta + i) % STA
            pltpu.make_async_remote_copy(
                src_ref=send1.at[d, :, cols],
                dst_ref=recv1.at[sta, :, cols],
                send_sem=sem1,
                recv_sem=rsem1.at[part],
                device_id={"sub": sub, "sta": d},
                device_id_type=MESH,
            ).start()
        pltpu.make_async_copy(send1.at[sta, :, cols], recv1.at[sta, :, cols], rsem1.at[part]).start()

    tables[1].wait()
    late = HEAD_START * (1 - (sub % 2))
    chirp_table(dm_ref, base_ref, h_ref, 0, late)
    load(order[QUARTER:])
    delay_rows(setup, xf_ref, send1, 0)
    pl.semaphore_wait(barrier, STA - 1 + rank)
    first(0, 0, 1024)
    def answer(r, _):
        pl.semaphore_signal(answer_sem, inc=1, device_id=column(r), device_id_type=MESH)
        return 0

    lax.fori_loop(0, rank, answer, 0)

    def more(part, _):
        delay_rows(setup, xf_ref, send1, part)
        first(part, part * 1024, 1024)
        return 0

    lax.fori_loop(1, CH, more, 0)
    for t in tables[2:]:
        t.start()

    for t in tables[2:]:
        t.wait()
    w_ref[...] = stacked_weights(bw_ref)
    chirp_table(dm_ref, base_ref, h_ref, late, 16)
    @pl.when(rank < SUB - 1)
    def _():
        pl.semaphore_wait(answer_sem, SUB - 1 - rank)

    for i in range(1, STA):
        pl.semaphore_signal(col_sem, inc=1, device_id={"sub": sub, "sta": (sta + i) % STA}, device_id_type=MESH)
    sg = sign_rows()

    def beams(part, _):
        cols = pl.ds(pl.multiple_of(part * 1024, 1024), 1024)
        pltpu.make_async_copy(recv1.at[:, :, cols], recv1.at[:, :, cols], rsem1.at[part]).wait()
        beamform(w_ref, recv1, bm_ref, part)
        inner_pass(bm_ref, part, twi_ref, sg)
        return 0

    lax.fori_loop(0, CH, beams, 0)

    def second(part, _):
        outer_and_encode(bm_ref, part, sta, twb_ref, sg, send2)
        for i in range(1, STA):
            d = (sta + i) % STA
            pltpu.make_async_remote_copy(
                src_ref=send2.at[d, part],
                dst_ref=recv2.at[sta, part],
                send_sem=sem2,
                recv_sem=rsem2.at[part],
                device_id={"sub": sub, "sta": d},
                device_id_type=MESH,
            ).start()
        pltpu.make_async_copy(send2.at[sta, part], recv2.at[sta, part], rsem2.at[part]).start()
        return 0

    lax.fori_loop(0, CH, second, 0)

    def spectra(part, _):
        pltpu.make_async_copy(recv2.at[:, part], recv2.at[:, part], rsem2.at[part]).wait()
        middle(part, recv2, h_ref, w1_ref, w2_ref, tws_ref, twb_ref, xs_ref, gt_ref, g_ref, sg)
        inner_pass(g_ref, part, twi_ref, -sg)
        return 0

    lax.fori_loop(0, CH, spectra, 0)

    pl.semaphore_wait(col_sem, STA - 1)
    x_lo, yh, jh_own = sta // 4, (sta // 2) % 2, sta % 2

    def group_of(i):
        return 4 * ((core + 1 - i // 4) % 2) + 2 * ((x_lo + 1 - (i // 2) % 2) % 2) + (yh + 1 - i % 2) % 2

    def copies(a0, planes):
        for n, z_to in enumerate(planes * 4):
            dx, dj = 1 - n // (2 * len(planes)), 1 - (n // len(planes)) % 2
            d = 64 * ((x_hi + dx) % 2) + 16 * z_to + 2 * a0 + (jh_own + dj) % 2

            def go():
                pltpu.make_async_remote_copy(
                    src_ref=send3.at[d],
                    dst_ref=recv3.at[me],
                    send_sem=sem3,
                    recv_sem=rsem3.at[sub],
                    device_id={"sub": d // STA, "sta": d % STA},
                    device_id_type=MESH,
                ).start()

            if dx or dj:
                go()
            else:
                pl.when(d != me)(go)

                @pl.when(d == me)
                def _():
                    pltpu.make_async_copy(send3.at[me], recv3.at[me], rsem3.at[sub]).start()

    def group(i, _):
        a0 = group_of(i)
        for jh in range(2):
            y = dft8([g_ref[8 * k0 + a0, pl.ds(4 * jh, 4)] for k0 in range(8)], -sg)
            for a1 in range(8):
                d = 16 * a1 + 2 * a0 + jh
                send3[d, 0:16], send3[d, 16:17] = pack(y[a1] * (1.0 / N))
        copies(a0, EARLY_Z)
        return 0

    lax.fori_loop(0, 8, group, 0)

    def rest(i, _):
        copies(group_of(i), LATE_Z)
        return 0

    lax.fori_loop(0, 8, rest, 0)

    for s in range(SUB):
        block = recv3.at[pl.ds(s * STA, STA)]
        pltpu.make_async_copy(block, block, rsem3.at[s]).wait()
    others = pl.ds(0, STA - 1)
    pltpu.make_async_copy(send1.at[others], send1.at[others], sem1).wait()
    pltpu.make_async_copy(send2.at[others], send2.at[others], sem2).wait()
    others = pl.ds(0, SUB * STA - 1)
    pltpu.make_async_copy(send3.at[others], send3.at[others], sem3).wait()


def assemble(q_ref, out_hbm, int_ref, out_ref, acc_ref, out_sem):
    acc_ref[...] = jnp.zeros_like(acc_ref)

    def one(s, _):
        for sta in range(STA):
            src = s * STA + sta
            v = unpack(q_ref[src])
            acc_ref[sta] += v * v
            for j4 in range(4):
                for ri in range(2):
                    first = s * 256 + (ri * 128 + sta * 16 + j4)
                    out_ref[pl.ds(first, 4, stride=4), :] = v[j4, 4 * ri : 4 * ri + 4]
        rows = pl.ds(pl.multiple_of(s * 256, 256), 256)
        pltpu.make_async_copy(out_ref.at[rows], out_hbm.at[rows], out_sem).start()
        return 0

    lax.fori_loop(0, SUB, one, 0)
    for sta in range(STA):
        for j4 in range(4):
            v = acc_ref[sta, j4]
            v = (v + swap(v)) * (1.0 / SUB)
            int_ref[pl.ds(sta * 16 + j4, 4, stride=4), :] = v[0:4]
    pltpu.make_async_copy(out_ref, out_hbm, out_sem).wait()


VM = pl.BlockSpec(memory_space=pltpu.VMEM)
SM = pl.BlockSpec(memory_space=pltpu.SMEM)
ANY = pl.BlockSpec(memory_space=pl.ANY)
HBM = pl.BlockSpec(memory_space=pltpu.HBM)


def shards(voltages, beam_weights, station_delays, dm_index):
    w1, w2 = dft_tables()
    big, small, inner = twist_tables()
    moved = pl.pallas_call(
        kernel,
        out_shape=pltpu.VMEM((128, 17, 128), jnp.int32),
        in_specs=[HBM] * 9,
        out_specs=ANY,
        scratch_shapes=[
            pltpu.SMEM((8,), jnp.int32),
            pltpu.SMEM((4,), jnp.int32),
            pltpu.VMEM((1, 2, 32, 64), BF16),
            pltpu.VMEM((1, 2, 8, N), BF16),
            pltpu.VMEM((256, 256), BF16),
            pltpu.VMEM((128, 256), BF16),
            pltpu.VMEM((2, 8, 128), F32),
            pltpu.VMEM((2, 64, 8, 128), F32),
            pltpu.VMEM((2, 8, 8, 128), F32),
            pltpu.VMEM((2, 640, 8, 128), F32),
            pltpu.VMEM((8, 16, 8192), BF16),
            pltpu.VMEM((8, 16, 8192), BF16),
            pltpu.VMEM((64, 128), BF16),
            pltpu.VMEM((64, 8, 8, 128), F32),
            pltpu.VMEM((8, CH, 33, 128), jnp.int32),
            pltpu.VMEM((8, CH, 33, 128), jnp.int32),
            pltpu.VMEM((512, 128), F32),
            pltpu.VMEM((512, 8, 128), F32),
            pltpu.VMEM((512, 256), BF16),
            pltpu.VMEM((8, 8, 8, 128), F32),
            pltpu.VMEM((64, 8, 8, 128), F32),
            pltpu.VMEM((128, 17, 128), jnp.int32),
            pltpu.SemaphoreType.DMA((LOADS + 8,)),
            pltpu.SemaphoreType.REGULAR,
            pltpu.SemaphoreType.REGULAR,
            pltpu.SemaphoreType.DMA,
            pltpu.SemaphoreType.DMA((CH,)),
            pltpu.SemaphoreType.DMA,
            pltpu.SemaphoreType.DMA((CH,)),
            pltpu.SemaphoreType.DMA,
            pltpu.SemaphoreType.DMA((SUB,)),
        ],
        compiler_params=pltpu.CompilerParams(
            collective_id=0, has_side_effects=True, vmem_limit_bytes=56 * 1024 * 1024
        ),
    )(
        station_delays, dm_index.reshape(4), voltages, beam_weights,
        jnp.asarray(w1), jnp.asarray(w2), jnp.asarray(small), jnp.asarray(big), jnp.asarray(inner),
    )
    out, power = pl.pallas_call(
        assemble,
        out_shape=(jax.ShapeDtypeStruct((4096, 128), F32), jax.ShapeDtypeStruct((128, 128), F32)),
        in_specs=[VM],
        out_specs=(ANY, VM),
        scratch_shapes=[
            pltpu.VMEM((4096, 128), F32),
            pltpu.VMEM((STA, 4, 8, 128), F32),
            pltpu.SemaphoreType.DMA,
        ],
        compiler_params=pltpu.CompilerParams(vmem_limit_bytes=16 * 1024 * 1024),
    )(moved)
    return out.reshape(16, 2, 32, 1, 512), power.reshape(32, 1, 512)


def solution(mesh):
    return jax.shard_map(
        shards,
        mesh=mesh,
        in_specs=(
            P("sub", None, "sta", None),
            P("sub", None, None, None),
            P("sta"),
            P("sta", None),
        ),
        out_specs=(P(None, None, None, None, ("sub", "sta")), P(None, None, ("sub", "sta"))),
        check_vma=False,
    )
```
